128 devices in a mesh: model: 1, replica: 64 (over z, y, x), fsdp: 2 (over core).
Axes of the slice: x: 4, y: 4, z: 4, core: 2. Of those that a mesh axis runs over, the one named last changes fastest.
Arguments:
- x_in: bfloat16 [4, 65536, 1024], P(None, ('model', 'replica', 'fsdp'))
- dy_out: bfloat16 [4, 65536, 1024], P(None, ('model', 'replica', 'fsdp'))
- lengths: int32 [4, 128], P(None, ('model', 'replica', 'fsdp'))
- w_up: bfloat16 [1, 1024, 4096], P(None, ('model', 'fsdp'))
- w_down: bfloat16 [1, 4096, 1024], P(None, ('model', 'fsdp'))
Outputs:
- output 1: float32 [1, 1024, 4096], P(None, ('model', 'fsdp'))
- output 2: float32 [1, 4096, 1024], P(None, ('model', 'fsdp'))
All inputs are finite; a program needn't handle non-finite values.
Results may differ from the reference program's by a relative error of at most 0.001.
Values are sent between devices in bfloat16 or wider.
A program may use at most 1 GiB of HBM per device.

```python
import jax
import jax.numpy as jnp
from jax import lax

D_MODEL = 1024
D_FF = 4096
N_LAYERS = 1
N_MICRO = 4
TOK_DEV = 512
N_REPLICA = 64
N_FSDP = 2

GROUP_DEV = N_REPLICA * N_FSDP
TOKENS = GROUP_DEV * TOK_DEV


def setup_inputs(seed: int = 0, part: int = 0) -> dict:
    base_key = jax.random.fold_in(jax.random.key(seed), part)
    key_list = jax.random.split(base_key, 5)
    grad_scale = (N_MICRO * TOKENS) ** -0.5
    x_in = jax.random.normal(key_list[0], (N_MICRO, TOKENS, D_MODEL), jnp.float32).astype(jnp.bfloat16)
    dy_out = (jax.random.normal(key_list[1], (N_MICRO, TOKENS, D_MODEL), jnp.float32) * grad_scale).astype(jnp.bfloat16)
    lengths = jax.random.randint(key_list[2], (N_MICRO, GROUP_DEV), TOK_DEV // 4, TOK_DEV + 1, dtype=jnp.int32)
    lengths = lengths.at[0, 0].set(TOK_DEV).at[N_MICRO - 1, GROUP_DEV - 1].set(TOK_DEV // 4)
    w_up = (jax.random.normal(key_list[3], (N_LAYERS, D_MODEL, D_FF), jnp.float32) * D_MODEL ** -0.5).astype(jnp.bfloat16)
    w_down = (jax.random.normal(key_list[4], (N_LAYERS, D_FF, D_MODEL), jnp.float32) * D_FF ** -0.5).astype(jnp.bfloat16)
    return {"x_in": x_in, "dy_out": dy_out, "lengths": lengths, "w_up": w_up, "w_down": w_down}


def layer_forward(x_cur, weights):
    w_up_l, w_down_l = weights
    hidden = jnp.dot(x_cur, w_up_l, preferred_element_type=jnp.float32).astype(jnp.bfloat16)
    act_bf = jax.nn.gelu(hidden.astype(jnp.float32)).astype(jnp.bfloat16)
    x_next = (x_cur.astype(jnp.float32) + jnp.dot(act_bf, w_down_l, preferred_element_type=jnp.float32)).astype(jnp.bfloat16)
    return x_next, (x_cur, hidden)


def layer_backward(grad_x, item):
    w_up_l, w_down_l, x_cur, hidden = item
    act_f32, gelu_vjp = jax.vjp(jax.nn.gelu, hidden.astype(jnp.float32))
    act_bf = act_f32.astype(jnp.bfloat16)
    grad_act = jnp.dot(grad_x, w_down_l.T, preferred_element_type=jnp.float32)
    grad_hid = gelu_vjp(grad_act)[0].astype(jnp.bfloat16)
    gw_down = jnp.dot(act_bf.T, grad_x, preferred_element_type=jnp.float32)
    gw_up = jnp.dot(x_cur.T, grad_hid, preferred_element_type=jnp.float32)
    grad_prev = (grad_x.astype(jnp.float32) + jnp.dot(grad_hid, w_up_l.T, preferred_element_type=jnp.float32)).astype(jnp.bfloat16)
    return grad_prev, (gw_up, gw_down)


def reference(x_in, dy_out, lengths, w_up, w_down):
    n_blocks = N_MICRO * GROUP_DEV
    x_blocks = x_in.reshape(n_blocks, TOK_DEV, D_MODEL)
    dy_blocks = dy_out.reshape(n_blocks, TOK_DEV, D_MODEL)
    len_blocks = lengths.reshape(n_blocks)

    def block_grads(acc_pair, block_in):
        x_blk, dy_blk, len_blk = block_in
        _, saved_acts = lax.scan(layer_forward, x_blk, (w_up, w_down))
        token_mask = jnp.arange(TOK_DEV) < len_blk
        grad_top = jnp.where(token_mask[:, None], dy_blk, jnp.zeros_like(dy_blk))
        _, grads = lax.scan(layer_backward, grad_top, (w_up, w_down, saved_acts[0], saved_acts[1]), reverse=True)
        return (acc_pair[0] + grads[0], acc_pair[1] + grads[1]), None

    init_pair = (jnp.zeros((N_LAYERS, D_MODEL, D_FF), jnp.float32), jnp.zeros((N_LAYERS, D_FF, D_MODEL), jnp.float32))
    (grad_up, grad_down), _ = lax.scan(block_grads, init_pair, (x_blocks, dy_blocks, len_blocks))
    return grad_up, grad_down
```

```python
import jax
import jax.numpy as jnp
from jax import lax
from jax.sharding import PartitionSpec as P


def solution(mesh):
    tok_spec = P(None, ("model", "replica", "fsdp"), None)
    len_spec = P(None, ("model", "replica", "fsdp"))
    w_spec = P(None, ("model", "fsdp"), None)

    def device_grads(x_in, dy_out, lengths, w_up, w_down):
        n_micro, tok_dev, d_model = x_in.shape
        mask = jnp.arange(tok_dev)[None, :] < lengths
        up_full = lax.all_gather(w_up[0], "fsdp", axis=0, tiled=True)
        down_full = lax.all_gather(w_down[0], "fsdp", axis=0, tiled=True)
        x = x_in.reshape(n_micro * tok_dev, d_model)
        dy = jnp.where(mask[:, :, None], dy_out, jnp.zeros_like(dy_out)).reshape(n_micro * tok_dev, d_model)
        hidden = jnp.dot(x, up_full, preferred_element_type=jnp.float32).astype(jnp.bfloat16)
        act_f32, gelu_vjp = jax.vjp(jax.nn.gelu, hidden.astype(jnp.float32))
        act_bf = act_f32.astype(jnp.bfloat16)
        grad_act = jnp.einsum("td,fd->tf", dy, down_full, preferred_element_type=jnp.float32)
        grad_hid = gelu_vjp(grad_act)[0].astype(jnp.bfloat16)
        gw_down = jnp.einsum("tf,td->fd", act_bf, dy, preferred_element_type=jnp.float32)
        gw_up = jnp.einsum("td,tf->df", x, grad_hid, preferred_element_type=jnp.float32)
        grad_down = lax.psum(lax.psum_scatter(gw_down, "fsdp", scatter_dimension=0, tiled=True), "replica")
        grad_up = lax.psum(lax.psum_scatter(gw_up, "fsdp", scatter_dimension=0, tiled=True), "replica")
        return grad_up[None], grad_down[None]

    return jax.shard_map(device_grads, mesh=mesh, in_specs=(tok_spec, tok_spec, len_spec, w_spec, w_spec), out_specs=(w_spec, w_spec), check_vma=False)
```

```python
import functools

import jax
import jax.numpy as jnp
from jax import lax
from jax.experimental import pallas as pl
from jax.experimental.pallas import tpu as pltpu
from jax.sharding import PartitionSpec as P

F32, BF16 = jnp.float32, jnp.bfloat16
MESH_ID = pl.DeviceIdType.MESH
SQRT_2_OVER_PI = 0.7978845608028654
CUBIC = 0.044715
NT_DIMS = (((1,), (1,)), ((), ()))

FC = 256
RING = 4
ROWS = 512
PH_ROWS = (128, 32, 8)
PH_OFF = (0, 384, 480)
R_ROWS = 504
W_SLOTS = 3
P_SLOTS = 2

SCHEDULE = (
    ("pair", 1),
    ("rs0b", 3),
    ("rs0c", 5),
    ("rs1b", 7),
    ("rs1c", 9),
    ("rs2b", 11),
    ("rs2c", 13),
    ("ag2b", 15),
    ("ag2c", 17),
    ("ag1b", 19),
    ("ag1c", 21),
    ("ag0b", 23),
    ("ag0c", 25),
    ("done", 29),
)


def gelu_and_slope(u):
    u2 = u * u
    t = jnp.tanh(SQRT_2_OVER_PI * (u + CUBIC * (u2 * u)))
    half = 0.5 * (1.0 + t)
    slope = half + 0.5 * u * (1.0 - t * t) * (SQRT_2_OVER_PI + (3.0 * CUBIC * SQRT_2_OVER_PI) * u2)
    return u * half, slope


def kernel(n_ticks, n_tok, n_micro,
           x_hbm, dy_hbm, len_ref, wu_hbm, wd_hbm, gu_hbm, gd_hbm,
           X, DY, XT, WU, WD, AT, DH, SU, SD, RU, RD, G, R, E,
           in_sem, w_local, w_send, w_recv, p_send, p_recv, rs1, rs2, ag1, ag2, send0, out_send, out_sem,
           g_free, w_credit, ru_credit, rd_credit):
    n_items = 2 * n_ticks
    tok = n_tok // n_micro
    rep = lax.axis_index("replica")
    me = lax.axis_index("fsdp")
    mate = 1 - me

    def dev(replica, core):
        return (0, replica, core)

    def axis_of(item, phase):
        a = (item + phase) % 3
        stride = 1 + 3 * a + 9 * ((a * (a - 1)) // 2)
        c = (rep // stride) % RING
        return stride, c

    def neighbour(stride, c, d):
        return rep + stride * ((c + d + RING) % RING - c)

    def base_of(item, phase):
        b = 0
        for p in range(phase):
            b = b + axis_of(item, p)[1] * PH_ROWS[p]
        return b

    def g_rows(item, h, start, n):
        row = pl.multiple_of(item * (2 * ROWS) + h * ROWS + start, 8)
        return G.at[pl.ds(row, n)]

    def r_rows(item, h, start, n):
        row = pl.multiple_of(item * (2 * R_ROWS) + h * R_ROWS + start, 8)
        return R.at[pl.ds(row, n)]

    def e_rows(item, h, start, n):
        row = pl.multiple_of(item * (2 * PH_ROWS[0]) + h * PH_ROWS[0] + start, 8)
        return E.at[pl.ds(row, n)]

    def wait_rows(sem, n):
        ref = G.at[pl.ds(0, n)]
        pltpu.make_async_copy(ref, ref, sem).wait()

    barrier = pltpu.get_barrier_semaphore()
    for a in range(3):
        stride = RING**a
        c = (rep // stride) % RING
        for d in (1, -1):
            pl.semaphore_signal(barrier, inc=1, device_id=dev(neighbour(stride, c, d), me), device_id_type=MESH_ID)
    pl.semaphore_signal(barrier, inc=1, device_id=dev(rep, mate), device_id_type=MESH_ID)

    def x_copy(k):
        return pltpu.make_async_copy(x_hbm.at[k], X.at[pl.ds(k * tok, tok)], in_sem.at[k])

    def dy_copy(k):
        return pltpu.make_async_copy(dy_hbm.at[k], DY.at[pl.ds(k * tok, tok)], in_sem.at[n_micro + k])

    for k in range(n_micro):
        x_copy(k).start()
    for k in range(n_micro):
        dy_copy(k).start()

    def w_copies(t):
        slot = t % W_SLOTS
        lo = pl.multiple_of(t * 128, 128)
        hi = pl.multiple_of(n_ticks * 128 + t * 128, 128)
        up_rows = pl.ds(pl.multiple_of(me * 512, 512), 512)
        down_rows = pl.ds(pl.multiple_of(me * 128, 128), 128)
        pairs = (
            (wu_hbm.at[0, :, pl.ds(lo, 128)], WU.at[slot, up_rows, pl.ds(0, 128)]),
            (wu_hbm.at[0, :, pl.ds(hi, 128)], WU.at[slot, up_rows, pl.ds(128, 128)]),
            (wd_hbm.at[0, pl.ds(lo, 128), :], WD.at[slot, down_rows, :]),
        )
        local = [pltpu.make_async_copy(s, d, w_local.at[slot]) for s, d in pairs]
        remote = [
            pltpu.make_async_remote_copy(s, d, w_send.at[slot], w_recv.at[slot], device_id=dev(rep, mate), device_id_type=MESH_ID)
            for s, d in pairs
        ]
        return local, remote

    def start_w(t):
        local, remote = w_copies(t)
        for c in local + remote:
            c.start()

    def wait_w(t):
        slot = t % W_SLOTS
        ref = WU.at[slot]
        for sem in (w_local, w_recv, w_send):
            pltpu.make_async_copy(ref, ref, sem.at[slot]).wait()

    pl.semaphore_wait(barrier, 7)
    start_w(0)
    if n_ticks > 1:
        start_w(1)

    rb = min(256, tok)
    for k in range(n_micro):
        x_copy(k).wait()

        def transpose_rows(s, carry, k=k):
            rows = pl.ds(pl.multiple_of(k * tok + s * rb, rb), rb)
            XT[:, rows] = X[rows, :].T
            return carry

        lax.fori_loop(0, tok // rb, transpose_rows, 0)
    mb = min(64, tok)
    for k in range(n_micro):
        dy_copy(k).wait()
        n_valid = len_ref[k, 0]

        def mask_rows(s, carry, k=k, n_valid=n_valid):
            rows = pl.ds(pl.multiple_of(k * tok + s * mb, mb), mb)
            v = DY[rows, :].astype(F32)
            at = s * mb + lax.broadcasted_iota(jnp.int32, v.shape, 0)
            DY[rows, :] = jnp.where(at < n_valid, v, 0.0).astype(BF16)
            return carry

        lax.fori_loop(0, tok // mb, mask_rows, 0)

    cb = min(512, n_tok // 2)

    def hidden_block(t, half):
        slot = t % W_SLOTS
        if half == 0:
            wait_w(t)
        for s in range(n_tok // 2 // cb):
            rows = pl.ds(half * (n_tok // 2) + s * cb, cb)
            h = jnp.dot(X[rows, :], WU[slot], preferred_element_type=F32).astype(BF16).astype(F32)
            da = lax.dot_general(DY[rows, :], WD[slot], NT_DIMS, preferred_element_type=F32)
            a, slope = gelu_and_slope(h)
            AT[:, rows] = a.astype(BF16).T
            DH[rows, :] = (da * slope).astype(BF16)
        if half == 0:
            @pl.when(t + 2 < n_ticks)
            def _():
                @pl.when(t + 2 >= W_SLOTS)
                def _():
                    pl.semaphore_wait(w_credit, 1)
                start_w(t + 2)
        else:
            @pl.when(t + W_SLOTS < n_ticks)
            def _():
                pl.semaphore_signal(w_credit, inc=1, device_id=dev(rep, mate), device_id_type=MESH_ID)

    def pair_copy(t, up):
        slot = t % P_SLOTS
        if up:
            src, dst, item = SU.at[pl.ds(pl.multiple_of(mate * 512, 512), 512)], RU.at[slot], 2 * t
        else:
            src, dst, item = SD.at[pl.ds(pl.multiple_of(mate * 128, 128), 128)], RD.at[slot], 2 * t + 1
        return pltpu.make_async_remote_copy(
            src, dst, p_send.at[0 if up else 1], p_recv.at[item], device_id=dev(rep, mate), device_id_type=MESH_ID)

    def up_block(t):
        for s in range(2):
            rows = pl.ds(s * 512, 512)
            SU[rows, :] = jnp.dot(XT[rows, :], DH[...], preferred_element_type=F32)

        @pl.when(t >= P_SLOTS)
        def _():
            pl.semaphore_wait(ru_credit, 1)
        pair_copy(t, True).start()

    def down_block(t):
        for s in range(2):
            cols = pl.ds(s * 512, 512)
            SD[:, cols] = jnp.dot(AT[...], DY[:, cols], preferred_element_type=F32)

        @pl.when(t >= P_SLOTS)
        def _():
            pl.semaphore_wait(rd_credit, 1)
        pair_copy(t, False).start()

    def send(sent, src, dst, recv, to):
        pltpu.make_async_remote_copy(
            src, dst, sent, recv, device_id=dev(to, me), device_id_type=MESH_ID).start()

    def pair_stage(item, up):
        t = item // 2
        copy = pair_copy(t, up)
        copy.wait_recv()
        g0 = item * (2 * ROWS)
        slot = t % P_SLOTS
        if up:
            own = pl.ds(pl.multiple_of(me * 512, 512), 512)
            for h in range(2):
                cols = pl.ds(h * 128, 128)
                G[pl.ds(pl.multiple_of(g0 + h * ROWS, 8), ROWS), :] = SU[own, cols] + RU[slot, :, cols]
        else:
            own = pl.ds(pl.multiple_of(me * 128, 128), 128)
            for s in range(8):
                cols = pl.ds(s * 128, 128)
                G[pl.ds(pl.multiple_of(g0 + s * 128, 8), 128), :] = SD[own, cols] + RD[slot, :, cols]
        copy.wait_send()

        @pl.when(t + P_SLOTS < n_ticks)
        def _():
            pl.semaphore_signal(ru_credit if up else rd_credit, inc=1, device_id=dev(rep, mate), device_id_type=MESH_ID)
        rs_a(item, 0)

    def rs_a(item, p):
        stride, c = axis_of(item, p)
        m, off, b = PH_ROWS[p], PH_OFF[p], base_of(item, p)
        sent = (send0 if p == 0 else out_send).at[item]
        for h, d in ((0, 1), (1, -1)):
            send(sent, g_rows(item, h, b + (c + 2) % RING * m, m), r_rows(item, h, off, m), rs1.at[item * 3 + p], neighbour(stride, c, d))
        for h, d in ((0, 1), (1, -1)):
            send(sent, g_rows(item, h, b + (c - d + RING) % RING * m, m), r_rows(item, h, off + m, m), rs2.at[item * 3 + p], neighbour(stride, c, -d))

    def rs_b(item, p):
        stride, c = axis_of(item, p)
        m, off, b = PH_ROWS[p], PH_OFF[p], base_of(item, p)
        wait_rows(rs1.at[item * 3 + p], 2 * m)
        for h, d in ((0, 1), (1, -1)):
            g = g_rows(item, h, b + (c + d + RING) % RING * m, m)
            g[...] = g[...] + r_rows(item, h, off, m)[...]
            send((send0 if p == 0 else out_send).at[item], g, r_rows(item, h, off + 2 * m, m), rs2.at[item * 3 + p], neighbour(stride, c, d))

    def rs_c(item, p):
        stride, c = axis_of(item, p)
        m, off, b = PH_ROWS[p], PH_OFF[p], base_of(item, p)
        wait_rows(rs2.at[item * 3 + p], 4 * m)
        for h in range(2):
            g = g_rows(item, h, b + c * m, m)
            out = e_rows(item, h, b + c * m - base_of(item, 1), m) if p == 2 else g
            out[...] = g[...] + (r_rows(item, h, off + m, m)[...] + r_rows(item, h, off + 2 * m, m)[...])
        if p < 2:
            rs_a(item, p + 1)
        else:
            ag_a(item, 2)
        if p == 1:
            wait_rows(send0.at[item], 6 * PH_ROWS[0])
            stride, c = axis_of(item, 0)
            for d in (1, -1):
                pl.semaphore_signal(g_free.at[item], inc=1, device_id=dev(neighbour(stride, c, d), me), device_id_type=MESH_ID)

    def ag_part(item, h, p, q):
        m = PH_ROWS[p]
        if p == 0:
            return g_rows(item, h, q * m, m)
        return e_rows(item, h, base_of(item, p) - base_of(item, 1) + q * m, m)

    def ag_a(item, p):
        stride, c = axis_of(item, p)
        if p == 0:
            pl.semaphore_wait(g_free.at[item], 2)
        for recv, sign in ((ag1, 1), (ag2, -1)):
            for h, d in ((0, 1), (1, -1)):
                part = ag_part(item, h, p, c)
                src = e_rows(item, h, 0, PH_ROWS[0]) if p == 0 else part
                send(out_send.at[item], src, part, recv.at[item * 3 + p], neighbour(stride, c, sign * d))

    def ag_b(item, p):
        stride, c = axis_of(item, p)
        wait_rows(ag1.at[item * 3 + p], 2 * PH_ROWS[p])
        for h, d in ((0, 1), (1, -1)):
            part = ag_part(item, h, p, (c - d + RING) % RING)
            send(out_send.at[item], part, part, ag2.at[item * 3 + p], neighbour(stride, c, d))

    def out_copies(item, up):
        t = item // 2
        c = axis_of(item, 0)[1]
        lo = pl.multiple_of(t * 128, 128)
        hi = pl.multiple_of(n_ticks * 128 + t * 128, 128)
        copies = []
        for h in range(2):
            for k in range(RING):
                q = (c + k) % RING
                src = e_rows(item, h, 0, 128) if k == 0 else g_rows(item, h, q * 128, 128)
                if up:
                    dst = gu_hbm.at[0, pl.ds(pl.multiple_of(q * 128, 128), 128), pl.ds(hi if h else lo, 128)]
                else:
                    dst = gd_hbm.at[0, pl.ds(lo, 128), pl.ds(pl.multiple_of(h * 512 + q * 128, 128), 128)]
                copies.append(pltpu.make_async_copy(src, dst, out_sem.at[item]))
        return copies

    def ag_c(item, p, up):
        wait_rows(ag2.at[item * 3 + p], 4 * PH_ROWS[p])
        if p > 0:
            ag_a(item, p - 1)
        else:
            for copy in out_copies(item, up):
                copy.start()

    def finish(item):
        wait_rows(out_sem.at[item], 2 * ROWS)
        wait_rows(out_send.at[item], 4 * R_ROWS - 6 * PH_ROWS[0])

    def stage(name, item, up):
        if name == "pair":
            pair_stage(item, up)
        elif name == "done":
            finish(item)
        else:
            kind, p, part = name[:2], int(name[2]), name[3]
            if kind == "rs":
                (rs_b if part == "b" else rs_c)(item, p)
            elif part == "b":
                ag_b(item, p)
            else:
                ag_c(item, p, up)

    by_kind = ("pair", "ag0c")

    def step(u, carry):
        t = u // 4
        block = u % 4
        live = t < n_ticks
        pl.when(live & (block == 0))(lambda: hidden_block(t, 0))
        pl.when(live & (block == 1))(lambda: hidden_block(t, 1))
        pl.when(live & (block == 2))(lambda: up_block(t))
        pl.when(live & (block == 3))(lambda: down_block(t))
        for name, lag in SCHEDULE:
            v = u - lag + 4
            vt, vb = v // 4 - 1, v % 4
            item = 2 * vt + vb - 2
            inside = (vt >= 0) & (vt < n_ticks) & (vb >= 2)
            if name in by_kind:
                pl.when(inside & (vb == 2))(functools.partial(stage, name, item, True))
                pl.when(inside & (vb == 3))(functools.partial(stage, name, item, False))
            else:
                pl.when(inside)(functools.partial(stage, name, item, None))
        return carry

    lax.fori_loop(0, 4 * n_ticks + SCHEDULE[-1][1], step, 0)


def solution(mesh):
    tok_spec = P(None, ("model", "replica", "fsdp"), None)
    len_spec = P(None, ("model", "replica", "fsdp"))
    w_spec = P(None, ("model", "fsdp"), None)

    def device_grads(x_in, dy_out, lengths, w_up, w_down):
        n_micro, tok, d = x_in.shape
        n_tok = n_micro * tok
        d_ff = w_up.shape[2]
        n_ticks = d_ff // FC
        n_items = 2 * n_ticks
        any_spec = pl.BlockSpec(memory_space=pl.ANY)
        dma = pltpu.SemaphoreType.DMA
        return pl.pallas_call(
            functools.partial(kernel, n_ticks, n_tok, n_micro),
            out_shape=(
                jax.ShapeDtypeStruct(w_up.shape, F32),
                jax.ShapeDtypeStruct(w_down.shape, F32),
            ),
            in_specs=[any_spec, any_spec, pl.BlockSpec(memory_space=pltpu.SMEM), any_spec, any_spec],
            out_specs=(any_spec, any_spec),
            scratch_shapes=[
                pltpu.VMEM((n_tok, d), BF16),
                pltpu.VMEM((n_tok, d), BF16),
                pltpu.VMEM((d, n_tok), BF16),
                pltpu.VMEM((W_SLOTS, d, FC), BF16),
                pltpu.VMEM((W_SLOTS, FC, d), BF16),
                pltpu.VMEM((FC, n_tok), BF16),
                pltpu.VMEM((n_tok, FC), BF16),
                pltpu.VMEM((d, FC), F32),
                pltpu.VMEM((FC, d), F32),
                pltpu.VMEM((P_SLOTS, d // 2, FC), F32),
                pltpu.VMEM((P_SLOTS, FC // 2, d), F32),
                pltpu.VMEM((n_items * 2 * ROWS, 128), F32),
                pltpu.VMEM((n_items * 2 * R_ROWS, 128), F32),
                pltpu.VMEM((n_items * 2 * PH_ROWS[0], 128), F32),
                dma((2 * n_micro,)),
                dma((W_SLOTS,)),
                dma((W_SLOTS,)),
                dma((W_SLOTS,)),
                dma((2,)),
                dma((n_items,)),
                dma((3 * n_items,)),
                dma((3 * n_items,)),
                dma((3 * n_items,)),
                dma((3 * n_items,)),
                dma((n_items,)),
                dma((n_items,)),
                dma((n_items,)),
                pltpu.SemaphoreType.REGULAR((n_items,)),
                pltpu.SemaphoreType.REGULAR,
                pltpu.SemaphoreType.REGULAR,
                pltpu.SemaphoreType.REGULAR,
            ],
            compiler_params=pltpu.CompilerParams(
                collective_id=0, has_side_effects=True, vmem_limit_bytes=67043328),
            name="grads",
        )(x_in, dy_out, lengths, w_up, w_down)

    return jax.shard_map(device_grads, mesh=mesh, in_specs=(tok_spec, tok_spec, len_spec, w_spec, w_spec), out_specs=(w_spec, w_spec), check_vma=False)
```

```python
import functools

import jax
import jax.numpy as jnp
from jax import lax
from jax.experimental import pallas as pl
from jax.experimental.pallas import tpu as pltpu
from jax.sharding import PartitionSpec as P

F32, BF16 = jnp.float32, jnp.bfloat16
MESH_ID = pl.DeviceIdType.MESH
SQRT_2_OVER_PI = 0.7978845608028654
CUBIC = 0.044715
NT_DIMS = (((1,), (1,)), ((), ()))

FC = 256
RING = 4
SUBS = 4
PH_ROWS = (128, 32, 8)
PH_OFF = (0, 384, 480)
R_ROWS = 504
W_SLOTS = 3
P_SLOTS = 2
STAGES = ("pair", "rs0b", "rs0c", "rs1b", "rs1c", "rs2b", "rs2c", "ag2b", "ag2c", "ag1b", "ag1c", "ag0b", "ag0c")

TABLE = (
    (),
    (),
    ((0, 0),),
    (),
    ((0, 1), (1, 0),),
    (),
    ((0, 2), (1, 1),),
    ((2, 0),),
    ((0, 3), (3, 0), (1, 2),),
    ((2, 1),),
    ((0, 4), (4, 0), (1, 3),),
    ((3, 1), (2, 2),),
    ((0, 5), (5, 0), (3, 2), (1, 4),),
    ((4, 1), (2, 3),),
    ((0, 6), (6, 0), (5, 1), (4, 2), (3, 3), (1, 5),),
    ((2, 4),),
    ((0, 7), (6, 1), (5, 2), (4, 3), (1, 6), (7, 0),),
    ((3, 4), (2, 5),),
    ((0, 8), (6, 2), (5, 3), (1, 7), (3, 5), (7, 1),),
    ((4, 4), (2, 6), (8, 0),),
    ((0, 9), (6, 3), (5, 4), (1, 8), (3, 6), (8, 1), (7, 2),),
    ((4, 5), (2, 7), (9, 0),),
    ((0, 10), (6, 4), (4, 6), (1, 9), (7, 3),),
    ((5, 5), (3, 7), (2, 8), (10, 0), (9, 1), (8, 2),),
    ((0, 11), (5, 6), (3, 8), (1, 10), (7, 4),),
    ((6, 5), (4, 7), (2, 9), (11, 0), (8, 3),),
    ((0, 12), (6, 6), (4, 8), (1, 11), (10, 1), (9, 2),),
    ((5, 7), (3, 9), (2, 10), (12, 0), (9, 3), (8, 4), (7, 5),),
    ((0, 13), (5, 8), (1, 12), (7, 6),),
    ((6, 7), (4, 9), (3, 10), (2, 11), (11, 1), (10, 2), (9, 4),),
    ((0, 14), (1, 13), (10, 3), (8, 5),),
    ((6, 8), (5, 9), (4, 10), (3, 11), (2, 12), (8, 6), (7, 7),),
    ((12, 1), (11, 2), (10, 4), (0, 15), (1, 14), (2, 13), (11, 3), (5, 10), (9, 5), (7, 8), (6, 9), (3, 12), (4, 11), (9, 6), (8, 7), (12, 2), (11, 4), (1, 15), (2, 14), (3, 13), (12, 3), (6, 10), (10, 5), (8, 8), (7, 9), (4, 12), (5, 11), (9, 7), (10, 6), (12, 4), (2, 15), (3, 14), (4, 13), (7, 10), (11, 5), (9, 8), (8, 9), (5, 12), (6, 11), (10, 7), (11, 6), (3, 15), (4, 14), (5, 13), (8, 10), (9, 9), (12, 5), (10, 8), (6, 12), (7, 11), (11, 7), (4, 15), (12, 6), (5, 14), (6, 13), (9, 10), (10, 9), (11, 8), (8, 11), (7, 12), (12, 7), (7, 13), (5, 15), (6, 14), (10, 10), (11, 9), (12, 8), (8, 12), (6, 15), (9, 11), (8, 13), (7, 14), (11, 10), (12, 9), (9, 12), (7, 15), (10, 11), (9, 13), (8, 14), (12, 10), (10, 12), (8, 15), (11, 11), (10, 13), (9, 14), (11, 12), (9, 15), (12, 11), (11, 13), (10, 14), (10, 15), (12, 12), (12, 13), (11, 14), (11, 15), (12, 14), (12, 15),),
)


def program(n_ticks):
    if n_ticks == 16 and TABLE:
        return TABLE
    slots = [[] for _ in range(2 * n_ticks + 1)]
    for t in range(n_ticks):
        for s in range(len(STAGES)):
            slots[min(2 * t + 2 + s, 2 * n_ticks)].append((s, t))
    slots[-1].sort()
    return slots


def gelu_and_slope(u):
    u2 = u * u
    half = 0.5 + 0.5 * jnp.tanh(u * (SQRT_2_OVER_PI + (CUBIC * SQRT_2_OVER_PI) * u2))
    a = u * half
    return a, half + (a * (1.0 - half)) * (2.0 * SQRT_2_OVER_PI + (6.0 * CUBIC * SQRT_2_OVER_PI) * u2)


def subs_of(t):
    return [(g, g % 3, 1 if g // 3 % 2 == 0 else -1) for g in range(SUBS * t, SUBS * t + SUBS)]


def kernel(n_ticks, n_tok, n_micro,
           x_hbm, dy_hbm, len_ref, wu_hbm, wd_hbm, gu_hbm, gd_hbm,
           X, DY, XT, WU, WD, AT, DH, SU, SD, RU, RD, GU, GD, R, E,
           in_sem, w_local, w_send, w_recv, p_send, p_recv, rs1, rs2, ag1, ag2, send0, send1, out_send, out_sem,
           g_free, w_credit, r_credit):
    tok = n_tok // n_micro
    half_ff = n_ticks * 128
    rep = lax.axis_index("replica")
    me = lax.axis_index("fsdp")
    mate = 1 - me

    def dev(replica, core):
        return (0, replica, core)

    strides = [RING**a for a in range(3)]
    coord = [(rep // s) % RING for s in strides]
    quarter = [[coord[a]] + [(coord[a] + k) % RING for k in range(1, RING)] for a in range(3)]
    near = [{d: rep + strides[a] * (quarter[a][d % RING] - coord[a]) for d in (1, -1)} for a in range(3)]

    def at_axis(color, phase):
        return (color + phase) % 3

    def row_in_quarter(color, phase):
        row = 0
        for p in range(1, phase):
            row = row + coord[at_axis(color, p)] * PH_ROWS[p]
        return row

    def g_part(g, q, row, n):
        t, s = g // SUBS, g % SUBS
        if s < 2:
            start = q * 128 + row
            return GU.at[pl.ds(pl.multiple_of(start, 8), n), pl.ds(s * half_ff + t * 128, 128)]
        start = t * 128 + row
        if not isinstance(start, int):
            start = pl.multiple_of(start, 8)
        return GD.at[pl.ds(start, n), pl.ds(pl.multiple_of((s - 2) * 512 + q * 128, 128), 128)]

    def r_part(g, start, n):
        return R.at[pl.ds(g * R_ROWS + start, n)]

    def e_part(g, row, n):
        start = g * PH_ROWS[0] + row
        if not isinstance(start, int):
            start = pl.multiple_of(start, 8)
        return E.at[pl.ds(start, n)]

    def wait_rows(sem, n):
        ref = R.at[pl.ds(0, n)]
        pltpu.make_async_copy(ref, ref, sem).wait()

    barrier = pltpu.get_barrier_semaphore()
    for a in range(3):
        for d in (1, -1):
            pl.semaphore_signal(barrier, inc=1, device_id=dev(near[a][d], me), device_id_type=MESH_ID)
    pl.semaphore_signal(barrier, inc=1, device_id=dev(rep, mate), device_id_type=MESH_ID)

    def x_copy(k):
        return pltpu.make_async_copy(x_hbm.at[k], X.at[pl.ds(k * tok, tok)], in_sem.at[k])

    def dy_copy(k):
        return pltpu.make_async_copy(dy_hbm.at[k], DY.at[pl.ds(k * tok, tok)], in_sem.at[n_micro + k])

    for k in range(n_micro):
        x_copy(k).start()
    for k in range(n_micro):
        dy_copy(k).start()

    def start_w(t):
        slot = t % W_SLOTS
        lo = pl.multiple_of(t * 128, 128)
        hi = pl.multiple_of(half_ff + t * 128, 128)
        up_rows = pl.ds(pl.multiple_of(me * 512, 512), 512)
        down_rows = pl.ds(pl.multiple_of(me * 128, 128), 128)
        pairs = (
            (wu_hbm.at[0, :, pl.ds(lo, 128)], WU.at[slot, up_rows, pl.ds(0, 128)]),
            (wu_hbm.at[0, :, pl.ds(hi, 128)], WU.at[slot, up_rows, pl.ds(128, 128)]),
            (wd_hbm.at[0, pl.ds(lo, 128), :], WD.at[slot, down_rows, :]),
        )
        for s, d in pairs:
            pltpu.make_async_remote_copy(
                s, d, w_send.at[slot], w_recv.at[slot], device_id=dev(rep, mate), device_id_type=MESH_ID).start()
        for s, d in pairs:
            pltpu.make_async_copy(s, d, w_local.at[slot]).start()

    def wait_w(t):
        slot = t % W_SLOTS
        ref = WU.at[slot]
        for sem in (w_local, w_recv, w_send):
            pltpu.make_async_copy(ref, ref, sem.at[slot]).wait()

    pl.semaphore_wait(barrier, 7)
    start_w(0)
    if n_ticks > 1:
        start_w(1)

    rb = min(256, tok)
    for k in range(n_micro):
        x_copy(k).wait()

        def transpose_rows(s, carry, k=k):
            rows = pl.ds(pl.multiple_of(k * tok + s * rb, rb), rb)
            XT[:, rows] = X[rows, :].T
            return carry

        lax.fori_loop(0, tok // rb, transpose_rows, 0)
    mb = min(64, tok)
    for k in range(n_micro):
        dy_copy(k).wait()
        n_valid = len_ref[k]

        def mask_rows(s, carry, k=k, n_valid=n_valid):
            rows = pl.ds(pl.multiple_of(k * tok + s * mb, mb), mb)
            v = DY[rows, :].astype(F32)
            at = s * mb + lax.broadcasted_iota(jnp.int32, v.shape, 0)
            DY[rows, :] = jnp.where(at < n_valid, v, 0.0).astype(BF16)
            return carry

        lax.fori_loop(0, tok // mb, mask_rows, 0)

    cb = min(512, n_tok)

    def hidden_block(t):
        slot = t % W_SLOTS
        wait_w(t)
        for s in range(n_tok // cb):
            rows = pl.ds(s * cb, cb)
            h = jnp.dot(X[rows, :], WU[slot], preferred_element_type=F32).astype(BF16).astype(F32)
            da = lax.dot_general(DY[rows, :], WD[slot], NT_DIMS, preferred_element_type=F32)
            a, slope = gelu_and_slope(h)
            AT[:, rows] = a.astype(BF16).T
            DH[rows, :] = (da * slope).astype(BF16)

        @pl.when(t + W_SLOTS < n_ticks)
        def _():
            pl.semaphore_signal(w_credit, inc=1, device_id=dev(rep, mate), device_id_type=MESH_ID)

    def pair_copies(t):
        slot = t % P_SLOTS
        other_up = pl.ds(pl.multiple_of(mate * 512, 512), 512)
        other_down = pl.ds(pl.multiple_of(mate * 128, 128), 128)
        return [
            pltpu.make_async_remote_copy(
                src, dst, p_send.at[slot], p_recv.at[slot], device_id=dev(rep, mate), device_id_type=MESH_ID)
            for src, dst in ((SU.at[other_up], RU.at[slot]), (SD.at[other_down], RD.at[slot]))
        ]

    def grad_block(t):
        @pl.when(t >= P_SLOTS)
        def _():
            pl.semaphore_wait(r_credit, 1)

        @pl.when((t + 2 < n_ticks) & (t + 2 >= W_SLOTS))
        def _():
            pl.semaphore_wait(w_credit, 1)

        @pl.when(t + 2 < n_ticks)
        def _():
            start_w(t + 2)

        for s in range(2):
            rows = pl.ds(s * 512, 512)
            SU[rows, :] = jnp.dot(XT[rows, :], DH[...], preferred_element_type=F32)
        for s in range(2):
            cols = pl.ds(s * 512, 512)
            SD[:, cols] = jnp.dot(AT[...], DY[:, cols], preferred_element_type=F32)
        for copy in pair_copies(t):
            copy.start()

    def send(sent, src, dst, recv, to):
        pltpu.make_async_remote_copy(
            src, dst, sent, recv, device_id=dev(to, me), device_id_type=MESH_ID).start()

    def pair_stage(t):
        slot = t % P_SLOTS
        pltpu.make_async_copy(SU, SU, p_recv.at[slot]).wait()
        own = pl.ds(pl.multiple_of(me * 512, 512), 512)
        for s in range(2):
            cols = pl.ds(s * 128, 128)
            GU[:, pl.ds(s * half_ff + t * 128, 128)] = SU[own, cols] + RU[slot, :, cols]
        own = pl.ds(pl.multiple_of(me * 128, 128), 128)
        GD[pl.ds(t * 128, 128), :] = SD[own, :] + RD[slot]
        pltpu.make_async_copy(SU, SU, p_send.at[slot]).wait()
        if t + P_SLOTS < n_ticks:
            pl.semaphore_signal(r_credit, inc=1, device_id=dev(rep, mate), device_id_type=MESH_ID)
        rs_a(t, 0)

    def rs_a(t, p):
        sent = (send0 if p == 0 else send1).at[t]
        m, off = PH_ROWS[p], PH_OFF[p]
        for relay in (True, False):
            for g, color, d in subs_of(t):
                a = at_axis(color, p)
                q = quarter[a][2 if relay else -d % RING]
                src = g_part(g, q, 0, m) if p == 0 else g_part(g, coord[color], row_in_quarter(color, p) + q * m, m)
                if relay:
                    send(sent, src, r_part(g, off, m), rs1.at[t * 3 + p], near[a][d])
                else:
                    send(sent, src, r_part(g, off + m, m), rs2.at[t * 3 + p], near[a][-d])

    def rs_b(t, p):
        sent = (send0 if p == 0 else send1).at[t]
        m, off = PH_ROWS[p], PH_OFF[p]
        wait_rows(rs1.at[t * 3 + p], SUBS * m)
        for g, color, d in subs_of(t):
            a = at_axis(color, p)
            q = quarter[a][d % RING]
            part = g_part(g, q, 0, m) if p == 0 else g_part(g, coord[color], row_in_quarter(color, p) + q * m, m)
            part[...] = part[...] + r_part(g, off, m)[...]
            send(sent, part, r_part(g, off + 2 * m, m), rs2.at[t * 3 + p], near[a][d])

    def rs_c(t, p):
        m, off = PH_ROWS[p], PH_OFF[p]
        wait_rows(rs2.at[t * 3 + p], 2 * SUBS * m)
        for g, color, d in subs_of(t):
            q = coord[at_axis(color, p)]
            row = 0 if p == 0 else row_in_quarter(color, p) + q * m
            part = g_part(g, coord[color], row, m)
            out = e_part(g, row, m) if p == 2 else part
            out[...] = part[...] + (r_part(g, off + m, m)[...] + r_part(g, off + 2 * m, m)[...])
        if p < 2:
            rs_a(t, p + 1)
        else:
            ag_a(t, 2)
        if p == 1:
            wait_rows(send0.at[t], 3 * SUBS * PH_ROWS[0])
            for a in sorted({color for _, color, _ in subs_of(t)}):
                for d in (1, -1):
                    pl.semaphore_signal(g_free.at[t], inc=1, device_id=dev(near[a][d], me), device_id_type=MESH_ID)

    def ag_part(g, color, p, q):
        if p == 0:
            return g_part(g, q, 0, PH_ROWS[0])
        return e_part(g, row_in_quarter(color, p) + q * PH_ROWS[p], PH_ROWS[p])

    def ag_a(t, p):
        if p == 0:
            pl.semaphore_wait(g_free.at[t], 2 * len({color for _, color, _ in subs_of(t)}))
        for recv, sign in ((ag1, 1), (ag2, -1)):
            for g, color, d in subs_of(t):
                a = at_axis(color, p)
                part = ag_part(g, color, p, coord[a])
                src = e_part(g, 0, PH_ROWS[0]) if p == 0 else part
                send(out_send.at[t], src, part, recv.at[t * 3 + p], near[a][sign * d])
        if p == 0:
            wait_rows(send1.at[t], 3 * SUBS * (PH_ROWS[1] + PH_ROWS[2]))
            for g, color, d in subs_of(t):
                g_part(g, coord[color], 0, PH_ROWS[0])[...] = e_part(g, 0, PH_ROWS[0])[...]

    def ag_b(t, p):
        wait_rows(ag1.at[t * 3 + p], SUBS * PH_ROWS[p])
        for g, color, d in subs_of(t):
            a = at_axis(color, p)
            part = ag_part(g, color, p, quarter[a][-d % RING])
            send(out_send.at[t], part, part, ag2.at[t * 3 + p], near[a][d])

    def out_copies(t):
        copies = []
        for s in range(2):
            cols = pl.ds(s * half_ff + t * 128, 128)
            copies.append(pltpu.make_async_copy(GU.at[:, cols], gu_hbm.at[0, :, cols], out_sem.at[t]))
        rows = pl.ds(t * 128, 128)
        copies.append(pltpu.make_async_copy(GD.at[rows], gd_hbm.at[0, rows], out_sem.at[t]))
        return copies

    def ag_c(t, p):
        wait_rows(ag2.at[t * 3 + p], 2 * SUBS * PH_ROWS[p])
        if p > 0:
            ag_a(t, p - 1)
        else:
            for copy in out_copies(t):
                copy.start()

    def run(ops):
        for s, t in ops:
            name = STAGES[s]
            with jax.named_scope(name):
                if name == "pair":
                    pair_stage(t)
                else:
                    p = int(name[2])
                    {"rsb": rs_b, "rsc": rs_c, "agb": ag_b, "agc": ag_c}[name[:2] + name[3]](t, p)

    slots = program(n_ticks)

    def pick(t, block, lo, hi):
        lists = [slots[2 * k + block] for k in range(lo, hi)]
        if not any(lists):
            return
        if hi - lo == 1:
            run(lists[0])
            return
        mid = (lo + hi) // 2
        pl.when(t < mid)(lambda: pick(t, block, lo, mid))
        pl.when(t >= mid)(lambda: pick(t, block, mid, hi))

    def tick(t, carry):
        with jax.named_scope("hidden"):
            hidden_block(t)
        pick(t, 0, 0, n_ticks)
        with jax.named_scope("grad"):
            grad_block(t)
        pick(t, 1, 0, n_ticks)
        return carry

    lax.fori_loop(0, n_ticks, tick, 0)
    run(slots[2 * n_ticks])
    for t in range(n_ticks):
        wait_rows(out_sem.at[t], SUBS * 512)
        wait_rows(out_send.at[t], SUBS * R_ROWS)


def solution(mesh):
    tok_spec = P(None, ("model", "replica", "fsdp"), None)
    len_spec = P(None, ("model", "replica", "fsdp"))
    w_spec = P(None, ("model", "fsdp"), None)

    def device_grads(x_in, dy_out, lengths, w_up, w_down):
        n_micro, tok, d = x_in.shape
        n_tok = n_micro * tok
        d_ff = w_up.shape[2]
        n_ticks = d_ff // FC
        any_spec = pl.BlockSpec(memory_space=pl.ANY)
        dma = pltpu.SemaphoreType.DMA
        regular = pltpu.SemaphoreType.REGULAR
        return pl.pallas_call(
            functools.partial(kernel, n_ticks, n_tok, n_micro),
            out_shape=(
                jax.ShapeDtypeStruct(w_up.shape, F32),
                jax.ShapeDtypeStruct(w_down.shape, F32),
            ),
            in_specs=[any_spec, any_spec, pl.BlockSpec(memory_space=pltpu.SMEM), any_spec, any_spec],
            out_specs=(any_spec, any_spec),
            scratch_shapes=[
                pltpu.VMEM((n_tok, d), BF16),
                pltpu.VMEM((n_tok, d), BF16),
                pltpu.VMEM((d, n_tok), BF16),
                pltpu.VMEM((W_SLOTS, d, FC), BF16),
                pltpu.VMEM((W_SLOTS, FC, d), BF16),
                pltpu.VMEM((FC, n_tok), BF16),
                pltpu.VMEM((n_tok, FC), BF16),
                pltpu.VMEM((d, FC), F32),
                pltpu.VMEM((FC, d), F32),
                pltpu.VMEM((P_SLOTS, d // 2, FC), F32),
                pltpu.VMEM((P_SLOTS, FC // 2, d), F32),
                pltpu.VMEM((d // 2, d_ff), F32),
                pltpu.VMEM((d_ff // 2, d), F32),
                pltpu.VMEM((n_ticks * SUBS * R_ROWS, 128), F32),
                pltpu.VMEM((n_ticks * SUBS * PH_ROWS[0], 128), F32),
                dma((2 * n_micro,)),
                dma((W_SLOTS,)),
                dma((W_SLOTS,)),
                dma((W_SLOTS,)),
                dma((P_SLOTS,)),
                dma((P_SLOTS,)),
                dma((3 * n_ticks,)),
                dma((3 * n_ticks,)),
                dma((3 * n_ticks,)),
                dma((3 * n_ticks,)),
                dma((n_ticks,)),
                dma((n_ticks,)),
                dma((n_ticks,)),
                dma((n_ticks,)),
                regular((n_ticks,)),
                regular,
                regular,
            ],
            compiler_params=pltpu.CompilerParams(
                collective_id=0, has_side_effects=True, vmem_limit_bytes=67043328),
            name="grads",
        )(x_in, dy_out, lengths.reshape(n_micro), w_up, w_down)

    return jax.shard_map(device_grads, mesh=mesh, in_specs=(tok_spec, tok_spec, len_spec, w_spec, w_spec), out_specs=(w_spec, w_spec), check_vma=False)
```

```python
import functools

import jax
import jax.numpy as jnp
from jax import lax
from jax.experimental import pallas as pl
from jax.experimental.pallas import tpu as pltpu
from jax.sharding import PartitionSpec as P

F32, BF16 = jnp.float32, jnp.bfloat16
MESH_ID = pl.DeviceIdType.MESH
SQRT_2_OVER_PI = 0.7978845608028654
CUBIC = 0.044715
NT_DIMS = (((1,), (1,)), ((), ()))

FC = 256
RING = 4
SUBS = 4
PH_ROWS = (128, 32, 8)
PH_OFF = (0, 384, 480)
R_ROWS = 504
W_SLOTS = 3
P_SLOTS = 2
STAGES = ("pair", "rs0b", "rs0c", "rs1b", "rs1c", "rs2b", "rs2c", "ag2b", "ag2c", "ag1b", "ag1c", "ag0b", "ag0c")

TABLE = (
    (),
    (),
    ((0, 0),),
    (),
    ((1, 0),),
    ((0, 1),),
    ((2, 0),),
    ((0, 2), (1, 1),),
    ((3, 0),),
    ((0, 3), (1, 2),),
    ((2, 1), (4, 0),),
    ((0, 4), (1, 3),),
    ((2, 2), (3, 1), (5, 0),),
    ((0, 5), (1, 4),),
    ((2, 3), (3, 2), (4, 1), (6, 0),),
    ((0, 6), (1, 5),),
    ((2, 4), (3, 3), (4, 2), (5, 1), (7, 0),),
    ((0, 7), (1, 6),),
    ((2, 5), (3, 4), (4, 3), (5, 2), (6, 1), (8, 0),),
    ((0, 8), (1, 7),),
    ((2, 6), (3, 5), (4, 4), (5, 3), (6, 2), (7, 1), (9, 0),),
    ((0, 9), (1, 8),),
    ((2, 7), (3, 6), (4, 5), (5, 4), (6, 3), (7, 2), (8, 1), (10, 0),),
    ((0, 10), (1, 9),),
    ((2, 8), (3, 7), (4, 6), (5, 5), (6, 4), (7, 3), (8, 2), (9, 1),),
    ((0, 11), (1, 10), (11, 0),),
    ((2, 9), (3, 8), (4, 7), (5, 6), (6, 5), (8, 3),),
    ((0, 12), (7, 4), (9, 2), (10, 1),),
    ((1, 11), (2, 10), (3, 9), (4, 8), (5, 7), (12, 0),),
    ((0, 13), (1, 12), (6, 6), (7, 5), (9, 3),),
    ((8, 4), (10, 2),),
    ((0, 14), (2, 11), (1, 13), (3, 10), (4, 9), (5, 8), (6, 7), (11, 1),),
    ((2, 12), (7, 6), (8, 5), (0, 15), (9, 4), (1, 14), (3, 11), (7, 7), (2, 13), (4, 10), (5, 9), (6, 8), (3, 12), (12, 1), (8, 6), (9, 5), (1, 15), (8, 7), (5, 10), (10, 3), (4, 12), (2, 14), (9, 6), (4, 11), (3, 13), (6, 9), (7, 8), (2, 15), (10, 4), (6, 10), (9, 7), (5, 12), (3, 14), (5, 11), (4, 13), (7, 9), (8, 8), (3, 15), (10, 5), (10, 6), (7, 10), (6, 12), (6, 11), (5, 13), (4, 14), (8, 9), (9, 8), (4, 15), (10, 7), (8, 10), (7, 12), (7, 11), (6, 13), (5, 14), (9, 9), (5, 15), (10, 8), (11, 2), (9, 10), (8, 12), (8, 11), (7, 13), (6, 14), (6, 15), (10, 9), (11, 3), (12, 2), (10, 10), (9, 12), (9, 11), (7, 14), (8, 13), (7, 15), (11, 4), (12, 3), (11, 5), (11, 6), (11, 7), (8, 14), (9, 13), (8, 15), (12, 4), (10, 11), (12, 5), (12, 6), (10, 12), (12, 7), (9, 14), (10, 13), (9, 15), (11, 8), (10, 14), (11, 9), (10, 15), (12, 8), (11, 10), (11, 11), (11, 12), (12, 9), (11, 13), (11, 14), (11, 15), (12, 10), (12, 11), (12, 12), (12, 13), (12, 14), (12, 15),),
)
SHAPES = (
    3, 0, 0, 6, 6, 6, 0, 2, 0, 6, 6, 6, 0, 0, 0, 6, 2, 5, 0, 0, 0, 6, 2, 6, 6, 0, 0, 6, 6, 7, 0, 0,
    0, 6, 6, 6, 0, 6, 0, 6, 6, 6, 0, 0, 6, 6, 6, 6, 5, 0, 4, 6, 6, 6, 0, 0, 5, 6, 6, 6, 0, 0, 4, 6,
)


def program(n_ticks):
    if n_ticks == 16 and TABLE:
        return TABLE
    slots = [[] for _ in range(2 * n_ticks + 1)]
    for t in range(n_ticks):
        made = 1 if t == 0 else 2 * t + 2 if t < n_ticks - 1 else 2 * n_ticks - 1
        for s in range(len(STAGES)):
            slots[min(made + 1 + s, 2 * n_ticks)].append((s, t))
    slots[-1].sort()
    return slots


def gelu_and_slope(u):
    u2 = u * u
    half = 0.5 + 0.5 * jnp.tanh(u * (SQRT_2_OVER_PI + (CUBIC * SQRT_2_OVER_PI) * u2))
    a = u * half
    return a, half + (a * (1.0 - half)) * (2.0 * SQRT_2_OVER_PI + (6.0 * CUBIC * SQRT_2_OVER_PI) * u2)


def subs_of(t):
    blocks = []
    for g in range(SUBS * t, SUBS * t + SUBS):
        code, a = SHAPES[g % len(SHAPES)], g % 3
        b, c = ((a + 1) % 3, (a + 2) % 3) if code % 2 == 0 else ((a + 2) % 3, (a + 1) % 3)
        dirs = (1 if g // 3 % 2 == 0 else -1, -1 if code & 2 else 1, -1 if code & 4 else 1)
        blocks.append((g, (a, b, c), dirs))
    return blocks


def kernel(n_ticks, n_tok, n_micro,
           x_hbm, dy_hbm, len_ref, wu_hbm, wd_hbm, GU, GD,
           X, DY, XT, WU, WD, AT, DH, SU, SD, RU, RD, R, E,
           in_sem, w_local, w_send, w_recv, p_send, p_recv, rs1, rs2, ag1, ag2, send0, send1, out_send,
           g_free, w_credit, r_credit):
    tok = n_tok // n_micro
    half_ff = n_ticks * 128
    rep = lax.axis_index("replica")
    me = lax.axis_index("fsdp")
    mate = 1 - me

    def dev(replica, core):
        return (0, replica, core)

    strides = [RING**a for a in range(3)]
    coord = [(rep // s) % RING for s in strides]
    quarter = [[coord[a]] + [(coord[a] + k) % RING for k in range(1, RING)] for a in range(3)]
    near = [{d: rep + strides[a] * (quarter[a][d % RING] - coord[a]) for d in (1, -1)} for a in range(3)]

    def row_in_quarter(axes, phase):
        row = 0
        for p in range(1, phase):
            row = row + coord[axes[p]] * PH_ROWS[p]
        return row

    def g_part(g, q, row, n):
        t, s = g // SUBS, g % SUBS
        if s < 2:
            start = q * 128 + row
            return GU.at[pl.ds(pl.multiple_of(start, 8), n), pl.ds(s * half_ff + t * 128, 128)]
        start = t * 128 + row
        if not isinstance(start, int):
            start = pl.multiple_of(start, 8)
        return GD.at[pl.ds(start, n), pl.ds(pl.multiple_of((s - 2) * 512 + q * 128, 128), 128)]

    def r_part(g, start, n):
        return R.at[pl.ds(g * R_ROWS + start, n)]

    def e_part(g, row, n):
        start = g * PH_ROWS[0] + row
        if not isinstance(start, int):
            start = pl.multiple_of(start, 8)
        return E.at[pl.ds(start, n)]

    def wait_rows(sem, n):
        ref = R.at[pl.ds(0, n)]
        pltpu.make_async_copy(ref, ref, sem).wait()

    barrier = pltpu.get_barrier_semaphore()
    for a in range(3):
        for d in (1, -1):
            pl.semaphore_signal(barrier, inc=1, device_id=dev(near[a][d], me), device_id_type=MESH_ID)
    pl.semaphore_signal(barrier, inc=1, device_id=dev(rep, mate), device_id_type=MESH_ID)

    def x_copy(k):
        return pltpu.make_async_copy(x_hbm.at[k], X.at[pl.ds(k * tok, tok)], in_sem.at[k])

    def dy_copy(k):
        return pltpu.make_async_copy(dy_hbm.at[k], DY.at[pl.ds(k * tok, tok)], in_sem.at[n_micro + k])

    for k in range(n_micro):
        x_copy(k).start()
    for k in range(n_micro):
        dy_copy(k).start()

    def start_w(t):
        slot = t % W_SLOTS
        lo = pl.multiple_of(t * 128, 128)
        hi = pl.multiple_of(half_ff + t * 128, 128)
        up_rows = pl.ds(pl.multiple_of(me * 512, 512), 512)
        down_rows = pl.ds(pl.multiple_of(me * 128, 128), 128)
        pairs = (
            (wu_hbm.at[0, :, pl.ds(lo, 128)], WU.at[slot, up_rows, pl.ds(0, 128)]),
            (wu_hbm.at[0, :, pl.ds(hi, 128)], WU.at[slot, up_rows, pl.ds(128, 128)]),
            (wd_hbm.at[0, pl.ds(lo, 128), :], WD.at[slot, down_rows, :]),
        )
        for s, d in pairs:
            pltpu.make_async_remote_copy(
                s, d, w_send.at[slot], w_recv.at[slot], device_id=dev(rep, mate), device_id_type=MESH_ID).start()
        for s, d in pairs:
            pltpu.make_async_copy(s, d, w_local.at[slot]).start()

    def wait_w(t):
        slot = t % W_SLOTS
        ref = WU.at[slot]
        for sem in (w_local, w_recv, w_send):
            pltpu.make_async_copy(ref, ref, sem.at[slot]).wait()

    with jax.named_scope("entry"):
        pl.semaphore_wait(barrier, 7)
    start_w(0)
    if n_ticks > 1:
        start_w(1)

    rb = min(256, tok)
    for k in range(n_micro):
        with jax.named_scope("xwait"):
            x_copy(k).wait()

        def transpose_rows(s, carry, k=k):
            rows = pl.ds(pl.multiple_of(k * tok + s * rb, rb), rb)
            XT[:, rows] = X[rows, :].T
            return carry

        lax.fori_loop(0, tok // rb, transpose_rows, 0)
    mb = min(64, tok)
    for k in range(n_micro):
        with jax.named_scope("dywait"):
            dy_copy(k).wait()
        n_valid = len_ref[k]

        def mask_rows(s, carry, k=k, n_valid=n_valid):
            rows = pl.ds(pl.multiple_of(k * tok + s * mb, mb), mb)
            v = DY[rows, :].astype(F32)
            at = s * mb + lax.broadcasted_iota(jnp.int32, v.shape, 0)
            DY[rows, :] = jnp.where(at < n_valid, v, 0.0).astype(BF16)
            return carry

        lax.fori_loop(0, tok // mb, mask_rows, 0)

    cb = min(512, n_tok // 2)

    def hidden(t, part):
        slot, buf = t % W_SLOTS, t % 2
        if part != 1:
            with jax.named_scope("wwait"):
                wait_w(t)
        lo, hi = (0, n_tok) if part is None else (part * (n_tok // 2), (part + 1) * (n_tok // 2))
        for at in range(lo, hi, cb):
            rows = pl.ds(at, cb)
            h = jnp.dot(X[rows, :], WU[slot], preferred_element_type=F32).astype(BF16).astype(F32)
            da = lax.dot_general(DY[rows, :], WD[slot], NT_DIMS, preferred_element_type=F32)
            a, slope = gelu_and_slope(h)
            AT[buf, :, rows] = a.astype(BF16).T
            DH[buf, rows, :] = (da * slope).astype(BF16)

    def free_w(t):
        @pl.when(t + W_SLOTS < n_ticks)
        def _():
            pl.semaphore_signal(w_credit, inc=1, device_id=dev(rep, mate), device_id_type=MESH_ID)

    def more_w(t):
        @pl.when((t < n_ticks) & (t >= W_SLOTS))
        def _():
            pl.semaphore_wait(w_credit, 1)

        @pl.when(t < n_ticks)
        def _():
            start_w(t)

    def send_to_mate(t, part):
        slot = t % P_SLOTS
        if part == 0:
            src, dst = SU.at[slot, pl.ds(pl.multiple_of(mate * 512, 512), 512)], RU.at[slot]
        else:
            src, dst = SD.at[slot, pl.ds(pl.multiple_of(mate * 128, 128), 128)], RD.at[slot]
        pltpu.make_async_remote_copy(
            src, dst, p_send.at[slot], p_recv.at[slot], device_id=dev(rep, mate), device_id_type=MESH_ID).start()

    def take_pair_room(t):
        @pl.when(t >= P_SLOTS)
        def _():
            pl.semaphore_wait(r_credit, 1)

    def up(t):
        buf = t % 2
        for s in range(2):
            rows = pl.ds(s * 512, 512)
            SU[buf, rows, :] = jnp.dot(XT[rows, :], DH[buf], preferred_element_type=F32)
        send_to_mate(t, 0)

    def down(t):
        buf = t % 2
        for s in range(2):
            cols = pl.ds(s * 512, 512)
            SD[buf, :, cols] = jnp.dot(AT[buf], DY[:, cols], preferred_element_type=F32)
        send_to_mate(t, 1)

    def send(sent, src, dst, recv, to):
        pltpu.make_async_remote_copy(
            src, dst, sent, recv, device_id=dev(to, me), device_id_type=MESH_ID).start()

    def pair_stage(t):
        slot = t % P_SLOTS
        whole = SU.at[slot]
        pltpu.make_async_copy(whole, whole, p_recv.at[slot]).wait()
        own = pl.ds(pl.multiple_of(me * 512, 512), 512)
        for s in range(2):
            cols = pl.ds(s * 128, 128)
            GU[:, pl.ds(s * half_ff + t * 128, 128)] = SU[slot, own, cols] + RU[slot, :, cols]
        own = pl.ds(pl.multiple_of(me * 128, 128), 128)
        GD[pl.ds(t * 128, 128), :] = SD[slot, own, :] + RD[slot]
        pltpu.make_async_copy(whole, whole, p_send.at[slot]).wait()
        if t + P_SLOTS < n_ticks:
            pl.semaphore_signal(r_credit, inc=1, device_id=dev(rep, mate), device_id_type=MESH_ID)
        rs_a(t, 0)

    def rs_a(t, p):
        sent = (send0 if p == 0 else send1).at[t]
        m, off = PH_ROWS[p], PH_OFF[p]
        for relay in (True, False):
            for g, axes, dirs in subs_of(t):
                a, d = axes[p], dirs[p]
                q = quarter[a][2 if relay else -d % RING]
                src = g_part(g, q, 0, m) if p == 0 else g_part(g, coord[axes[0]], row_in_quarter(axes, p) + q * m, m)
                if relay:
                    send(sent, src, r_part(g, off, m), rs1.at[t * 3 + p], near[a][d])
                else:
                    send(sent, src, r_part(g, off + m, m), rs2.at[t * 3 + p], near[a][-d])

    def rs_b(t, p):
        sent = (send0 if p == 0 else send1).at[t]
        m, off = PH_ROWS[p], PH_OFF[p]
        wait_rows(rs1.at[t * 3 + p], SUBS * m)
        for g, axes, dirs in subs_of(t):
            a, d = axes[p], dirs[p]
            q = quarter[a][d % RING]
            part = g_part(g, q, 0, m) if p == 0 else g_part(g, coord[axes[0]], row_in_quarter(axes, p) + q * m, m)
            part[...] = part[...] + r_part(g, off, m)[...]
            send(sent, part, r_part(g, off + 2 * m, m), rs2.at[t * 3 + p], near[a][d])

    def rs_c(t, p):
        m, off = PH_ROWS[p], PH_OFF[p]
        wait_rows(rs2.at[t * 3 + p], 2 * SUBS * m)
        for g, axes, dirs in subs_of(t):
            row = 0 if p == 0 else row_in_quarter(axes, p) + coord[axes[p]] * m
            part = g_part(g, coord[axes[0]], row, m)
            out = e_part(g, row, m) if p == 2 else part
            out[...] = part[...] + (r_part(g, off + m, m)[...] + r_part(g, off + 2 * m, m)[...])
        if p < 2:
            rs_a(t, p + 1)
        else:
            ag_a(t, 2)
        if p == 1:
            wait_rows(send0.at[t], 3 * SUBS * PH_ROWS[0])
            for a in sorted({axes[0] for _, axes, _ in subs_of(t)}):
                for d in (1, -1):
                    pl.semaphore_signal(g_free.at[t], inc=1, device_id=dev(near[a][d], me), device_id_type=MESH_ID)

    def ag_part(g, axes, p, q):
        if p == 0:
            return g_part(g, q, 0, PH_ROWS[0])
        return e_part(g, row_in_quarter(axes, p) + q * PH_ROWS[p], PH_ROWS[p])

    def ag_a(t, p):
        if p == 0:
            pl.semaphore_wait(g_free.at[t], 2 * len({axes[0] for _, axes, _ in subs_of(t)}))
        for recv, sign in ((ag1, 1), (ag2, -1)):
            for g, axes, dirs in subs_of(t):
                a, d = axes[p], dirs[p]
                part = ag_part(g, axes, p, coord[a])
                src = e_part(g, 0, PH_ROWS[0]) if p == 0 else part
                send(out_send.at[t], src, part, recv.at[t * 3 + p], near[a][sign * d])
        if p == 0:
            wait_rows(send1.at[t], 3 * SUBS * (PH_ROWS[1] + PH_ROWS[2]))
            for g, axes, dirs in subs_of(t):
                g_part(g, coord[axes[0]], 0, PH_ROWS[0])[...] = e_part(g, 0, PH_ROWS[0])[...]

    def ag_b(t, p):
        wait_rows(ag1.at[t * 3 + p], SUBS * PH_ROWS[p])
        for g, axes, dirs in subs_of(t):
            a, d = axes[p], dirs[p]
            part = ag_part(g, axes, p, quarter[a][-d % RING])
            send(out_send.at[t], part, part, ag2.at[t * 3 + p], near[a][d])

    def ag_c(t, p):
        wait_rows(ag2.at[t * 3 + p], 2 * SUBS * PH_ROWS[p])
        if p > 0:
            ag_a(t, p - 1)

    def run(ops):
        for s, t in ops:
            name = STAGES[s]
            with jax.named_scope(name):
                if name == "pair":
                    pair_stage(t)
                else:
                    p = int(name[2])
                    {"rsb": rs_b, "rsc": rs_c, "agb": ag_b, "agc": ag_c}[name[:2] + name[3]](t, p)

    slots = program(n_ticks)

    def pick(t, first, lo, hi):
        lists = [slots[first(k)] for k in range(lo, hi)]
        if not any(lists):
            return
        if hi - lo == 1:
            run(lists[0])
            return
        mid = (lo + hi) // 2
        pl.when(t < mid)(lambda: pick(t, first, lo, mid))
        pl.when(t >= mid)(lambda: pick(t, first, mid, hi))

    def opening(t, carry):
        with jax.named_scope("hidden"):
            hidden(t, None)
            free_w(t)

        @pl.when(t == 0)
        def _():
            more_w(2)
            with jax.named_scope("grad"):
                up(0)
                down(0)
            run(slots[1])
        return carry

    lax.fori_loop(0, 2, opening, 0)
    run(slots[2])

    def tick(t, carry):
        more_w(t + 1)
        take_pair_room(t - 1)
        with jax.named_scope("blocka"):
            hidden(t, 0)
            up(t - 1)
        pick(t, lambda k: 2 * k - 1, 2, n_ticks)
        with jax.named_scope("blockb"):
            hidden(t, 1)
            free_w(t)
            down(t - 1)
        pick(t, lambda k: 2 * k, 2, n_ticks)
        return carry

    lax.fori_loop(2, n_ticks, tick, 0)
    take_pair_room(n_ticks - 1)
    with jax.named_scope("grad"):
        up(n_ticks - 1)
        down(n_ticks - 1)
    run(slots[2 * n_ticks - 1])
    run(slots[2 * n_ticks])
    for t in range(n_ticks):
        wait_rows(out_send.at[t], SUBS * R_ROWS)


def solution(mesh):
    tok_spec = P(None, ("model", "replica", "fsdp"), None)
    len_spec = P(None, ("model", "replica", "fsdp"))
    w_spec = P(None, ("model", "fsdp"), None)

    def device_grads(x_in, dy_out, lengths, w_up, w_down):
        n_micro, tok, d = x_in.shape
        n_tok = n_micro * tok
        d_ff = w_up.shape[2]
        n_ticks = d_ff // FC
        any_spec = pl.BlockSpec(memory_space=pl.ANY)
        dma = pltpu.SemaphoreType.DMA
        regular = pltpu.SemaphoreType.REGULAR
        gu, gd = pl.pallas_call(
            functools.partial(kernel, n_ticks, n_tok, n_micro),
            out_shape=(
                pltpu.VMEM((d // 2, d_ff), F32),
                pltpu.VMEM((d_ff // 2, d), F32),
            ),
            in_specs=[any_spec, any_spec, pl.BlockSpec(memory_space=pltpu.SMEM), any_spec, any_spec],
            out_specs=(pl.BlockSpec(memory_space=pltpu.VMEM),) * 2,
            scratch_shapes=[
                pltpu.VMEM((n_tok, d), BF16),
                pltpu.VMEM((n_tok, d), BF16),
                pltpu.VMEM((d, n_tok), BF16),
                pltpu.VMEM((W_SLOTS, d, FC), BF16),
                pltpu.VMEM((W_SLOTS, FC, d), BF16),
                pltpu.VMEM((2, FC, n_tok), BF16),
                pltpu.VMEM((2, n_tok, FC), BF16),
                pltpu.VMEM((P_SLOTS, d, FC), F32),
                pltpu.VMEM((P_SLOTS, FC, d), F32),
                pltpu.VMEM((P_SLOTS, d // 2, FC), F32),
                pltpu.VMEM((P_SLOTS, FC // 2, d), F32),
                pltpu.VMEM((n_ticks * SUBS * R_ROWS, 128), F32),
                pltpu.VMEM((n_ticks * SUBS * PH_ROWS[0], 128), F32),
                dma((2 * n_micro,)),
                dma((W_SLOTS,)),
                dma((W_SLOTS,)),
                dma((W_SLOTS,)),
                dma((P_SLOTS,)),
                dma((P_SLOTS,)),
                dma((3 * n_ticks,)),
                dma((3 * n_ticks,)),
                dma((3 * n_ticks,)),
                dma((3 * n_ticks,)),
                dma((n_ticks,)),
                dma((n_ticks,)),
                dma((n_ticks,)),
                regular((n_ticks,)),
                regular,
                regular,
            ],
            compiler_params=pltpu.CompilerParams(
                collective_id=0, has_side_effects=True, vmem_limit_bytes=67043328 - (16 << 20)),
            name="grads",
        )(x_in, dy_out, lengths.reshape(n_micro), w_up, w_down)
        return gu[None], gd[None]

    return jax.shard_map(device_grads, mesh=mesh, in_specs=(tok_spec, tok_spec, len_spec, w_spec, w_spec), out_specs=(w_spec, w_spec), check_vma=False)
```

```python
import functools

import jax
import jax.numpy as jnp
from jax import lax
from jax.experimental import pallas as pl
from jax.experimental.pallas import tpu as pltpu
from jax.sharding import PartitionSpec as P

F32, BF16 = jnp.float32, jnp.bfloat16
MESH_ID = pl.DeviceIdType.MESH
SQRT_2_OVER_PI = 0.7978845608028654
CUBIC = 0.044715
NT_DIMS = (((1,), (1,)), ((), ()))

FC = 256
RING = 4
SUBS = 4
PH_ROWS = (128, 32, 8)
PH_OFF = (0, 384, 480)
R_ROWS = 504
W_SLOTS = 3
P_SLOTS = 2
STAGES = ("pair", "rs0b", "rs0c", "rs1b", "rs1c", "rs2b", "rs2c", "ag2b", "ag2c", "ag1b", "ag1c", "ag0b", "ag0c")

BLOCKS = 3
TABLE = (
    (),
    (),
    (),
    (),
    ((0, 0),),
    (),
    ((1, 0),),
    ((0, 1),),
    ((2, 0),),
    ((1, 1),),
    ((0, 2),),
    ((4, 0), (2, 1),),
    (),
    ((1, 2), (0, 3),),
    ((4, 1), (6, 0),),
    ((2, 2),),
    ((0, 4), (1, 3),),
    ((6, 1), (8, 0),),
    ((4, 2), (1, 4),),
    ((0, 5),),
    ((2, 3), (8, 1), (10, 0),),
    ((6, 2),),
    ((2, 4), (0, 6), (1, 5),),
    ((4, 3), (10, 1),),
    (),
    ((0, 7), (8, 2), (3, 4),),
    ((11, 0),),
    ((2, 5), (6, 3),),
    ((0, 8), (1, 6), (11, 1), (1, 7),),
    ((3, 5), (10, 2),),
    ((4, 4), (12, 0), (1, 8),),
    ((0, 9),),
    ((8, 3), (2, 6),),
    ((12, 1),),
    ((4, 5), (5, 4), (2, 7), (0, 10), (11, 2),),
    ((1, 9), (2, 8),),
    ((3, 6), (6, 4), (5, 5), (3, 7), (10, 3),),
    ((0, 11),),
    ((1, 10), (12, 2), (3, 8),),
    ((6, 5), (4, 7), (7, 4), (4, 6),),
    ((2, 9), (0, 12), (11, 3),),
    ((2, 10), (1, 11), (4, 8), (7, 5), (5, 7), (8, 4),),
    ((3, 9), (5, 6),),
    ((0, 13), (1, 12),),
    ((9, 4), (4, 9), (8, 5), (6, 7), (6, 6), (2, 11), (5, 8), (3, 10), (1, 13),),
    ((0, 14),),
    ((7, 7), (9, 5), (10, 4), (5, 9),),
    ((1, 14), (12, 3), (4, 10), (3, 11), (7, 6), (2, 13), (2, 12), (6, 8), (0, 15), (8, 7), (8, 6),),
    ((3, 13), (4, 11), (3, 12), (5, 10), (2, 14), (7, 8), (6, 9), (11, 4), (1, 15), (9, 6), (4, 13), (6, 10), (5, 11), (9, 7), (4, 12), (7, 9), (3, 14), (8, 8), (10, 5), (6, 11), (2, 15), (7, 10), (5, 12), (5, 13), (8, 9), (9, 8), (4, 14), (10, 6), (8, 10), (12, 4), (11, 5), (3, 15), (6, 12), (7, 11), (5, 14), (6, 13), (9, 9), (10, 7), (9, 10), (11, 6), (4, 15), (6, 14), (7, 12), (7, 13), (8, 11), (12, 5), (10, 8), (11, 7), (5, 15), (10, 9), (7, 14), (8, 12), (8, 13), (10, 10), (9, 11), (6, 15), (11, 9), (11, 8), (8, 14), (9, 13), (7, 15), (10, 11), (11, 10), (9, 12), (12, 9), (9, 14), (8, 15), (10, 13), (12, 6), (11, 11), (9, 15), (10, 12), (12, 7), (12, 8), (10, 14), (12, 10), (11, 12), (12, 11), (10, 15), (11, 13), (11, 14), (11, 15), (12, 13), (12, 14), (12, 12), (12, 15),),
)
DIRECT = (0, 1, 2, 3)
LANES = 128
SHAPES = (
    3, 0, 0, 6, 6, 6, 0, 2, 0, 6, 6, 6, 0, 0, 0, 6, 2, 5, 0, 0, 0, 6, 2, 6, 6, 0, 0, 6, 6, 7, 0, 0,
    0, 6, 6, 6, 0, 6, 0, 6, 6, 6, 0, 0, 6, 6, 6, 6, 5, 0, 4, 6, 6, 6, 0, 0, 5, 6, 6, 6, 0, 0, 4, 6,
)


def stages_of(t):
    return [k for k, n in enumerate(STAGES) if not (t in DIRECT and n in ("rs1b", "rs2b", "ag2b", "ag1b"))]


def program(n_ticks):
    if n_ticks == 16 and TABLE:
        return TABLE
    slots = [[] for _ in range(BLOCKS * n_ticks + 1)]
    for t in range(n_ticks):
        for k, s in enumerate(stages_of(t)):
            slots[min(BLOCKS * (t + 1) + 1 + k, BLOCKS * n_ticks)].append((s, t))
    slots[-1].sort()
    return slots


def gelu_and_slope(u):
    u2 = u * u
    half = 0.5 + 0.5 * jnp.tanh(u * (SQRT_2_OVER_PI + (CUBIC * SQRT_2_OVER_PI) * u2))
    a = u * half
    return a, half + (a * (1.0 - half)) * (2.0 * SQRT_2_OVER_PI + (6.0 * CUBIC * SQRT_2_OVER_PI) * u2)


def subs_of(t):
    blocks = []
    for g in range(SUBS * t, SUBS * t + SUBS):
        code, a = SHAPES[g % len(SHAPES)], g % 3
        b, c = ((a + 1) % 3, (a + 2) % 3) if code % 2 == 0 else ((a + 2) % 3, (a + 1) % 3)
        dirs = (1 if g // 3 % 2 == 0 else -1, -1 if code & 2 else 1, -1 if code & 4 else 1)
        blocks.append((g, (a, b, c), dirs))
    return blocks


def kernel(n_ticks, n_tok, n_micro,
           x_hbm, dy_hbm, len_ref, wu_hbm, wd_hbm, GU, GD,
           X, DY, XT, WU, WD, AT, DH, SU, SD, RU, RD, R, E,
           in_sem, w_local, w_send, w_recv, p_send, p_recv, rs1, rs2, ag1, ag2, send0, send1, out_send,
           g_free, w_credit, r_credit):
    tok = n_tok // n_micro
    half_ff = n_ticks * 128
    rep = lax.axis_index("replica")
    me = lax.axis_index("fsdp")
    mate = 1 - me

    def dev(replica, core):
        return (0, replica, core)

    strides = [RING**a for a in range(3)]
    coord = [(rep // s) % RING for s in strides]
    quarter = [[coord[a]] + [(coord[a] + k) % RING for k in range(1, RING)] for a in range(3)]
    near = [{d: rep + strides[a] * (quarter[a][d % RING] - coord[a]) for d in (1, -1, 2, 3)} for a in range(3)]

    def row_in_quarter(axes, phase):
        row = 0
        for p in range(1, phase):
            row = row + coord[axes[p]] * PH_ROWS[p]
        return row

    def g_part(g, q, row, n):
        t, s = g // SUBS, g % SUBS
        if s < 2:
            start = q * 128 + row
            return GU.at[pl.ds(pl.multiple_of(start, 8), n), pl.ds(s * half_ff + t * 128, 128)]
        start = t * 128 + row
        if not isinstance(start, int):
            start = pl.multiple_of(start, 8)
        return GD.at[pl.ds(start, n), pl.ds(pl.multiple_of((s - 2) * 512 + q * 128, 128), 128)]

    def r_part(g, start, n):
        return R.at[pl.ds(g * R_ROWS + start, n)]

    def e_part(g, row, n):
        start = g * PH_ROWS[0] + row
        if not isinstance(start, int):
            start = pl.multiple_of(start, 8)
        return E.at[pl.ds(start, n)]

    def wait_rows(sem, n):
        ref = R.at[pl.ds(0, n)]
        pltpu.make_async_copy(ref, ref, sem).wait()

    barrier = pltpu.get_barrier_semaphore()
    for a in range(3):
        for d in (1, -1, 2):
            pl.semaphore_signal(barrier, inc=1, device_id=dev(near[a][d], me), device_id_type=MESH_ID)
    pl.semaphore_signal(barrier, inc=1, device_id=dev(rep, mate), device_id_type=MESH_ID)

    n_cols = X.shape[0]

    def x_copy(k):
        return [pltpu.make_async_copy(x_hbm.at[k, :, pl.ds(c * LANES, LANES)], X.at[c, pl.ds(k * tok, tok)], in_sem.at[k]) for c in range(n_cols)]

    def dy_copy(k):
        return [pltpu.make_async_copy(dy_hbm.at[k, :, pl.ds(c * LANES, LANES)], DY.at[c, pl.ds(k * tok, tok)], in_sem.at[n_micro + k]) for c in range(n_cols)]

    for k in range(n_micro):
        for copy in x_copy(k):
            copy.start()
    for k in range(n_micro):
        for copy in dy_copy(k):
            copy.start()

    def landed(ref, k, sem):
        block = ref.at[:, pl.ds(k * tok, tok)]
        pltpu.make_async_copy(block, block, sem).wait()

    def start_w(t):
        slot = t % W_SLOTS
        lo = pl.multiple_of(t * 128, 128)
        hi = pl.multiple_of(half_ff + t * 128, 128)
        up_rows = pl.ds(pl.multiple_of(me * 512, 512), 512)
        down_rows = pl.ds(pl.multiple_of(me * 128, 128), 128)
        pairs = (
            (wu_hbm.at[0, :, pl.ds(lo, 128)], WU.at[slot, up_rows, pl.ds(0, 128)]),
            (wu_hbm.at[0, :, pl.ds(hi, 128)], WU.at[slot, up_rows, pl.ds(128, 128)]),
            (wd_hbm.at[0, pl.ds(lo, 128), :], WD.at[slot, down_rows, :]),
        )
        for s, d in pairs:
            pltpu.make_async_remote_copy(
                s, d, w_send.at[slot], w_recv.at[slot], device_id=dev(rep, mate), device_id_type=MESH_ID).start()
        for s, d in pairs:
            pltpu.make_async_copy(s, d, w_local.at[slot]).start()

    def wait_w(t):
        slot = t % W_SLOTS
        ref = WU.at[slot]
        for sem in (w_local, w_recv, w_send):
            pltpu.make_async_copy(ref, ref, sem.at[slot]).wait()

    with jax.named_scope("entry"):
        pl.semaphore_wait(barrier, 10)
    start_w(0)
    if n_ticks > 1:
        start_w(1)

    rb = min(256, tok)
    for k in range(n_micro):
        with jax.named_scope("xwait"):
            landed(X, k, in_sem.at[k])

        def transpose_rows(s, carry, k=k):
            rows = pl.ds(pl.multiple_of(k * tok + s * rb, rb), rb)
            for c in range(n_cols):
                XT[pl.ds(c * LANES, LANES), rows] = X[c, rows, :].T
            return carry

        lax.fori_loop(0, tok // rb, transpose_rows, 0)
    mb = min(64, tok)
    for k in range(n_micro):
        with jax.named_scope("dywait"):
            landed(DY, k, in_sem.at[n_micro + k])
        n_valid = len_ref[k]

        def mask_rows(s, carry, k=k, n_valid=n_valid):
            rows = pl.ds(pl.multiple_of(k * tok + s * mb, mb), mb)
            at = s * mb + lax.broadcasted_iota(jnp.int32, (mb, LANES), 0)
            for c in range(n_cols):
                DY[c, rows, :] = jnp.where(at < n_valid, DY[c, rows, :].astype(F32), 0.0).astype(BF16)
            return carry

        lax.fori_loop(0, tok // mb, mask_rows, 0)

    def wide(ref, rows, lo, hi):
        return jnp.concatenate([ref[c, rows, :] for c in range(lo, hi)], axis=1)

    cb = min(512, n_tok // 2)

    def hidden(t, part):
        slot = t % W_SLOTS
        if part == 0:
            with jax.named_scope("wwait"):
                wait_w(t)
        for at in range(part * (n_tok // 2), (part + 1) * (n_tok // 2), cb):
            rows = pl.ds(at, cb)
            h = jnp.dot(wide(X, rows, 0, n_cols), WU[slot], preferred_element_type=F32).astype(BF16).astype(F32)
            da = lax.dot_general(wide(DY, rows, 0, n_cols), WD[slot], NT_DIMS, preferred_element_type=F32)
            a, slope = gelu_and_slope(h)
            AT[:, rows] = a.astype(BF16).T
            DH[rows, :] = (da * slope).astype(BF16)

    def free_w(t):
        @pl.when(t + W_SLOTS < n_ticks)
        def _():
            pl.semaphore_signal(w_credit, inc=1, device_id=dev(rep, mate), device_id_type=MESH_ID)

    def more_w(t):
        @pl.when((t < n_ticks) & (t >= W_SLOTS))
        def _():
            pl.semaphore_wait(w_credit, 1)

        @pl.when(t < n_ticks)
        def _():
            start_w(t)

    def send_to_mate(t, part):
        slot = t % P_SLOTS
        if part == 0:
            src, dst = SU.at[slot, pl.ds(pl.multiple_of(mate * 512, 512), 512)], RU.at[slot]
        else:
            src, dst = SD.at[slot, pl.ds(pl.multiple_of(mate * 128, 128), 128)], RD.at[slot]
        pltpu.make_async_remote_copy(
            src, dst, p_send.at[slot], p_recv.at[slot], device_id=dev(rep, mate), device_id_type=MESH_ID).start()

    def take_pair_room(t):
        @pl.when(t >= P_SLOTS)
        def _():
            pl.semaphore_wait(r_credit, 1)

    def up(t):
        slot = t % P_SLOTS
        for s in range(2):
            rows = pl.ds(s * 512, 512)
            SU[slot, rows, :] = jnp.dot(XT[rows, :], DH[...], preferred_element_type=F32)
        send_to_mate(t, 0)

    def down(t):
        slot = t % P_SLOTS
        for s in range(2):
            cols = pl.ds(s * 512, 512)
            SD[slot, :, cols] = jnp.dot(AT[...], wide(DY, slice(None), 4 * s, 4 * s + 4), preferred_element_type=F32)
        send_to_mate(t, 1)

    def send(sent, src, dst, recv, to):
        pltpu.make_async_remote_copy(
            src, dst, sent, recv, device_id=dev(to, me), device_id_type=MESH_ID).start()

    def pair_stage(t):
        slot = t % P_SLOTS
        whole = SU.at[slot]
        pltpu.make_async_copy(whole, whole, p_recv.at[slot]).wait()
        own = pl.ds(pl.multiple_of(me * 512, 512), 512)
        for s in range(2):
            cols = pl.ds(s * 128, 128)
            GU[:, pl.ds(s * half_ff + t * 128, 128)] = SU[slot, own, cols] + RU[slot, :, cols]
        own = pl.ds(pl.multiple_of(me * 128, 128), 128)
        GD[pl.ds(t * 128, 128), :] = SD[slot, own, :] + RD[slot]
        pltpu.make_async_copy(whole, whole, p_send.at[slot]).wait()
        if t + P_SLOTS < n_ticks:
            pl.semaphore_signal(r_credit, inc=1, device_id=dev(rep, mate), device_id_type=MESH_ID)
        rs_a(t, 0)

    def rs_a(t, p):
        sent = (send0 if p == 0 else send1).at[t]
        m, off = PH_ROWS[p], PH_OFF[p]
        if p > 0 and t in DIRECT:
            for k in (2, 1, 3):
                for g, axes, dirs in subs_of(t):
                    a = axes[p]
                    src = g_part(g, coord[axes[0]], row_in_quarter(axes, p) + quarter[a][k] * m, m)
                    send(sent, src, r_part(g, off + (k - 1) * m, m), rs2.at[t * 3 + p], near[a][k])
            return
        for relay in (True, False):
            for g, axes, dirs in subs_of(t):
                a, d = axes[p], dirs[p]
                q = quarter[a][2 if relay else -d % RING]
                src = g_part(g, q, 0, m) if p == 0 else g_part(g, coord[axes[0]], row_in_quarter(axes, p) + q * m, m)
                if relay:
                    send(sent, src, r_part(g, off, m), rs1.at[t * 3 + p], near[a][d])
                else:
                    send(sent, src, r_part(g, off + m, m), rs2.at[t * 3 + p], near[a][-d])

    def rs_b(t, p):
        sent = (send0 if p == 0 else send1).at[t]
        m, off = PH_ROWS[p], PH_OFF[p]
        wait_rows(rs1.at[t * 3 + p], SUBS * m)
        for g, axes, dirs in subs_of(t):
            a, d = axes[p], dirs[p]
            q = quarter[a][d % RING]
            part = g_part(g, q, 0, m) if p == 0 else g_part(g, coord[axes[0]], row_in_quarter(axes, p) + q * m, m)
            part[...] = part[...] + r_part(g, off, m)[...]
            send(sent, part, r_part(g, off + 2 * m, m), rs2.at[t * 3 + p], near[a][d])

    def rs_c(t, p):
        m, off = PH_ROWS[p], PH_OFF[p]
        straight = p > 0 and t in DIRECT
        wait_rows(rs2.at[t * 3 + p], (3 if straight else 2) * SUBS * m)
        for g, axes, dirs in subs_of(t):
            row = 0 if p == 0 else row_in_quarter(axes, p) + coord[axes[p]] * m
            part = g_part(g, coord[axes[0]], row, m)
            out = e_part(g, row, m) if p == 2 else part
            total = part[...] + (r_part(g, off + m, m)[...] + r_part(g, off + 2 * m, m)[...])
            out[...] = total + r_part(g, off, m)[...] if straight else total
        if p < 2:
            rs_a(t, p + 1)
        else:
            ag_a(t, 2)
        if p == 1:
            wait_rows(send0.at[t], 3 * SUBS * PH_ROWS[0])
            for a in sorted({axes[0] for _, axes, _ in subs_of(t)}):
                for d in (1, -1):
                    pl.semaphore_signal(g_free.at[t], inc=1, device_id=dev(near[a][d], me), device_id_type=MESH_ID)

    def ag_part(g, axes, p, q):
        if p == 0:
            return g_part(g, q, 0, PH_ROWS[0])
        return e_part(g, row_in_quarter(axes, p) + q * PH_ROWS[p], PH_ROWS[p])

    def ag_a(t, p):
        if p == 0:
            pl.semaphore_wait(g_free.at[t], 2 * len({axes[0] for _, axes, _ in subs_of(t)}))
        if p > 0 and t in DIRECT:
            for k in (2, 1, 3):
                for g, axes, dirs in subs_of(t):
                    part = ag_part(g, axes, p, coord[axes[p]])
                    send(out_send.at[t], part, part, ag2.at[t * 3 + p], near[axes[p]][k])
            return
        for recv, sign in ((ag1, 1), (ag2, -1)):
            for g, axes, dirs in subs_of(t):
                a, d = axes[p], dirs[p]
                part = ag_part(g, axes, p, coord[a])
                src = e_part(g, 0, PH_ROWS[0]) if p == 0 else part
                send(out_send.at[t], src, part, recv.at[t * 3 + p], near[a][sign * d])
        if p == 0:
            wait_rows(send1.at[t], 3 * SUBS * (PH_ROWS[1] + PH_ROWS[2]))
            for g, axes, dirs in subs_of(t):
                g_part(g, coord[axes[0]], 0, PH_ROWS[0])[...] = e_part(g, 0, PH_ROWS[0])[...]

    def ag_b(t, p):
        wait_rows(ag1.at[t * 3 + p], SUBS * PH_ROWS[p])
        for g, axes, dirs in subs_of(t):
            a, d = axes[p], dirs[p]
            part = ag_part(g, axes, p, quarter[a][-d % RING])
            send(out_send.at[t], part, part, ag2.at[t * 3 + p], near[a][d])

    def ag_c(t, p):
        wait_rows(ag2.at[t * 3 + p], (3 if p > 0 and t in DIRECT else 2) * SUBS * PH_ROWS[p])
        if p > 0:
            ag_a(t, p - 1)

    def run(ops):
        for s, t in ops:
            name = STAGES[s]
            with jax.named_scope(name):
                if name == "pair":
                    pair_stage(t)
                else:
                    p = int(name[2])
                    {"rsb": rs_b, "rsc": rs_c, "agb": ag_b, "agc": ag_c}[name[:2] + name[3]](t, p)

    slots = program(n_ticks)

    def pick(t, first, lo, hi):
        lists = [slots[first(k)] for k in range(lo, hi)]
        if not any(lists):
            return
        if hi - lo == 1:
            run(lists[0])
            return
        mid = (lo + hi) // 2
        pl.when(t < mid)(lambda: pick(t, first, lo, mid))
        pl.when(t >= mid)(lambda: pick(t, first, mid, hi))

    def tick(t, carry):
        with jax.named_scope("hid0"):
            hidden(t, 0)
        pick(t, lambda k: BLOCKS * k, 0, n_ticks)
        with jax.named_scope("hid1"):
            hidden(t, 1)
        free_w(t)
        pick(t, lambda k: BLOCKS * k + 1, 0, n_ticks)
        more_w(t + 2)
        take_pair_room(t)
        with jax.named_scope("grad"):
            up(t)
            down(t)
        pick(t, lambda k: BLOCKS * k + 2, 0, n_ticks)
        return carry

    lax.fori_loop(0, n_ticks, tick, 0)
    run(slots[BLOCKS * n_ticks])
    for t in range(n_ticks):
        wait_rows(out_send.at[t], SUBS * R_ROWS)


def solution(mesh):
    tok_spec = P(None, ("model", "replica", "fsdp"), None)
    len_spec = P(None, ("model", "replica", "fsdp"))
    w_spec = P(None, ("model", "fsdp"), None)

    def device_grads(x_in, dy_out, lengths, w_up, w_down):
        n_micro, tok, d = x_in.shape
        n_tok = n_micro * tok
        d_ff = w_up.shape[2]
        n_ticks = d_ff // FC
        any_spec = pl.BlockSpec(memory_space=pl.ANY)
        dma = pltpu.SemaphoreType.DMA
        regular = pltpu.SemaphoreType.REGULAR
        gu, gd = pl.pallas_call(
            functools.partial(kernel, n_ticks, n_tok, n_micro),
            out_shape=(
                pltpu.VMEM((d // 2, d_ff), F32),
                pltpu.VMEM((d_ff // 2, d), F32),
            ),
            in_specs=[any_spec, any_spec, pl.BlockSpec(memory_space=pltpu.SMEM), any_spec, any_spec],
            out_specs=(pl.BlockSpec(memory_space=pltpu.VMEM),) * 2,
            scratch_shapes=[
                pltpu.VMEM((d // LANES, n_tok, LANES), BF16),
                pltpu.VMEM((d // LANES, n_tok, LANES), BF16),
                pltpu.VMEM((d, n_tok), BF16),
                pltpu.VMEM((W_SLOTS, d, FC), BF16),
                pltpu.VMEM((W_SLOTS, FC, d), BF16),
                pltpu.VMEM((FC, n_tok), BF16),
                pltpu.VMEM((n_tok, FC), BF16),
                pltpu.VMEM((P_SLOTS, d, FC), F32),
                pltpu.VMEM((P_SLOTS, FC, d), F32),
                pltpu.VMEM((P_SLOTS, d // 2, FC), F32),
                pltpu.VMEM((P_SLOTS, FC // 2, d), F32),
                pltpu.VMEM((n_ticks * SUBS * R_ROWS, 128), F32),
                pltpu.VMEM((n_ticks * SUBS * PH_ROWS[0], 128), F32),
                dma((2 * n_micro,)),
                dma((W_SLOTS,)),
                dma((W_SLOTS,)),
                dma((W_SLOTS,)),
                dma((P_SLOTS,)),
                dma((P_SLOTS,)),
                dma((3 * n_ticks,)),
                dma((3 * n_ticks,)),
                dma((3 * n_ticks,)),
                dma((3 * n_ticks,)),
                dma((n_ticks,)),
                dma((n_ticks,)),
                dma((n_ticks,)),
                regular((n_ticks,)),
                regular,
                regular,
            ],
            compiler_params=pltpu.CompilerParams(
                collective_id=0, has_side_effects=True, vmem_limit_bytes=67043328 - (16 << 20)),
            name="grads",
        )(x_in, dy_out, lengths.reshape(n_micro), w_up, w_down)
        return gu[None], gd[None]

    return jax.shard_map(device_grads, mesh=mesh, in_specs=(tok_spec, tok_spec, len_spec, w_spec, w_spec), out_specs=(w_spec, w_spec), check_vma=False)
```

```python
import functools

import jax
import jax.numpy as jnp
from jax import lax
from jax.experimental import pallas as pl
from jax.experimental.pallas import tpu as pltpu
from jax.sharding import PartitionSpec as P

F32, BF16 = jnp.float32, jnp.bfloat16
MESH_ID = pl.DeviceIdType.MESH
SQRT_2_OVER_PI = 0.7978845608028654
CUBIC = 0.044715
NT_DIMS = (((1,), (1,)), ((), ()))

FC = 256
RING = 4
SUBS = 4
PH_ROWS = (128, 32, 8)
PH_OFF = (0, 384, 480)
R_ROWS = 504
W_SLOTS = 3
P_SLOTS = 2
STAGES = ("pair", "rs0b", "rs0c", "rs1b", "rs1c", "rs2b", "rs2c", "ag2b", "ag2c", "ag1b", "ag1c", "ag0b", "ag0c")

BLOCKS = 3
TABLE = (
    (),
    (),
    (),
    (),
    ((0, 0),),
    (),
    (),
    ((1, 0), (0, 1),),
    (),
    (),
    ((2, 0), (0, 2),),
    ((1, 1),),
    (),
    ((4, 0), (0, 3),),
    ((1, 2),),
    ((6, 0), (2, 1),),
    ((0, 4), (1, 3),),
    ((2, 2),),
    ((4, 1), (8, 0),),
    ((1, 4), (0, 5),),
    ((2, 3),),
    ((6, 1), (4, 2), (10, 0),),
    ((2, 4), (0, 6), (1, 5),),
    (),
    ((6, 2), (8, 1),),
    ((4, 3), (0, 7),),
    ((3, 4), (1, 6),),
    ((2, 5), (8, 2),),
    ((6, 3), (10, 1), (0, 8),),
    ((3, 5), (2, 6),),
    ((1, 7), (10, 2), (4, 4),),
    ((0, 9), (8, 3),),
    ((1, 8), (3, 6),),
    ((4, 5),),
    ((2, 7), (5, 4), (11, 0),),
    ((11, 2), (1, 9),),
    ((0, 10),),
    ((4, 6), (6, 4), (5, 5), (3, 7), (2, 8), (0, 11), (10, 3),),
    (),
    ((1, 10),),
    ((7, 4), (5, 6), (2, 9), (4, 7), (6, 5), (3, 8), (0, 12), (11, 1),),
    (),
    ((1, 11),),
    ((4, 8), (5, 7), (7, 5), (2, 10), (6, 6), (0, 13),),
    ((8, 4), (1, 12),),
    ((3, 9), (2, 11), (5, 8), (8, 5), (3, 10),),
    ((7, 6), (6, 7), (0, 14), (1, 13),),
    (),
    ((9, 4), (3, 11), (4, 9), (6, 8), (2, 12), (4, 10), (8, 6), (1, 14), (0, 15), (2, 13), (5, 10), (7, 8), (4, 11), (5, 9), (3, 12), (9, 6), (9, 5), (10, 4), (1, 15), (2, 14), (6, 10), (7, 7), (12, 2), (3, 13), (5, 11), (4, 12), (6, 9), (8, 8), (10, 5), (2, 15), (3, 14), (4, 13), (6, 11), (5, 12), (7, 9), (7, 10), (8, 7), (11, 4), (11, 3), (11, 5), (3, 15), (7, 11), (4, 14), (5, 13), (9, 7), (6, 12), (10, 6), (8, 9), (8, 10), (4, 15), (5, 14), (6, 13), (8, 11), (7, 12), (9, 8), (10, 7), (11, 6), (5, 15), (6, 14), (7, 13), (9, 9), (9, 10), (8, 12), (9, 11), (10, 8), (7, 14), (12, 3), (6, 15), (8, 13), (11, 7), (10, 9), (12, 5), (12, 6), (12, 4), (9, 12), (8, 14), (7, 15), (11, 8), (10, 10), (9, 13), (11, 9), (9, 14), (8, 15), (10, 12), (10, 11), (9, 15), (10, 14), (10, 13), (12, 1), (12, 8), (10, 15), (12, 9), (11, 14), (12, 0), (11, 12), (11, 13), (11, 15), (11, 10), (11, 11), (12, 14), (12, 7), (12, 15), (12, 13), (12, 12), (12, 10), (12, 11),),
)
DIRECT = (0, 1, 2, 3)
LANES = 128
SHAPES = (
    3, 0, 0, 6, 6, 6, 0, 2, 0, 6, 6, 6, 0, 0, 0, 6, 2, 5, 0, 0, 0, 6, 2, 6, 6, 0, 0, 6, 6, 7, 0, 0,
    0, 6, 6, 6, 0, 6, 0, 6, 6, 6, 0, 0, 6, 6, 6, 6, 5, 0, 4, 6, 6, 6, 0, 0, 5, 6, 6, 6, 0, 0, 4, 6,
)


def stages_of(t):
    return [k for k, n in enumerate(STAGES) if not (t in DIRECT and n in ("rs1b", "rs2b", "ag2b", "ag1b"))]


def program(n_ticks):
    if n_ticks == 16 and TABLE:
        return TABLE
    slots = [[] for _ in range(BLOCKS * n_ticks + 1)]
    for t in range(n_ticks):
        for k, s in enumerate(stages_of(t)):
            slots[min(BLOCKS * (t + 1) + 1 + k, BLOCKS * n_ticks)].append((s, t))
    slots[-1].sort()
    return slots


def gelu_and_slope(u):
    u2 = u * u
    half = 0.5 + 0.5 * jnp.tanh(u * (SQRT_2_OVER_PI + (CUBIC * SQRT_2_OVER_PI) * u2))
    a = u * half
    return a, half + (a * (1.0 - half)) * (2.0 * SQRT_2_OVER_PI + (6.0 * CUBIC * SQRT_2_OVER_PI) * u2)


def subs_of(t):
    blocks = []
    for g in range(SUBS * t, SUBS * t + SUBS):
        code, a = SHAPES[g % len(SHAPES)], g % 3
        b, c = ((a + 1) % 3, (a + 2) % 3) if code % 2 == 0 else ((a + 2) % 3, (a + 1) % 3)
        dirs = (1 if g // 3 % 2 == 0 else -1, -1 if code & 2 else 1, -1 if code & 4 else 1)
        blocks.append((g, (a, b, c), dirs))
    return blocks


def kernel(n_ticks, n_tok, n_micro, sems, *refs):
    pl.run_scoped(functools.partial(body, n_ticks, n_tok, n_micro, refs), *sems)


def body(n_ticks, n_tok, n_micro, refs,
         in_sem, w_local, w_send, w_recv, p_send, p_recv, rs1, rs2, ag1, ag2, send0, send1, out_send,
         g_free, w_credit, r_credit):
    (x_hbm, dy_hbm, len_ref, wu_hbm, wd_hbm, GU, GD,
     X, DY, XT, WU, WD, AT, DH, SU, SD, RU, RD, R, E) = refs
    tok = n_tok // n_micro
    half_ff = n_ticks * 128
    rep = lax.axis_index("replica")
    me = lax.axis_index("fsdp")
    mate = 1 - me

    def dev(replica, core):
        return (0, replica, core)

    strides = [RING**a for a in range(3)]
    coord = [(rep // s) % RING for s in strides]
    quarter = [[coord[a]] + [(coord[a] + k) % RING for k in range(1, RING)] for a in range(3)]
    near = [{d: rep + strides[a] * (quarter[a][d % RING] - coord[a]) for d in (1, -1, 2, 3)} for a in range(3)]

    def row_in_quarter(axes, phase):
        row = 0
        for p in range(1, phase):
            row = row + coord[axes[p]] * PH_ROWS[p]
        return row

    def g_part(g, q, row, n):
        t, s = g // SUBS, g % SUBS
        if s < 2:
            start = q * 128 + row
            return GU.at[pl.ds(pl.multiple_of(start, 8), n), pl.ds(s * half_ff + t * 128, 128)]
        start = t * 128 + row
        if not isinstance(start, int):
            start = pl.multiple_of(start, 8)
        return GD.at[pl.ds(start, n), pl.ds(pl.multiple_of((s - 2) * 512 + q * 128, 128), 128)]

    def r_part(g, start, n):
        return R.at[pl.ds(g * R_ROWS + start, n)]

    def e_part(g, row, n):
        start = g * PH_ROWS[0] + row
        if not isinstance(start, int):
            start = pl.multiple_of(start, 8)
        return E.at[pl.ds(start, n)]

    def wait_rows(sem, n):
        ref = R.at[pl.ds(0, n)]
        pltpu.make_async_copy(ref, ref, sem).wait()

    barrier = pltpu.get_barrier_semaphore()
    for a in range(3):
        for d in (1, -1, 2):
            pl.semaphore_signal(barrier, inc=1, device_id=dev(near[a][d], me), device_id_type=MESH_ID)
    pl.semaphore_signal(barrier, inc=1, device_id=dev(rep, mate), device_id_type=MESH_ID)

    n_cols = X.shape[0]

    def x_copy(k):
        return [pltpu.make_async_copy(x_hbm.at[k, :, pl.ds(c * LANES, LANES)], X.at[c, pl.ds(k * tok, tok)], in_sem.at[k]) for c in range(n_cols)]

    def dy_copy(k):
        return [pltpu.make_async_copy(dy_hbm.at[k, :, pl.ds(c * LANES, LANES)], DY.at[c, pl.ds(k * tok, tok)], in_sem.at[n_micro + k]) for c in range(n_cols)]

    for k in range(n_micro):
        for copy in x_copy(k):
            copy.start()
    for k in range(n_micro):
        for copy in dy_copy(k):
            copy.start()

    def landed(ref, k, sem):
        block = ref.at[:, pl.ds(k * tok, tok)]
        pltpu.make_async_copy(block, block, sem).wait()

    def start_w(t):
        slot = t % W_SLOTS
        lo = pl.multiple_of(t * 128, 128)
        hi = pl.multiple_of(half_ff + t * 128, 128)
        up_rows = pl.ds(pl.multiple_of(me * 512, 512), 512)
        down_rows = pl.ds(pl.multiple_of(me * 128, 128), 128)
        pairs = (
            (wu_hbm.at[0, :, pl.ds(lo, 128)], WU.at[slot, up_rows, pl.ds(0, 128)]),
            (wu_hbm.at[0, :, pl.ds(hi, 128)], WU.at[slot, up_rows, pl.ds(128, 128)]),
            (wd_hbm.at[0, pl.ds(lo, 128), :], WD.at[slot, down_rows, :]),
        )
        for s, d in pairs:
            pltpu.make_async_remote_copy(
                s, d, w_send.at[slot], w_recv.at[slot], device_id=dev(rep, mate), device_id_type=MESH_ID).start()
        for s, d in pairs:
            pltpu.make_async_copy(s, d, w_local.at[slot]).start()

    def wait_w(t):
        slot = t % W_SLOTS
        ref = WU.at[slot]
        for sem in (w_local, w_recv, w_send):
            pltpu.make_async_copy(ref, ref, sem.at[slot]).wait()

    with jax.named_scope("entry"):
        pl.semaphore_wait(barrier, 10)
    start_w(0)
    if n_ticks > 1:
        start_w(1)

    rb = min(256, tok)
    for k in range(n_micro):
        with jax.named_scope("xwait"):
            landed(X, k, in_sem.at[k])

        def transpose_rows(s, carry, k=k):
            rows = pl.ds(pl.multiple_of(k * tok + s * rb, rb), rb)
            for c in range(n_cols):
                XT[pl.ds(c * LANES, LANES), rows] = X[c, rows, :].T
            return carry

        lax.fori_loop(0, tok // rb, transpose_rows, 0)
    mb = min(64, tok)
    for k in range(n_micro):
        with jax.named_scope("dywait"):
            landed(DY, k, in_sem.at[n_micro + k])
        n_valid = len_ref[k]

        def mask_rows(s, carry, k=k, n_valid=n_valid):
            rows = pl.ds(pl.multiple_of(k * tok + s * mb, mb), mb)
            at = s * mb + lax.broadcasted_iota(jnp.int32, (mb, LANES), 0)
            for c in range(n_cols):
                DY[c, rows, :] = jnp.where(at < n_valid, DY[c, rows, :].astype(F32), 0.0).astype(BF16)
            return carry

        lax.fori_loop(0, tok // mb, mask_rows, 0)

    def wide(ref, rows, lo, hi):
        return jnp.concatenate([ref[c, rows, :] for c in range(lo, hi)], axis=1)

    cb = min(256, n_tok // 2)

    def hidden(t, part):
        slot = t % W_SLOTS
        if part == 0:
            with jax.named_scope("wwait"):
                wait_w(t)
        for at in range(part * (n_tok // 2), (part + 1) * (n_tok // 2), cb):
            rows = pl.ds(at, cb)
            h = jnp.dot(wide(X, rows, 0, n_cols), WU[slot], preferred_element_type=F32).astype(BF16).astype(F32)
            da = lax.dot_general(wide(DY, rows, 0, n_cols), WD[slot], NT_DIMS, preferred_element_type=F32)
            a, slope = gelu_and_slope(h)
            AT[:, rows] = a.astype(BF16).T
            DH[rows, :] = (da * slope).astype(BF16)

    def free_w(t):
        @pl.when(t + W_SLOTS < n_ticks)
        def _():
            pl.semaphore_signal(w_credit, inc=1, device_id=dev(rep, mate), device_id_type=MESH_ID)

    def more_w(t):
        @pl.when((t < n_ticks) & (t >= W_SLOTS))
        def _():
            pl.semaphore_wait(w_credit, 1)

        @pl.when(t < n_ticks)
        def _():
            start_w(t)

    def send_to_mate(t, part):
        slot = t % P_SLOTS
        if part == 0:
            src, dst = SU.at[slot, pl.ds(pl.multiple_of(mate * 512, 512), 512)], RU.at[slot]
        else:
            src, dst = SD.at[slot, pl.ds(pl.multiple_of(mate * 128, 128), 128)], RD.at[slot]
        pltpu.make_async_remote_copy(
            src, dst, p_send.at[slot], p_recv.at[slot], device_id=dev(rep, mate), device_id_type=MESH_ID).start()

    def take_pair_room(t):
        @pl.when(t >= P_SLOTS)
        def _():
            pl.semaphore_wait(r_credit, 1)

    def up(t):
        slot = t % P_SLOTS
        for s in range(2):
            rows = pl.ds(s * 512, 512)
            SU[slot, rows, :] = jnp.dot(XT[rows, :], DH[...], preferred_element_type=F32)

    def down(t):
        slot = t % P_SLOTS
        for s in range(2):
            cols = pl.ds(s * 512, 512)
            SD[slot, :, cols] = jnp.dot(AT[...], wide(DY, slice(None), 4 * s, 4 * s + 4), preferred_element_type=F32)

    def send(sent, src, dst, recv, to):
        pltpu.make_async_remote_copy(
            src, dst, sent, recv, device_id=dev(to, me), device_id_type=MESH_ID).start()

    def pair_stage(t):
        slot = t % P_SLOTS
        whole = SU.at[slot]
        pltpu.make_async_copy(whole, whole, p_recv.at[slot]).wait()
        own = pl.ds(pl.multiple_of(me * 512, 512), 512)
        for s in range(2):
            cols = pl.ds(s * 128, 128)
            GU[:, pl.ds(s * half_ff + t * 128, 128)] = SU[slot, own, cols] + RU[slot, :, cols]
        own = pl.ds(pl.multiple_of(me * 128, 128), 128)
        GD[pl.ds(t * 128, 128), :] = SD[slot, own, :] + RD[slot]
        pltpu.make_async_copy(whole, whole, p_send.at[slot]).wait()
        if t + P_SLOTS < n_ticks:
            pl.semaphore_signal(r_credit, inc=1, device_id=dev(rep, mate), device_id_type=MESH_ID)
        rs_a(t, 0)

    def rs_a(t, p):
        sent = (send0 if p == 0 else send1).at[t]
        m, off = PH_ROWS[p], PH_OFF[p]
        if p > 0 and t in DIRECT:
            for k in (2, 1, 3):
                for g, axes, dirs in subs_of(t):
                    a = axes[p]
                    src = g_part(g, coord[axes[0]], row_in_quarter(axes, p) + quarter[a][k] * m, m)
                    send(sent, src, r_part(g, off + (k - 1) * m, m), rs2.at[t * 3 + p], near[a][k])
            return
        for relay in (True, False):
            for g, axes, dirs in subs_of(t):
                a, d = axes[p], dirs[p]
                q = quarter[a][2 if relay else -d % RING]
                src = g_part(g, q, 0, m) if p == 0 else g_part(g, coord[axes[0]], row_in_quarter(axes, p) + q * m, m)
                if relay:
                    send(sent, src, r_part(g, off, m), rs1.at[t * 3 + p], near[a][d])
                else:
                    send(sent, src, r_part(g, off + m, m), rs2.at[t * 3 + p], near[a][-d])

    def rs_b(t, p):
        sent = (send0 if p == 0 else send1).at[t]
        m, off = PH_ROWS[p], PH_OFF[p]
        wait_rows(rs1.at[t * 3 + p], SUBS * m)
        for g, axes, dirs in subs_of(t):
            a, d = axes[p], dirs[p]
            q = quarter[a][d % RING]
            part = g_part(g, q, 0, m) if p == 0 else g_part(g, coord[axes[0]], row_in_quarter(axes, p) + q * m, m)
            part[...] = part[...] + r_part(g, off, m)[...]
            send(sent, part, r_part(g, off + 2 * m, m), rs2.at[t * 3 + p], near[a][d])

    def rs_c(t, p):
        m, off = PH_ROWS[p], PH_OFF[p]
        straight = p > 0 and t in DIRECT
        wait_rows(rs2.at[t * 3 + p], (3 if straight else 2) * SUBS * m)
        for g, axes, dirs in subs_of(t):
            row = 0 if p == 0 else row_in_quarter(axes, p) + coord[axes[p]] * m
            part = g_part(g, coord[axes[0]], row, m)
            out = e_part(g, row, m) if p == 2 else part
            total = part[...] + (r_part(g, off + m, m)[...] + r_part(g, off + 2 * m, m)[...])
            out[...] = total + r_part(g, off, m)[...] if straight else total
        if p < 2:
            rs_a(t, p + 1)
        else:
            ag_a(t, 2)
        if p == 1:
            wait_rows(send0.at[t], 3 * SUBS * PH_ROWS[0])
            for a in sorted({axes[0] for _, axes, _ in subs_of(t)}):
                for d in (1, -1):
                    pl.semaphore_signal(g_free.at[t], inc=1, device_id=dev(near[a][d], me), device_id_type=MESH_ID)

    def ag_part(g, axes, p, q):
        if p == 0:
            return g_part(g, q, 0, PH_ROWS[0])
        return e_part(g, row_in_quarter(axes, p) + q * PH_ROWS[p], PH_ROWS[p])

    def ag_a(t, p):
        if p == 0:
            pl.semaphore_wait(g_free.at[t], 2 * len({axes[0] for _, axes, _ in subs_of(t)}))
        if p > 0 and t in DIRECT:
            for k in (2, 1, 3):
                for g, axes, dirs in subs_of(t):
                    part = ag_part(g, axes, p, coord[axes[p]])
                    send(out_send.at[t], part, part, ag2.at[t * 3 + p], near[axes[p]][k])
            return
        for recv, sign in ((ag1, 1), (ag2, -1)):
            for g, axes, dirs in subs_of(t):
                a, d = axes[p], dirs[p]
                part = ag_part(g, axes, p, coord[a])
                src = e_part(g, 0, PH_ROWS[0]) if p == 0 else part
                send(out_send.at[t], src, part, recv.at[t * 3 + p], near[a][sign * d])
        if p == 0:
            wait_rows(send1.at[t], 3 * SUBS * (PH_ROWS[1] + PH_ROWS[2]))
            for g, axes, dirs in subs_of(t):
                g_part(g, coord[axes[0]], 0, PH_ROWS[0])[...] = e_part(g, 0, PH_ROWS[0])[...]

    def ag_b(t, p):
        wait_rows(ag1.at[t * 3 + p], SUBS * PH_ROWS[p])
        for g, axes, dirs in subs_of(t):
            a, d = axes[p], dirs[p]
            part = ag_part(g, axes, p, quarter[a][-d % RING])
            send(out_send.at[t], part, part, ag2.at[t * 3 + p], near[a][d])

    def ag_c(t, p):
        wait_rows(ag2.at[t * 3 + p], (3 if p > 0 and t in DIRECT else 2) * SUBS * PH_ROWS[p])
        if p > 0:
            ag_a(t, p - 1)

    def run(ops):
        for s, t in ops:
            name = STAGES[s]
            with jax.named_scope(name):
                if name == "pair":
                    pair_stage(t)
                else:
                    p = int(name[2])
                    {"rsb": rs_b, "rsc": rs_c, "agb": ag_b, "agc": ag_c}[name[:2] + name[3]](t, p)

    slots = program(n_ticks)

    def pick(t, first, lo, hi):
        lists = [slots[first(k)] for k in range(lo, hi)]
        if not any(lists):
            return
        if hi - lo == 1:
            run(lists[0])
            return
        mid = (lo + hi) // 2
        pl.when(t < mid)(lambda: pick(t, first, lo, mid))
        pl.when(t >= mid)(lambda: pick(t, first, mid, hi))

    def tick(t, carry):
        with jax.named_scope("hid0"):
            hidden(t, 0)
        pick(t, lambda k: BLOCKS * k, 0, n_ticks)
        with jax.named_scope("hid1"):
            hidden(t, 1)
        free_w(t)
        pick(t, lambda k: BLOCKS * k + 1, 0, n_ticks)
        more_w(t + 2)
        take_pair_room(t)
        with jax.named_scope("grad"):
            up(t)
            down(t)
            send_to_mate(t, 0)
            send_to_mate(t, 1)
        pick(t, lambda k: BLOCKS * k + 2, 0, n_ticks)
        return carry

    lax.fori_loop(0, n_ticks, tick, 0)
    run(slots[BLOCKS * n_ticks])
    for t in range(n_ticks):
        wait_rows(out_send.at[t], SUBS * R_ROWS)


FLUSH = 8


def flush(gu, gd, gu_hbm, gd_hbm, sem):
    copies = []
    for k in range(FLUSH):
        for ref, out, s in ((gu, gu_hbm, 0), (gd, gd_hbm, 1)):
            rows = pl.ds(k * (ref.shape[0] // FLUSH), ref.shape[0] // FLUSH)
            copies.append(pltpu.make_async_copy(ref.at[rows], out.at[0, rows], sem.at[2 * k + s]))
    for copy in copies:
        copy.start()
    for copy in copies:
        copy.wait()


def solution(mesh):
    tok_spec = P(None, ("model", "replica", "fsdp"), None)
    len_spec = P(None, ("model", "replica", "fsdp"))
    w_spec = P(None, ("model", "fsdp"), None)

    def device_grads(x_in, dy_out, lengths, w_up, w_down):
        n_micro, tok, d = x_in.shape
        n_tok = n_micro * tok
        d_ff = w_up.shape[2]
        n_ticks = d_ff // FC
        any_spec = pl.BlockSpec(memory_space=pl.ANY)
        dma = pltpu.SemaphoreType.DMA
        regular = pltpu.SemaphoreType.REGULAR
        sems = [
            dma((2 * n_micro,)),
            dma((W_SLOTS,)),
            dma((W_SLOTS,)),
            dma((W_SLOTS,)),
            dma((P_SLOTS,)),
            dma((P_SLOTS,)),
            dma((3 * n_ticks,)),
            dma((3 * n_ticks,)),
            dma((3 * n_ticks,)),
            dma((3 * n_ticks,)),
            dma((n_ticks,)),
            dma((n_ticks,)),
            dma((n_ticks,)),
            regular((n_ticks,)),
            regular,
            regular,
        ]
        gu, gd = pl.pallas_call(
            functools.partial(kernel, n_ticks, n_tok, n_micro, sems),
            out_shape=(
                pltpu.VMEM((d // 2, d_ff), F32),
                pltpu.VMEM((d_ff // 2, d), F32),
            ),
            in_specs=[any_spec, any_spec, pl.BlockSpec(memory_space=pltpu.SMEM), any_spec, any_spec],
            out_specs=(pl.BlockSpec(memory_space=pltpu.VMEM),) * 2,
            scratch_shapes=[
                pltpu.VMEM((d // LANES, n_tok, LANES), BF16),
                pltpu.VMEM((d // LANES, n_tok, LANES), BF16),
                pltpu.VMEM((d, n_tok), BF16),
                pltpu.VMEM((W_SLOTS, d, FC), BF16),
                pltpu.VMEM((W_SLOTS, FC, d), BF16),
                pltpu.VMEM((FC, n_tok), BF16),
                pltpu.VMEM((n_tok, FC), BF16),
                pltpu.VMEM((P_SLOTS, d, FC), F32),
                pltpu.VMEM((P_SLOTS, FC, d), F32),
                pltpu.VMEM((P_SLOTS, d // 2, FC), F32),
                pltpu.VMEM((P_SLOTS, FC // 2, d), F32),
                pltpu.VMEM((n_ticks * SUBS * R_ROWS, 128), F32),
                pltpu.VMEM((n_ticks * SUBS * PH_ROWS[0], 128), F32),
            ],
            compiler_params=pltpu.CompilerParams(
                collective_id=0, has_side_effects=True, vmem_limit_bytes=67043328 - (16 << 20)),
            name="grads",
        )(x_in, dy_out, lengths.reshape(n_micro), w_up, w_down)
        vmem = pl.BlockSpec(memory_space=pltpu.VMEM)
        return pl.pallas_call(
            flush,
            out_shape=(
                jax.ShapeDtypeStruct(w_up.shape, F32),
                jax.ShapeDtypeStruct(w_down.shape, F32),
            ),
            in_specs=[vmem, vmem],
            out_specs=(any_spec, any_spec),
            scratch_shapes=[dma((2 * FLUSH,))],
            compiler_params=pltpu.CompilerParams(vmem_limit_bytes=1 << 20),
            name="flush",
        )(pltpu.with_memory_space_constraint(gu, pltpu.VMEM), pltpu.with_memory_space_constraint(gd, pltpu.VMEM))

    return jax.shard_map(device_grads, mesh=mesh, in_specs=(tok_spec, tok_spec, len_spec, w_spec, w_spec), out_specs=(w_spec, w_spec), check_vma=False)
```

```python
import functools

import jax
import jax.numpy as jnp
from jax import lax
from jax.experimental import pallas as pl
from jax.experimental.pallas import tpu as pltpu
from jax.sharding import PartitionSpec as P

F32, BF16 = jnp.float32, jnp.bfloat16
MESH_ID = pl.DeviceIdType.MESH
SQRT_2_OVER_PI = 0.7978845608028654
CUBIC = 0.044715
NT_DIMS = (((1,), (1,)), ((), ()))

FC = 256
RING = 4
SUBS = 4
PH_ROWS = (128, 32, 8)
PH_OFF = (0, 384, 480)
R_ROWS = 504
W_SLOTS = 3
P_SLOTS = 2
STAGES = ("pair", "rs0b", "rs0c", "rs1b", "rs1c", "rs2b", "rs2c", "ag2b", "ag2c", "ag1b", "ag1c", "ag0b", "ag0c")

OPENING = 4
MIN_LEN = 128
TABLE = (
    (),
    (),
    (),
    (),
    ((0, 0),),
    (),
    ((1, 0),),
    ((0, 1),),
    ((2, 0),),
    ((1, 1), (0, 2),),
    ((4, 0), (0, 3),),
    ((1, 2), (2, 1),),
    ((6, 0), (0, 4), (1, 3),),
    ((2, 2),),
    ((8, 0), (4, 1), (1, 4), (0, 5),),
    ((2, 3),),
    ((4, 2), (6, 1), (0, 6), (2, 4),),
    ((1, 5), (10, 0),),
    ((6, 2), (0, 7), (8, 1), (4, 3),),
    ((2, 5), (3, 4), (1, 6),),
    ((1, 7), (0, 8),),
    ((6, 3), (10, 1), (4, 4), (3, 5), (8, 2),),
    ((2, 6), (1, 8), (11, 0), (2, 7), (0, 9),),
    (),
    ((5, 4), (3, 6), (4, 5), (0, 10), (10, 2),),
    ((2, 8),),
    ((5, 5), (6, 4), (4, 6), (1, 9), (3, 7), (8, 3), (0, 11),),
    ((1, 10), (3, 8), (11, 2),),
    ((5, 6), (6, 5), (4, 7), (7, 4), (2, 9), (0, 12),),
    ((1, 11), (10, 3),),
    ((2, 10), (4, 8), (6, 6), (0, 13), (3, 9), (8, 4), (5, 7), (7, 5),),
    ((2, 11), (1, 12), (11, 1),),
    ((7, 6), (5, 8), (0, 14),),
    (),
    ((3, 11), (4, 9), (3, 10), (1, 13), (8, 5), (6, 7), (9, 4), (2, 12), (8, 6), (0, 15), (5, 9), (4, 11), (6, 8), (1, 14), (2, 13), (3, 12), (9, 6), (4, 10), (7, 7), (9, 5), (10, 4), (6, 9), (1, 15), (5, 10), (7, 8), (4, 12), (5, 11), (2, 14), (10, 6), (3, 13), (8, 7), (5, 12), (7, 9), (6, 10), (8, 8), (2, 15), (3, 14), (6, 11), (10, 5), (7, 10), (8, 9), (4, 13), (9, 7), (6, 12), (3, 15), (11, 6), (7, 11), (4, 14), (11, 4), (11, 5), (8, 10), (4, 15), (9, 8), (7, 12), (5, 13), (5, 14), (8, 11), (10, 7), (9, 9), (11, 3), (12, 2), (5, 15), (6, 13), (9, 10), (6, 14), (10, 8), (9, 11), (8, 12), (7, 13), (6, 15), (7, 14), (11, 7), (10, 9), (11, 8), (7, 15), (8, 13), (9, 12), (8, 14), (10, 10), (12, 3), (11, 9), (12, 6), (8, 15), (9, 13), (12, 4), (12, 1), (10, 12), (12, 5), (9, 14), (10, 11), (9, 15), (10, 13), (12, 9), (10, 14), (10, 15), (12, 0), (11, 13), (11, 12), (12, 8), (11, 11), (11, 15), (12, 7), (11, 10), (11, 14), (12, 11), (12, 13), (12, 15), (12, 12), (12, 10), (12, 14),),
)
DIRECT = (0, 1, 2, 3)
LANES = 128
SHAPES = (
    3, 0, 0, 6, 6, 6, 0, 2, 0, 6, 6, 6, 0, 0, 0, 6, 2, 5, 0, 0, 0, 6, 2, 6, 6, 0, 0, 6, 6, 7, 0, 0,
    0, 6, 6, 6, 0, 6, 0, 6, 6, 6, 0, 0, 6, 6, 6, 6, 5, 0, 4, 6, 6, 6, 0, 0, 5, 6, 6, 6, 0, 0, 4, 6,
)


def stages_of(t):
    return [k for k, n in enumerate(STAGES) if not (t in DIRECT and n in ("rs1b", "rs2b", "ag2b", "ag1b"))]


def program(n_ticks):
    if n_ticks == 16 and TABLE:
        return TABLE
    last = OPENING + 2 * (n_ticks - 1)
    slots = [[] for _ in range(last + 1)]
    for t in range(n_ticks):
        for k, s in enumerate(stages_of(t)):
            slots[min(OPENING + 2 * t + k, last)].append((s, t))
    slots[-1].sort()
    return slots


def gelu_and_slope(u):
    u2 = u * u
    half = 0.5 + 0.5 * jnp.tanh(u * (SQRT_2_OVER_PI + (CUBIC * SQRT_2_OVER_PI) * u2))
    a = u * half
    return a, half + (a * (1.0 - half)) * (2.0 * SQRT_2_OVER_PI + (6.0 * CUBIC * SQRT_2_OVER_PI) * u2)


def subs_of(t):
    blocks = []
    for g in range(SUBS * t, SUBS * t + SUBS):
        code, a = SHAPES[g % len(SHAPES)], g % 3
        b, c = ((a + 1) % 3, (a + 2) % 3) if code % 2 == 0 else ((a + 2) % 3, (a + 1) % 3)
        dirs = (1 if g // 3 % 2 == 0 else -1, -1 if code & 2 else 1, -1 if code & 4 else 1)
        blocks.append((g, (a, b, c), dirs))
    return blocks


def kernel(n_ticks, n_tok, n_micro, sems, *refs):
    pl.run_scoped(functools.partial(body, n_ticks, n_tok, n_micro, refs), *sems)


def body(n_ticks, n_tok, n_micro, refs,
         in_sem, w_local, w_send, w_recv, p_send, p_recv, rs1, rs2, ag1, ag2, send0, send1, out_send,
         g_free, w_credit, r_credit):
    (x_hbm, dy_hbm, len_ref, wu_hbm, wd_hbm, GU, GD,
     X, DY, XT, WU, WD, AT, DH, SU, SD, RU, RD, R, E) = refs
    tok = n_tok // n_micro
    half_ff = n_ticks * 128
    rep = lax.axis_index("replica")
    me = lax.axis_index("fsdp")
    mate = 1 - me

    def dev(replica, core):
        return (0, replica, core)

    strides = [RING**a for a in range(3)]
    coord = [(rep // s) % RING for s in strides]
    quarter = [[coord[a]] + [(coord[a] + k) % RING for k in range(1, RING)] for a in range(3)]
    near = [{d: rep + strides[a] * (quarter[a][d % RING] - coord[a]) for d in (1, -1, 2, 3)} for a in range(3)]

    def row_in_quarter(axes, phase):
        row = 0
        for p in range(1, phase):
            row = row + coord[axes[p]] * PH_ROWS[p]
        return row

    def g_part(g, q, row, n):
        t, s = g // SUBS, g % SUBS
        if s < 2:
            start = q * 128 + row
            return GU.at[pl.ds(pl.multiple_of(start, 8), n), pl.ds(s * half_ff + t * 128, 128)]
        start = t * 128 + row
        if not isinstance(start, int):
            start = pl.multiple_of(start, 8)
        return GD.at[pl.ds(start, n), pl.ds(pl.multiple_of((s - 2) * 512 + q * 128, 128), 128)]

    def r_part(g, start, n):
        return R.at[pl.ds(g * R_ROWS + start, n)]

    def e_part(g, row, n):
        start = g * PH_ROWS[0] + row
        if not isinstance(start, int):
            start = pl.multiple_of(start, 8)
        return E.at[pl.ds(start, n)]

    def wait_rows(sem, n):
        ref = R.at[pl.ds(0, n)]
        pltpu.make_async_copy(ref, ref, sem).wait()

    barrier = pltpu.get_barrier_semaphore()
    for a in range(3):
        for d in (1, -1, 2):
            pl.semaphore_signal(barrier, inc=1, device_id=dev(near[a][d], me), device_id_type=MESH_ID)
    pl.semaphore_signal(barrier, inc=1, device_id=dev(rep, mate), device_id_type=MESH_ID)

    n_cols = X.shape[0]

    def x_copy(k):
        return [pltpu.make_async_copy(x_hbm.at[k, :, pl.ds(c * LANES, LANES)], X.at[c, pl.ds(k * tok, tok)], in_sem.at[k]) for c in range(n_cols)]

    def dy_copy(k):
        return [pltpu.make_async_copy(dy_hbm.at[k, :, pl.ds(c * LANES, LANES)], DY.at[c, pl.ds(k * tok, tok)], in_sem.at[n_micro + k]) for c in range(n_cols)]

    for k in range(n_micro):
        for copy in x_copy(k):
            copy.start()
    for k in range(n_micro):
        for copy in dy_copy(k):
            copy.start()

    def landed(ref, k, sem):
        block = ref.at[:, pl.ds(k * tok, tok)]
        pltpu.make_async_copy(block, block, sem).wait()

    def start_w(t):
        slot = t % W_SLOTS
        lo = pl.multiple_of(t * 128, 128)
        hi = pl.multiple_of(half_ff + t * 128, 128)
        up_rows = pl.ds(pl.multiple_of(me * 512, 512), 512)
        down_rows = pl.ds(pl.multiple_of(me * 128, 128), 128)
        pairs = (
            (wu_hbm.at[0, :, pl.ds(lo, 128)], WU.at[slot, up_rows, pl.ds(0, 128)]),
            (wu_hbm.at[0, :, pl.ds(hi, 128)], WU.at[slot, up_rows, pl.ds(128, 128)]),
            (wd_hbm.at[0, pl.ds(lo, 128), :], WD.at[slot, down_rows, :]),
        )
        for s, d in pairs:
            pltpu.make_async_remote_copy(
                s, d, w_send.at[slot], w_recv.at[slot], device_id=dev(rep, mate), device_id_type=MESH_ID).start()
        for s, d in pairs:
            pltpu.make_async_copy(s, d, w_local.at[slot]).start()

    def wait_w(t):
        slot = t % W_SLOTS
        ref = WU.at[slot]
        for sem in (w_local, w_recv, w_send):
            pltpu.make_async_copy(ref, ref, sem.at[slot]).wait()

    with jax.named_scope("entry"):
        pl.semaphore_wait(barrier, 10)
    start_w(0)
    if n_ticks > 1:
        start_w(1)

    mb = min(128, tok)
    clean = MIN_LEN if tok > MIN_LEN else 0

    def mask_micro(k):
        landed(DY, k, in_sem.at[n_micro + k])
        n_valid = len_ref[k]

        def mask_rows(s, carry):
            rows = pl.ds(pl.multiple_of(k * tok + clean + s * mb, mb), mb)
            at = clean + s * mb + lax.broadcasted_iota(jnp.int32, (mb, LANES), 0)
            keep = jnp.where(at < n_valid, 1.0, 0.0).astype(BF16)
            for c in range(n_cols):
                DY[c, rows, :] = DY[c, rows, :] * keep
            return carry

        lax.fori_loop(0, (tok - clean) // mb, mask_rows, 0)

    def wide(ref, rows, lo, hi):
        return jnp.concatenate([ref[c, rows, :] for c in range(lo, hi)], axis=1)

    cb = min(256, n_tok // 2)

    def hidden(t, lo, hi, turn=False):
        slot = t % W_SLOTS
        for at in range(lo, hi, cb):
            rows = pl.ds(at, cb)
            if turn:
                for c in range(n_cols):
                    XT[pl.ds(c * LANES, LANES), rows] = X[c, rows, :].T
            h = jnp.dot(wide(X, rows, 0, n_cols), WU[slot], preferred_element_type=F32).astype(BF16).astype(F32)
            da = lax.dot_general(wide(DY, rows, 0, n_cols), WD[slot], NT_DIMS, preferred_element_type=F32)
            a, slope = gelu_and_slope(h)
            AT[:, rows] = a.astype(BF16).T
            DH[rows, :] = (da * slope).astype(BF16)

    def free_w(t):
        @pl.when(t + W_SLOTS < n_ticks)
        def _():
            pl.semaphore_signal(w_credit, inc=1, device_id=dev(rep, mate), device_id_type=MESH_ID)

    def more_w(t):
        @pl.when((t < n_ticks) & (t >= W_SLOTS))
        def _():
            pl.semaphore_wait(w_credit, 1)

        @pl.when(t < n_ticks)
        def _():
            start_w(t)

    def send_to_mate(t, part):
        slot = t % P_SLOTS
        if part == 0:
            src, dst = SU.at[slot, pl.ds(pl.multiple_of(mate * 512, 512), 512)], RU.at[slot]
        else:
            src, dst = SD.at[slot, pl.ds(pl.multiple_of(mate * 128, 128), 128)], RD.at[slot]
        pltpu.make_async_remote_copy(
            src, dst, p_send.at[slot], p_recv.at[slot], device_id=dev(rep, mate), device_id_type=MESH_ID).start()

    def take_pair_room(t):
        @pl.when(t >= P_SLOTS)
        def _():
            pl.semaphore_wait(r_credit, 1)

    def up(t):
        slot = t % P_SLOTS
        for s in range(2):
            rows = pl.ds(s * 512, 512)
            SU[slot, rows, :] = jnp.dot(XT[rows, :], DH[...], preferred_element_type=F32)

    def down(t):
        slot = t % P_SLOTS
        for s in range(2):
            cols = pl.ds(s * 512, 512)
            SD[slot, :, cols] = jnp.dot(AT[...], wide(DY, slice(None), 4 * s, 4 * s + 4), preferred_element_type=F32)

    def send(sent, src, dst, recv, to):
        pltpu.make_async_remote_copy(
            src, dst, sent, recv, device_id=dev(to, me), device_id_type=MESH_ID).start()

    def pair_stage(t):
        slot = t % P_SLOTS
        whole = SU.at[slot]
        pltpu.make_async_copy(whole, whole, p_recv.at[slot]).wait()
        own = pl.ds(pl.multiple_of(me * 512, 512), 512)
        for s in range(2):
            cols = pl.ds(s * 128, 128)
            GU[:, pl.ds(s * half_ff + t * 128, 128)] = SU[slot, own, cols] + RU[slot, :, cols]
        own = pl.ds(pl.multiple_of(me * 128, 128), 128)
        GD[pl.ds(t * 128, 128), :] = SD[slot, own, :] + RD[slot]
        pltpu.make_async_copy(whole, whole, p_send.at[slot]).wait()
        if t + P_SLOTS < n_ticks:
            pl.semaphore_signal(r_credit, inc=1, device_id=dev(rep, mate), device_id_type=MESH_ID)
        rs_a(t, 0)

    def rs_a(t, p):
        sent = (send0 if p == 0 else send1).at[t]
        m, off = PH_ROWS[p], PH_OFF[p]
        if p > 0 and t in DIRECT:
            for k in (2, 1, 3):
                for g, axes, dirs in subs_of(t):
                    a = axes[p]
                    src = g_part(g, coord[axes[0]], row_in_quarter(axes, p) + quarter[a][k] * m, m)
                    send(sent, src, r_part(g, off + (k - 1) * m, m), rs2.at[t * 3 + p], near[a][k])
            return
        for relay in (True, False):
            for g, axes, dirs in subs_of(t):
                a, d = axes[p], dirs[p]
                q = quarter[a][2 if relay else -d % RING]
                src = g_part(g, q, 0, m) if p == 0 else g_part(g, coord[axes[0]], row_in_quarter(axes, p) + q * m, m)
                if relay:
                    send(sent, src, r_part(g, off, m), rs1.at[t * 3 + p], near[a][d])
                else:
                    send(sent, src, r_part(g, off + m, m), rs2.at[t * 3 + p], near[a][-d])

    def rs_b(t, p):
        sent = (send0 if p == 0 else send1).at[t]
        m, off = PH_ROWS[p], PH_OFF[p]
        wait_rows(rs1.at[t * 3 + p], SUBS * m)
        for g, axes, dirs in subs_of(t):
            a, d = axes[p], dirs[p]
            q = quarter[a][d % RING]
            part = g_part(g, q, 0, m) if p == 0 else g_part(g, coord[axes[0]], row_in_quarter(axes, p) + q * m, m)
            part[...] = part[...] + r_part(g, off, m)[...]
            send(sent, part, r_part(g, off + 2 * m, m), rs2.at[t * 3 + p], near[a][d])

    def rs_c(t, p):
        m, off = PH_ROWS[p], PH_OFF[p]
        straight = p > 0 and t in DIRECT
        wait_rows(rs2.at[t * 3 + p], (3 if straight else 2) * SUBS * m)
        for g, axes, dirs in subs_of(t):
            row = 0 if p == 0 else row_in_quarter(axes, p) + coord[axes[p]] * m
            part = g_part(g, coord[axes[0]], row, m)
            out = e_part(g, row, m) if p == 2 else part
            total = part[...] + (r_part(g, off + m, m)[...] + r_part(g, off + 2 * m, m)[...])
            out[...] = total + r_part(g, off, m)[...] if straight else total
        if p < 2:
            rs_a(t, p + 1)
        else:
            ag_a(t, 2)
        if p == 1:
            wait_rows(send0.at[t], 3 * SUBS * PH_ROWS[0])
            for a in sorted({axes[0] for _, axes, _ in subs_of(t)}):
                for d in (1, -1):
                    pl.semaphore_signal(g_free.at[t], inc=1, device_id=dev(near[a][d], me), device_id_type=MESH_ID)

    def ag_part(g, axes, p, q):
        if p == 0:
            return g_part(g, q, 0, PH_ROWS[0])
        return e_part(g, row_in_quarter(axes, p) + q * PH_ROWS[p], PH_ROWS[p])

    def ag_a(t, p):
        if p == 0:
            pl.semaphore_wait(g_free.at[t], 2 * len({axes[0] for _, axes, _ in subs_of(t)}))
        if p > 0 and t in DIRECT:
            for k in (2, 1, 3):
                for g, axes, dirs in subs_of(t):
                    part = ag_part(g, axes, p, coord[axes[p]])
                    send(out_send.at[t], part, part, ag2.at[t * 3 + p], near[axes[p]][k])
            return
        for recv, sign in ((ag1, 1), (ag2, -1)):
            for g, axes, dirs in subs_of(t):
                a, d = axes[p], dirs[p]
                part = ag_part(g, axes, p, coord[a])
                src = e_part(g, 0, PH_ROWS[0]) if p == 0 else part
                send(out_send.at[t], src, part, recv.at[t * 3 + p], near[a][sign * d])
        if p == 0:
            wait_rows(send1.at[t], 3 * SUBS * (PH_ROWS[1] + PH_ROWS[2]))
            for g, axes, dirs in subs_of(t):
                g_part(g, coord[axes[0]], 0, PH_ROWS[0])[...] = e_part(g, 0, PH_ROWS[0])[...]

    def ag_b(t, p):
        wait_rows(ag1.at[t * 3 + p], SUBS * PH_ROWS[p])
        for g, axes, dirs in subs_of(t):
            a, d = axes[p], dirs[p]
            part = ag_part(g, axes, p, quarter[a][-d % RING])
            send(out_send.at[t], part, part, ag2.at[t * 3 + p], near[a][d])

    def ag_c(t, p):
        wait_rows(ag2.at[t * 3 + p], (3 if p > 0 and t in DIRECT else 2) * SUBS * PH_ROWS[p])
        if p > 0:
            ag_a(t, p - 1)

    def run(ops):
        for s, t in ops:
            name = STAGES[s]
            with jax.named_scope(name):
                if name == "pair":
                    pair_stage(t)
                else:
                    p = int(name[2])
                    {"rsb": rs_b, "rsc": rs_c, "agb": ag_b, "agc": ag_c}[name[:2] + name[3]](t, p)

    slots = program(n_ticks)

    def pick(t, first, lo, hi):
        lists = [slots[first(k)] for k in range(lo, hi)]
        if not any(lists):
            return
        if hi - lo == 1:
            run(lists[0])
            return
        mid = (lo + hi) // 2
        pl.when(t < mid)(lambda: pick(t, first, lo, mid))
        pl.when(t >= mid)(lambda: pick(t, first, mid, hi))

    n_half = n_tok // 2
    for part in range(2):
        for k in range(part * n_micro // 2, (part + 1) * n_micro // 2):
            landed(X, k, in_sem.at[k])
            with jax.named_scope("mask"):
                mask_micro(k)
        if part == 0:
            with jax.named_scope("wwait"):
                wait_w(0)
        with jax.named_scope("hidfirst"):
            hidden(0, part * n_half, (part + 1) * n_half, turn=True)
        run(slots[part])
    free_w(0)
    more_w(2)
    with jax.named_scope("upfirst"):
        up(0)
    send_to_mate(0, 0)
    run(slots[2])
    with jax.named_scope("downfirst"):
        down(0)
    send_to_mate(0, 1)
    run(slots[3])

    def tick(t, carry):
        with jax.named_scope("wwait"):
            wait_w(t)
        with jax.named_scope("hidden"):
            hidden(t, 0, n_tok)
        free_w(t)
        pick(t, lambda k: OPENING + 2 * k - 2, 1, n_ticks)
        more_w(t + 2)
        take_pair_room(t)
        with jax.named_scope("grad"):
            up(t)
            down(t)
            send_to_mate(t, 0)
            send_to_mate(t, 1)
        pick(t, lambda k: OPENING + 2 * k - 1, 1, n_ticks)
        return carry

    lax.fori_loop(1, n_ticks, tick, 0)
    run(slots[-1])
    for t in range(n_ticks):
        wait_rows(out_send.at[t], SUBS * R_ROWS)


FLUSH = 8


def flush(gu, gd, gu_hbm, gd_hbm, sem):
    copies = []
    for k in range(FLUSH):
        for ref, out, s in ((gu, gu_hbm, 0), (gd, gd_hbm, 1)):
            rows = pl.ds(k * (ref.shape[0] // FLUSH), ref.shape[0] // FLUSH)
            copies.append(pltpu.make_async_copy(ref.at[rows], out.at[0, rows], sem.at[2 * k + s]))
    for copy in copies:
        copy.start()
    for copy in copies:
        copy.wait()


def solution(mesh):
    tok_spec = P(None, ("model", "replica", "fsdp"), None)
    len_spec = P(None, ("model", "replica", "fsdp"))
    w_spec = P(None, ("model", "fsdp"), None)

    def device_grads(x_in, dy_out, lengths, w_up, w_down):
        n_micro, tok, d = x_in.shape
        n_tok = n_micro * tok
        d_ff = w_up.shape[2]
        n_ticks = d_ff // FC
        any_spec = pl.BlockSpec(memory_space=pl.ANY)
        dma = pltpu.SemaphoreType.DMA
        regular = pltpu.SemaphoreType.REGULAR
        sems = [
            dma((2 * n_micro,)),
            dma((W_SLOTS,)),
            dma((W_SLOTS,)),
            dma((W_SLOTS,)),
            dma((P_SLOTS,)),
            dma((P_SLOTS,)),
            dma((3 * n_ticks,)),
            dma((3 * n_ticks,)),
            dma((3 * n_ticks,)),
            dma((3 * n_ticks,)),
            dma((n_ticks,)),
            dma((n_ticks,)),
            dma((n_ticks,)),
            regular((n_ticks,)),
            regular,
            regular,
        ]
        gu, gd = pl.pallas_call(
            functools.partial(kernel, n_ticks, n_tok, n_micro, sems),
            out_shape=(
                pltpu.VMEM((d // 2, d_ff), F32),
                pltpu.VMEM((d_ff // 2, d), F32),
            ),
            in_specs=[any_spec, any_spec, pl.BlockSpec(memory_space=pltpu.SMEM), any_spec, any_spec],
            out_specs=(pl.BlockSpec(memory_space=pltpu.VMEM),) * 2,
            scratch_shapes=[
                pltpu.VMEM((d // LANES, n_tok, LANES), BF16),
                pltpu.VMEM((d // LANES, n_tok, LANES), BF16),
                pltpu.VMEM((d, n_tok), BF16),
                pltpu.VMEM((W_SLOTS, d, FC), BF16),
                pltpu.VMEM((W_SLOTS, FC, d), BF16),
                pltpu.VMEM((FC, n_tok), BF16),
                pltpu.VMEM((n_tok, FC), BF16),
                pltpu.VMEM((P_SLOTS, d, FC), F32),
                pltpu.VMEM((P_SLOTS, FC, d), F32),
                pltpu.VMEM((P_SLOTS, d // 2, FC), F32),
                pltpu.VMEM((P_SLOTS, FC // 2, d), F32),
                pltpu.VMEM((n_ticks * SUBS * R_ROWS, 128), F32),
                pltpu.VMEM((n_ticks * SUBS * PH_ROWS[0], 128), F32),
            ],
            compiler_params=pltpu.CompilerParams(
                collective_id=0, has_side_effects=True, vmem_limit_bytes=67043328 - (16 << 20)),
            name="grads",
        )(x_in, dy_out, lengths.reshape(n_micro), w_up, w_down)
        vmem = pl.BlockSpec(memory_space=pltpu.VMEM)
        return pl.pallas_call(
            flush,
            out_shape=(
                jax.ShapeDtypeStruct(w_up.shape, F32),
                jax.ShapeDtypeStruct(w_down.shape, F32),
            ),
            in_specs=[vmem, vmem],
            out_specs=(any_spec, any_spec),
            scratch_shapes=[dma((2 * FLUSH,))],
            compiler_params=pltpu.CompilerParams(vmem_limit_bytes=1 << 20),
            name="flush",
        )(pltpu.with_memory_space_constraint(gu, pltpu.VMEM), pltpu.with_memory_space_constraint(gd, pltpu.VMEM))

    return jax.shard_map(device_grads, mesh=mesh, in_specs=(tok_spec, tok_spec, len_spec, w_spec, w_spec), out_specs=(w_spec, w_spec), check_vma=False)
```

```python
import functools

import jax
import jax.numpy as jnp
from jax import lax
from jax.experimental import pallas as pl
from jax.experimental.pallas import tpu as pltpu
from jax.sharding import PartitionSpec as P

F32, BF16 = jnp.float32, jnp.bfloat16
MESH_ID = pl.DeviceIdType.MESH
SQRT_2_OVER_PI = 0.7978845608028654
CUBIC = 0.044715
NT_DIMS = (((1,), (1,)), ((), ()))

FC = 256
RING = 4
SUBS = 4
PH_ROWS = (128, 32, 8)
PH_OFF = (0, 384, 480)
R_ROWS = 504
W_SLOTS = 3
P_SLOTS = 2
STAGES = ("pair", "rs0b", "rs0c", "rs1b", "rs1c", "rs2b", "rs2c", "ag2b", "ag2c", "ag1b", "ag1c", "ag0b", "ag0c")

OPENING = 4
MIN_LEN = 128
TABLE = (
    (),
    (),
    (),
    (),
    ((0, 0),),
    (),
    ((1, 0),),
    ((0, 1),),
    ((2, 0),),
    ((0, 2), (1, 1),),
    ((4, 0), (0, 3),),
    ((1, 2),),
    ((2, 1), (1, 3), (6, 0),),
    ((2, 2), (0, 4),),
    ((4, 1), (0, 5), (2, 3),),
    ((4, 2), (8, 0), (1, 4),),
    ((6, 1), (1, 5), (0, 6),),
    ((4, 3), (6, 2), (10, 0),),
    ((8, 1), (0, 7),),
    ((2, 5), (2, 4), (1, 6),),
    ((6, 3), (8, 2), (0, 8),),
    ((3, 5), (10, 1),),
    ((2, 6), (3, 4), (0, 9), (8, 3),),
    ((1, 7), (4, 5), (1, 8), (10, 2),),
    ((4, 4), (3, 6),),
    ((1, 9), (0, 10),),
    ((2, 8), (2, 7), (5, 4), (5, 5), (10, 3), (0, 11),),
    ((1, 10),),
    ((3, 8), (4, 6), (3, 7), (11, 0), (2, 9), (0, 12),),
    ((1, 11),),
    ((6, 5), (5, 6), (2, 10), (4, 7), (4, 8), (6, 4), (0, 13), (11, 2),),
    ((3, 9), (6, 6), (2, 11), (5, 7), (3, 10), (11, 1), (5, 8), (7, 4), (1, 12), (0, 14),),
    ((6, 7), (7, 6), (3, 11), (4, 9), (7, 5), (4, 10), (8, 4), (11, 3), (1, 13),),
    (),
    ((2, 12), (7, 7), (6, 8), (1, 14), (5, 9), (4, 11), (5, 10), (9, 4), (8, 5), (12, 2), (0, 15), (8, 6), (7, 8), (8, 7), (6, 10), (2, 13), (2, 14), (5, 11), (6, 9), (3, 12), (9, 5), (1, 15), (10, 4), (3, 14), (3, 13), (7, 10), (7, 9), (6, 11), (4, 12), (8, 8), (9, 6), (2, 15), (10, 5), (7, 11), (5, 12), (9, 8), (4, 13), (4, 14), (8, 9), (8, 10), (3, 15), (9, 7), (10, 6), (5, 14), (12, 3), (5, 13), (8, 11), (6, 12), (12, 0), (11, 5), (4, 15), (9, 10), (10, 7), (9, 9), (6, 14), (6, 13), (11, 6), (7, 12), (9, 11), (5, 15), (10, 8), (11, 4), (12, 1), (8, 12), (7, 13), (7, 14), (6, 15), (10, 9), (10, 10), (9, 12), (7, 15), (8, 13), (8, 14), (11, 9), (11, 7), (11, 8), (12, 6), (8, 15), (9, 13), (12, 5), (9, 14), (10, 11), (10, 12), (9, 15), (10, 14), (12, 7), (10, 13), (12, 9), (10, 15), (11, 10), (12, 8), (11, 12), (11, 11), (11, 15), (11, 14), (12, 10), (11, 13), (12, 15), (12, 4), (12, 11), (12, 12), (12, 14), (12, 13),),
)
DIRECT = (0, 1, 2, 3)
LANES = 128
SHAPES = (
    3, 0, 0, 6, 6, 6, 0, 2, 0, 6, 6, 6, 0, 0, 0, 6, 2, 5, 0, 0, 0, 6, 2, 6, 6, 0, 0, 6, 6, 7, 0, 0,
    0, 6, 6, 6, 0, 6, 0, 6, 6, 6, 0, 0, 6, 6, 6, 6, 5, 0, 4, 6, 6, 6, 0, 0, 5, 6, 6, 6, 0, 0, 4, 6,
)


def stages_of(t):
    return [k for k, n in enumerate(STAGES) if not (t in DIRECT and n in ("rs1b", "rs2b", "ag2b", "ag1b"))]


def program(n_ticks):
    if n_ticks == 16 and TABLE:
        return TABLE
    last = OPENING + 2 * (n_ticks - 1)
    slots = [[] for _ in range(last + 1)]
    for t in range(n_ticks):
        for k, s in enumerate(stages_of(t)):
            slots[min(OPENING + 2 * t + k, last)].append((s, t))
    slots[-1].sort()
    return slots


def gelu_and_slope(u):
    u2 = u * u
    half = 0.5 + 0.5 * jnp.tanh(u * (SQRT_2_OVER_PI + (CUBIC * SQRT_2_OVER_PI) * u2))
    a = u * half
    return a, half + (a * (1.0 - half)) * (2.0 * SQRT_2_OVER_PI + (6.0 * CUBIC * SQRT_2_OVER_PI) * u2)


def subs_of(t):
    blocks = []
    for g in range(SUBS * t, SUBS * t + SUBS):
        code, a = SHAPES[g % len(SHAPES)], g % 3
        b, c = ((a + 1) % 3, (a + 2) % 3) if code % 2 == 0 else ((a + 2) % 3, (a + 1) % 3)
        dirs = (1 if g // 3 % 2 == 0 else -1, -1 if code & 2 else 1, -1 if code & 4 else 1)
        blocks.append((g, (a, b, c), dirs))
    return blocks


def kernel(n_ticks, n_tok, n_micro, sems, *refs):
    pl.run_scoped(functools.partial(body, n_ticks, n_tok, n_micro, refs), *sems)


def body(n_ticks, n_tok, n_micro, refs,
         in_sem, w_local, w_send, w_recv, p_send, p_recv, rs1, rs2, ag1, ag2, send0, send1, out_send,
         g_free, w_credit, r_credit):
    (x_hbm, dy_hbm, len_ref, wu_hbm, wd_hbm, GU, GD,
     X, DY, XT, WU, WD, AT, DH, SU, SD, RU, RD, R, E) = refs
    tok = n_tok // n_micro
    half_ff = n_ticks * 128
    rep = lax.axis_index("replica")
    me = lax.axis_index("fsdp")
    mate = 1 - me

    def dev(replica, core):
        return (0, replica, core)

    strides = [RING**a for a in range(3)]
    coord = [(rep // s) % RING for s in strides]
    quarter = [[coord[a]] + [(coord[a] + k) % RING for k in range(1, RING)] for a in range(3)]
    near = [{d: rep + strides[a] * (quarter[a][d % RING] - coord[a]) for d in (1, -1, 2, 3)} for a in range(3)]

    def row_in_quarter(axes, phase):
        row = 0
        for p in range(1, phase):
            row = row + coord[axes[p]] * PH_ROWS[p]
        return row

    def g_part(g, q, row, n):
        t, s = g // SUBS, g % SUBS
        if s < 2:
            start = q * 128 + row
            return GU.at[pl.ds(pl.multiple_of(start, 8), n), pl.ds(s * half_ff + t * 128, 128)]
        start = t * 128 + row
        if not isinstance(start, int):
            start = pl.multiple_of(start, 8)
        return GD.at[pl.ds(start, n), pl.ds(pl.multiple_of((s - 2) * 512 + q * 128, 128), 128)]

    def r_part(g, start, n):
        return R.at[pl.ds(g * R_ROWS + start, n)]

    def e_part(g, row, n):
        start = g * PH_ROWS[0] + row
        if not isinstance(start, int):
            start = pl.multiple_of(start, 8)
        return E.at[pl.ds(start, n)]

    def wait_rows(sem, n):
        ref = R.at[pl.ds(0, n)]
        pltpu.make_async_copy(ref, ref, sem).wait()

    barrier = pltpu.get_barrier_semaphore()
    for a in range(3):
        for d in (1, -1, 2):
            pl.semaphore_signal(barrier, inc=1, device_id=dev(near[a][d], me), device_id_type=MESH_ID)
    pl.semaphore_signal(barrier, inc=1, device_id=dev(rep, mate), device_id_type=MESH_ID)

    n_cols = X.shape[0]

    def x_copy(k):
        return [pltpu.make_async_copy(x_hbm.at[k, :, pl.ds(c * LANES, LANES)], X.at[c, pl.ds(k * tok, tok)], in_sem.at[k]) for c in range(n_cols)]

    def dy_copy(k):
        return [pltpu.make_async_copy(dy_hbm.at[k, :, pl.ds(c * LANES, LANES)], DY.at[c, pl.ds(k * tok, tok)], in_sem.at[n_micro + k]) for c in range(n_cols)]

    def landed(ref, k, sem):
        block = ref.at[:, pl.ds(k * tok, tok)]
        pltpu.make_async_copy(block, block, sem).wait()

    def w_parts(t):
        slot = t % W_SLOTS
        lo = pl.multiple_of(t * 128, 128)
        hi = pl.multiple_of(half_ff + t * 128, 128)
        up_rows = pl.ds(pl.multiple_of(me * 512, 512), 512)
        down_rows = pl.ds(pl.multiple_of(me * 128, 128), 128)
        return (
            (wu_hbm.at[0, :, pl.ds(lo, 128)], WU.at[slot, up_rows, pl.ds(0, 128)]),
            (wu_hbm.at[0, :, pl.ds(hi, 128)], WU.at[slot, up_rows, pl.ds(128, 128)]),
            (wd_hbm.at[0, pl.ds(lo, 128), :], WD.at[slot, down_rows, :]),
        )

    def load_w(t):
        for s, d in w_parts(t):
            pltpu.make_async_copy(s, d, w_local.at[t % W_SLOTS]).start()

    def push_w(t, from_vmem):
        for s, d in w_parts(t):
            pltpu.make_async_remote_copy(
                d if from_vmem else s, d, w_send.at[t % W_SLOTS], w_recv.at[t % W_SLOTS],
                device_id=dev(rep, mate), device_id_type=MESH_ID).start()

    def start_w(t):
        push_w(t, False)
        load_w(t)

    def wait_w(t, sems=None):
        slot = t % W_SLOTS
        ref = WU.at[slot]
        for sem in sems or (w_local, w_recv, w_send):
            pltpu.make_async_copy(ref, ref, sem.at[slot]).wait()

    load_w(0)
    for k in range(n_micro):
        for copy in x_copy(k):
            copy.start()
    for k in range(n_micro):
        for copy in dy_copy(k):
            copy.start()


    with jax.named_scope("entry"):
        pl.semaphore_wait(barrier, 10)
    wait_w(0, (w_local,))
    push_w(0, True)
    if n_ticks > 1:
        start_w(1)

    mb = min(128, tok)
    clean = MIN_LEN if tok > MIN_LEN else 0

    def mask_micro(k):
        landed(DY, k, in_sem.at[n_micro + k])
        n_valid = len_ref[k]

        def mask_rows(s, carry):
            rows = pl.ds(pl.multiple_of(k * tok + clean + s * mb, mb), mb)
            at = clean + s * mb + lax.broadcasted_iota(jnp.int32, (mb, LANES), 0)
            keep = jnp.where(at < n_valid, 1.0, 0.0).astype(BF16)
            for c in range(n_cols):
                DY[c, rows, :] = DY[c, rows, :] * keep
            return carry

        lax.fori_loop(0, (tok - clean) // mb, mask_rows, 0)

    def wide(ref, rows, lo, hi):
        return jnp.concatenate([ref[c, rows, :] for c in range(lo, hi)], axis=1)

    cb = min(256, n_tok // 2)

    def hidden(t, lo, hi, turn=False):
        slot = t % W_SLOTS
        for at in range(lo, hi, cb):
            rows = pl.ds(at, cb)
            if turn:
                for c in range(n_cols):
                    XT[pl.ds(c * LANES, LANES), rows] = X[c, rows, :].T
            h = jnp.dot(wide(X, rows, 0, n_cols), WU[slot], preferred_element_type=F32).astype(BF16).astype(F32)
            da = lax.dot_general(wide(DY, rows, 0, n_cols), WD[slot], NT_DIMS, preferred_element_type=F32)
            a, slope = gelu_and_slope(h)
            AT[:, rows] = a.astype(BF16).T
            DH[rows, :] = (da * slope).astype(BF16)

    def free_w(t):
        @pl.when(t + W_SLOTS < n_ticks)
        def _():
            pl.semaphore_signal(w_credit, inc=1, device_id=dev(rep, mate), device_id_type=MESH_ID)

    def more_w(t):
        @pl.when((t < n_ticks) & (t >= W_SLOTS))
        def _():
            pl.semaphore_wait(w_credit, 1)

        @pl.when(t < n_ticks)
        def _():
            start_w(t)

    def send_to_mate(t, part):
        slot = t % P_SLOTS
        if part == 0:
            src, dst = SU.at[slot, pl.ds(pl.multiple_of(mate * 512, 512), 512)], RU.at[slot]
        else:
            src, dst = SD.at[slot, pl.ds(pl.multiple_of(mate * 128, 128), 128)], RD.at[slot]
        pltpu.make_async_remote_copy(
            src, dst, p_send.at[slot], p_recv.at[slot], device_id=dev(rep, mate), device_id_type=MESH_ID).start()

    def take_pair_room(t):
        @pl.when(t >= P_SLOTS)
        def _():
            pl.semaphore_wait(r_credit, 1)

    def up(t):
        slot = t % P_SLOTS
        for s in range(2):
            rows = pl.ds(s * 512, 512)
            SU[slot, rows, :] = jnp.dot(XT[rows, :], DH[...], preferred_element_type=F32)

    def down(t):
        slot = t % P_SLOTS
        for s in range(2):
            cols = pl.ds(s * 512, 512)
            SD[slot, :, cols] = jnp.dot(AT[...], wide(DY, slice(None), 4 * s, 4 * s + 4), preferred_element_type=F32)

    def send(sent, src, dst, recv, to):
        pltpu.make_async_remote_copy(
            src, dst, sent, recv, device_id=dev(to, me), device_id_type=MESH_ID).start()

    def pair_stage(t):
        slot = t % P_SLOTS
        whole = SU.at[slot]
        pltpu.make_async_copy(whole, whole, p_recv.at[slot]).wait()
        own = pl.ds(pl.multiple_of(me * 512, 512), 512)
        for s in range(2):
            cols = pl.ds(s * 128, 128)
            GU[:, pl.ds(s * half_ff + t * 128, 128)] = SU[slot, own, cols] + RU[slot, :, cols]
        own = pl.ds(pl.multiple_of(me * 128, 128), 128)
        GD[pl.ds(t * 128, 128), :] = SD[slot, own, :] + RD[slot]
        pltpu.make_async_copy(whole, whole, p_send.at[slot]).wait()
        if t + P_SLOTS < n_ticks:
            pl.semaphore_signal(r_credit, inc=1, device_id=dev(rep, mate), device_id_type=MESH_ID)
        rs_a(t, 0)

    def rs_a(t, p):
        sent = (send0 if p == 0 else send1).at[t]
        m, off = PH_ROWS[p], PH_OFF[p]
        if p > 0 and t in DIRECT:
            for k in (2, 1, 3):
                for g, axes, dirs in subs_of(t):
                    a = axes[p]
                    src = g_part(g, coord[axes[0]], row_in_quarter(axes, p) + quarter[a][k] * m, m)
                    send(sent, src, r_part(g, off + (k - 1) * m, m), rs2.at[t * 3 + p], near[a][k])
            return
        for relay in (True, False):
            for g, axes, dirs in subs_of(t):
                a, d = axes[p], dirs[p]
                q = quarter[a][2 if relay else -d % RING]
                src = g_part(g, q, 0, m) if p == 0 else g_part(g, coord[axes[0]], row_in_quarter(axes, p) + q * m, m)
                if relay:
                    send(sent, src, r_part(g, off, m), rs1.at[t * 3 + p], near[a][d])
                else:
                    send(sent, src, r_part(g, off + m, m), rs2.at[t * 3 + p], near[a][-d])

    def rs_b(t, p):
        sent = (send0 if p == 0 else send1).at[t]
        m, off = PH_ROWS[p], PH_OFF[p]
        wait_rows(rs1.at[t * 3 + p], SUBS * m)
        for g, axes, dirs in subs_of(t):
            a, d = axes[p], dirs[p]
            q = quarter[a][d % RING]
            part = g_part(g, q, 0, m) if p == 0 else g_part(g, coord[axes[0]], row_in_quarter(axes, p) + q * m, m)
            part[...] = part[...] + r_part(g, off, m)[...]
            send(sent, part, r_part(g, off + 2 * m, m), rs2.at[t * 3 + p], near[a][d])

    def rs_c(t, p):
        m, off = PH_ROWS[p], PH_OFF[p]
        straight = p > 0 and t in DIRECT
        wait_rows(rs2.at[t * 3 + p], (3 if straight else 2) * SUBS * m)
        for g, axes, dirs in subs_of(t):
            row = 0 if p == 0 else row_in_quarter(axes, p) + coord[axes[p]] * m
            part = g_part(g, coord[axes[0]], row, m)
            out = e_part(g, row, m) if p == 2 else part
            total = part[...] + (r_part(g, off + m, m)[...] + r_part(g, off + 2 * m, m)[...])
            out[...] = total + r_part(g, off, m)[...] if straight else total
        if p < 2:
            rs_a(t, p + 1)
        else:
            ag_a(t, 2)
        if p == 1:
            wait_rows(send0.at[t], 3 * SUBS * PH_ROWS[0])
            for a in sorted({axes[0] for _, axes, _ in subs_of(t)}):
                for d in (1, -1):
                    pl.semaphore_signal(g_free.at[t], inc=1, device_id=dev(near[a][d], me), device_id_type=MESH_ID)

    def ag_part(g, axes, p, q):
        if p == 0:
            return g_part(g, q, 0, PH_ROWS[0])
        return e_part(g, row_in_quarter(axes, p) + q * PH_ROWS[p], PH_ROWS[p])

    def ag_a(t, p):
        if p == 0:
            pl.semaphore_wait(g_free.at[t], 2 * len({axes[0] for _, axes, _ in subs_of(t)}))
        if p > 0 and t in DIRECT:
            for k in (2, 1, 3):
                for g, axes, dirs in subs_of(t):
                    part = ag_part(g, axes, p, coord[axes[p]])
                    send(out_send.at[t], part, part, ag2.at[t * 3 + p], near[axes[p]][k])
            return
        for recv, sign in ((ag1, 1), (ag2, -1)):
            for g, axes, dirs in subs_of(t):
                a, d = axes[p], dirs[p]
                part = ag_part(g, axes, p, coord[a])
                src = e_part(g, 0, PH_ROWS[0]) if p == 0 else part
                send(out_send.at[t], src, part, recv.at[t * 3 + p], near[a][sign * d])
        if p == 0:
            wait_rows(send1.at[t], 3 * SUBS * (PH_ROWS[1] + PH_ROWS[2]))
            for g, axes, dirs in subs_of(t):
                g_part(g, coord[axes[0]], 0, PH_ROWS[0])[...] = e_part(g, 0, PH_ROWS[0])[...]

    def ag_b(t, p):
        wait_rows(ag1.at[t * 3 + p], SUBS * PH_ROWS[p])
        for g, axes, dirs in subs_of(t):
            a, d = axes[p], dirs[p]
            part = ag_part(g, axes, p, quarter[a][-d % RING])
            send(out_send.at[t], part, part, ag2.at[t * 3 + p], near[a][d])

    def ag_c(t, p):
        wait_rows(ag2.at[t * 3 + p], (3 if p > 0 and t in DIRECT else 2) * SUBS * PH_ROWS[p])
        if p > 0:
            ag_a(t, p - 1)

    def run(ops):
        for s, t in ops:
            name = STAGES[s]
            with jax.named_scope(name):
                if name == "pair":
                    pair_stage(t)
                else:
                    p = int(name[2])
                    {"rsb": rs_b, "rsc": rs_c, "agb": ag_b, "agc": ag_c}[name[:2] + name[3]](t, p)

    slots = program(n_ticks)

    def pick(t, first, lo, hi):
        lists = [slots[first(k)] for k in range(lo, hi)]
        if not any(lists):
            return
        if hi - lo == 1:
            run(lists[0])
            return
        mid = (lo + hi) // 2
        pl.when(t < mid)(lambda: pick(t, first, lo, mid))
        pl.when(t >= mid)(lambda: pick(t, first, mid, hi))

    n_half = n_tok // 2
    for part in range(2):
        for k in range(part * n_micro // 2, (part + 1) * n_micro // 2):
            landed(X, k, in_sem.at[k])
            with jax.named_scope("mask"):
                mask_micro(k)
        if part == 0:
            with jax.named_scope("wwait"):
                wait_w(0, (w_recv, w_send))
        with jax.named_scope("hidfirst"):
            hidden(0, part * n_half, (part + 1) * n_half, turn=True)
        run(slots[part])
    free_w(0)
    more_w(2)
    with jax.named_scope("upfirst"):
        up(0)
    send_to_mate(0, 0)
    run(slots[2])
    with jax.named_scope("downfirst"):
        down(0)
    send_to_mate(0, 1)
    run(slots[3])

    def tick(t, carry):
        with jax.named_scope("wwait"):
            wait_w(t)
        with jax.named_scope("hidden"):
            hidden(t, 0, n_tok)
        free_w(t)
        pick(t, lambda k: OPENING + 2 * k - 2, 1, n_ticks)
        more_w(t + 2)
        take_pair_room(t)
        with jax.named_scope("grad"):
            up(t)
            down(t)
            send_to_mate(t, 0)
            send_to_mate(t, 1)
        pick(t, lambda k: OPENING + 2 * k - 1, 1, n_ticks)
        return carry

    lax.fori_loop(1, n_ticks, tick, 0)
    run(slots[-1])
    for t in range(n_ticks):
        wait_rows(out_send.at[t], SUBS * R_ROWS)


FLUSH = 8


def flush(gu, gd, gu_hbm, gd_hbm, sem):
    copies = []
    for k in range(FLUSH):
        for ref, out, s in ((gu, gu_hbm, 0), (gd, gd_hbm, 1)):
            rows = pl.ds(k * (ref.shape[0] // FLUSH), ref.shape[0] // FLUSH)
            copies.append(pltpu.make_async_copy(ref.at[rows], out.at[0, rows], sem.at[2 * k + s]))
    for copy in copies:
        copy.start()
    for copy in copies:
        copy.wait()


def solution(mesh):
    tok_spec = P(None, ("model", "replica", "fsdp"), None)
    len_spec = P(None, ("model", "replica", "fsdp"))
    w_spec = P(None, ("model", "fsdp"), None)

    def device_grads(x_in, dy_out, lengths, w_up, w_down):
        n_micro, tok, d = x_in.shape
        n_tok = n_micro * tok
        d_ff = w_up.shape[2]
        n_ticks = d_ff // FC
        any_spec = pl.BlockSpec(memory_space=pl.ANY)
        dma = pltpu.SemaphoreType.DMA
        regular = pltpu.SemaphoreType.REGULAR
        sems = [
            dma((2 * n_micro,)),
            dma((W_SLOTS,)),
            dma((W_SLOTS,)),
            dma((W_SLOTS,)),
            dma((P_SLOTS,)),
            dma((P_SLOTS,)),
            dma((3 * n_ticks,)),
            dma((3 * n_ticks,)),
            dma((3 * n_ticks,)),
            dma((3 * n_ticks,)),
            dma((n_ticks,)),
            dma((n_ticks,)),
            dma((n_ticks,)),
            regular((n_ticks,)),
            regular,
            regular,
        ]
        gu, gd = pl.pallas_call(
            functools.partial(kernel, n_ticks, n_tok, n_micro, sems),
            out_shape=(
                pltpu.VMEM((d // 2, d_ff), F32),
                pltpu.VMEM((d_ff // 2, d), F32),
            ),
            in_specs=[any_spec, any_spec, pl.BlockSpec(memory_space=pltpu.SMEM), any_spec, any_spec],
            out_specs=(pl.BlockSpec(memory_space=pltpu.VMEM),) * 2,
            scratch_shapes=[
                pltpu.VMEM((d // LANES, n_tok, LANES), BF16),
                pltpu.VMEM((d // LANES, n_tok, LANES), BF16),
                pltpu.VMEM((d, n_tok), BF16),
                pltpu.VMEM((W_SLOTS, d, FC), BF16),
                pltpu.VMEM((W_SLOTS, FC, d), BF16),
                pltpu.VMEM((FC, n_tok), BF16),
                pltpu.VMEM((n_tok, FC), BF16),
                pltpu.VMEM((P_SLOTS, d, FC), F32),
                pltpu.VMEM((P_SLOTS, FC, d), F32),
                pltpu.VMEM((P_SLOTS, d // 2, FC), F32),
                pltpu.VMEM((P_SLOTS, FC // 2, d), F32),
                pltpu.VMEM((n_ticks * SUBS * R_ROWS, 128), F32),
                pltpu.VMEM((n_ticks * SUBS * PH_ROWS[0], 128), F32),
            ],
            compiler_params=pltpu.CompilerParams(
                collective_id=0, has_side_effects=True, vmem_limit_bytes=67043328 - (16 << 20)),
            name="grads",
        )(x_in, dy_out, lengths.reshape(n_micro), w_up, w_down)
        vmem = pl.BlockSpec(memory_space=pltpu.VMEM)
        return pl.pallas_call(
            flush,
            out_shape=(
                jax.ShapeDtypeStruct(w_up.shape, F32),
                jax.ShapeDtypeStruct(w_down.shape, F32),
            ),
            in_specs=[vmem, vmem],
            out_specs=(any_spec, any_spec),
            scratch_shapes=[dma((2 * FLUSH,))],
            compiler_params=pltpu.CompilerParams(vmem_limit_bytes=1 << 20),
            name="flush",
        )(pltpu.with_memory_space_constraint(gu, pltpu.VMEM), pltpu.with_memory_space_constraint(gd, pltpu.VMEM))

    return jax.shard_map(device_grads, mesh=mesh, in_specs=(tok_spec, tok_spec, len_spec, w_spec, w_spec), out_specs=(w_spec, w_spec), check_vma=False)
```

```python
import functools

import jax
import jax.numpy as jnp
from jax import lax
from jax.experimental import pallas as pl
from jax.experimental.pallas import tpu as pltpu
from jax.sharding import PartitionSpec as P

F32, BF16 = jnp.float32, jnp.bfloat16
MESH_ID = pl.DeviceIdType.MESH
SQRT_2_OVER_PI = 0.7978845608028654
CUBIC = 0.044715
NT_DIMS = (((1,), (1,)), ((), ()))

FC = 256
RING = 4
SUBS = 4
PH_ROWS = (128, 32, 8)
PH_OFF = (0, 384, 480)
R_ROWS = 504
W_SLOTS = 3
P_SLOTS = 2
STAGES = ("pair", "rs0b", "rs0c", "rs1b", "rs1c", "rs2b", "rs2c", "ag2b", "ag2c", "ag1b", "ag1c", "ag0b", "ag0c")

OPENING = 4
MIN_LEN = 128
TABLE = (
    (),
    (),
    (),
    (),
    ((0, 0),),
    (),
    ((1, 0),),
    ((0, 1),),
    ((2, 0),),
    ((1, 1), (0, 2),),
    ((4, 0), (0, 3),),
    ((1, 2), (2, 1),),
    ((6, 0), (0, 4), (1, 3),),
    ((2, 2),),
    ((8, 0), (4, 1), (1, 4), (0, 5),),
    ((2, 3),),
    ((4, 2), (6, 1), (0, 6), (2, 4),),
    ((1, 5), (10, 0),),
    ((6, 2), (0, 7), (8, 1), (4, 3),),
    ((2, 5), (3, 4), (1, 6),),
    ((1, 7), (0, 8),),
    ((6, 3), (10, 1), (4, 4), (3, 5), (8, 2),),
    ((2, 6), (1, 8), (11, 0), (2, 7), (0, 9),),
    (),
    ((5, 4), (3, 6), (4, 5), (0, 10), (10, 2),),
    ((2, 8),),
    ((5, 5), (6, 4), (4, 6), (1, 9), (3, 7), (8, 3), (0, 11),),
    ((1, 10), (3, 8), (11, 2),),
    ((5, 6), (6, 5), (4, 7), (7, 4), (2, 9), (0, 12),),
    ((1, 11), (10, 3),),
    ((2, 10), (4, 8), (6, 6), (0, 13), (3, 9), (8, 4), (5, 7), (7, 5),),
    ((2, 11), (1, 12), (11, 1),),
    ((7, 6), (5, 8), (0, 14),),
    (),
    ((3, 11), (4, 9), (3, 10), (1, 13), (8, 5), (6, 7), (9, 4), (2, 12), (8, 6), (0, 15), (5, 9), (4, 11), (6, 8), (1, 14), (2, 13), (3, 12), (9, 6), (4, 10), (7, 7), (9, 5), (10, 4), (6, 9), (1, 15), (5, 10), (7, 8), (4, 12), (5, 11), (2, 14), (10, 6), (3, 13), (8, 7), (5, 12), (7, 9), (6, 10), (8, 8), (2, 15), (3, 14), (6, 11), (10, 5), (7, 10), (8, 9), (4, 13), (9, 7), (6, 12), (3, 15), (11, 6), (7, 11), (4, 14), (11, 4), (11, 5), (8, 10), (4, 15), (9, 8), (7, 12), (5, 13), (5, 14), (8, 11), (10, 7), (9, 9), (11, 3), (12, 2), (5, 15), (6, 13), (9, 10), (6, 14), (10, 8), (9, 11), (8, 12), (7, 13), (6, 15), (7, 14), (11, 7), (10, 9), (11, 8), (7, 15), (8, 13), (9, 12), (8, 14), (10, 10), (12, 3), (11, 9), (12, 6), (8, 15), (9, 13), (12, 4), (12, 1), (10, 12), (12, 5), (9, 14), (10, 11), (9, 15), (10, 13), (12, 9), (10, 14), (10, 15), (12, 0), (11, 13), (11, 12), (12, 8), (11, 11), (11, 15), (12, 7), (11, 10), (11, 14), (12, 11), (12, 13), (12, 15), (12, 12), (12, 10), (12, 14),),
)
DIRECT = (0, 1, 2, 3)
LANES = 128
SHAPES = (
    3, 0, 0, 6, 6, 6, 0, 2, 0, 6, 6, 6, 0, 0, 0, 6, 2, 5, 0, 0, 0, 6, 2, 6, 6, 0, 0, 6, 6, 7, 0, 0,
    0, 6, 6, 6, 0, 6, 0, 6, 6, 6, 0, 0, 6, 6, 6, 6, 5, 0, 4, 6, 6, 6, 0, 0, 5, 6, 6, 6, 0, 0, 4, 6,
)


def stages_of(t):
    return [k for k, n in enumerate(STAGES) if not (t in DIRECT and n in ("rs1b", "rs2b", "ag2b", "ag1b"))]


def program(n_ticks):
    if n_ticks == 16 and TABLE:
        return TABLE
    last = OPENING + 2 * (n_ticks - 1)
    slots = [[] for _ in range(last + 1)]
    for t in range(n_ticks):
        for k, s in enumerate(stages_of(t)):
            slots[min(OPENING + 2 * t + k, last)].append((s, t))
    slots[-1].sort()
    return slots


def gelu_and_slope(u):
    u2 = u * u
    half = 0.5 + 0.5 * jnp.tanh(u * (SQRT_2_OVER_PI + (CUBIC * SQRT_2_OVER_PI) * u2))
    a = u * half
    return a, half + (a * (1.0 - half)) * (2.0 * SQRT_2_OVER_PI + (6.0 * CUBIC * SQRT_2_OVER_PI) * u2)


def subs_of(t):
    blocks = []
    for g in range(SUBS * t, SUBS * t + SUBS):
        code, a = SHAPES[g % len(SHAPES)], g % 3
        b, c = ((a + 1) % 3, (a + 2) % 3) if code % 2 == 0 else ((a + 2) % 3, (a + 1) % 3)
        dirs = (1 if g // 3 % 2 == 0 else -1, -1 if code & 2 else 1, -1 if code & 4 else 1)
        blocks.append((g, (a, b, c), dirs))
    return blocks


def kernel(n_ticks, n_tok, n_micro, sems, *refs):
    pl.run_scoped(functools.partial(body, n_ticks, n_tok, n_micro, refs), *sems)


def body(n_ticks, n_tok, n_micro, refs,
         in_sem, w_local, w_send, w_recv, p_send, p_recv, rs1, rs2, ag1, ag2, send0, send1, out_send,
         g_free, w_credit, r_credit):
    (x_hbm, dy_hbm, len_ref, wu_hbm, wd_hbm, GU, GD,
     X, DY, XT, WU, WD, AT, DH, SU, SD, RU, RD, R, E) = refs
    tok = n_tok // n_micro
    half_ff = n_ticks * 128
    rep = lax.axis_index("replica")
    me = lax.axis_index("fsdp")
    mate = 1 - me

    def dev(replica, core):
        return (0, replica, core)

    strides = [RING**a for a in range(3)]
    coord = [(rep // s) % RING for s in strides]
    quarter = [[coord[a]] + [(coord[a] + k) % RING for k in range(1, RING)] for a in range(3)]
    near = [{d: rep + strides[a] * (quarter[a][d % RING] - coord[a]) for d in (1, -1, 2, 3)} for a in range(3)]

    def row_in_quarter(axes, phase):
        row = 0
        for p in range(1, phase):
            row = row + coord[axes[p]] * PH_ROWS[p]
        return row

    def g_part(g, q, row, n):
        t, s = g // SUBS, g % SUBS
        if s < 2:
            start = q * 128 + row
            return GU.at[pl.ds(pl.multiple_of(start, 8), n), pl.ds(s * half_ff + t * 128, 128)]
        start = t * 128 + row
        if not isinstance(start, int):
            start = pl.multiple_of(start, 8)
        return GD.at[pl.ds(start, n), pl.ds(pl.multiple_of((s - 2) * 512 + q * 128, 128), 128)]

    def r_part(g, start, n):
        return R.at[pl.ds(g * R_ROWS + start, n)]

    def e_part(g, row, n):
        start = g * PH_ROWS[0] + row
        if not isinstance(start, int):
            start = pl.multiple_of(start, 8)
        return E.at[pl.ds(start, n)]

    def wait_rows(sem, n):
        ref = R.at[pl.ds(0, n)]
        pltpu.make_async_copy(ref, ref, sem).wait()

    barrier = pltpu.get_barrier_semaphore()
    for a in range(3):
        for d in (1, -1, 2):
            pl.semaphore_signal(barrier, inc=1, device_id=dev(near[a][d], me), device_id_type=MESH_ID)
    pl.semaphore_signal(barrier, inc=1, device_id=dev(rep, mate), device_id_type=MESH_ID)

    n_cols = X.shape[0]

    def x_copy(k):
        return [pltpu.make_async_copy(x_hbm.at[k, :, pl.ds(c * LANES, LANES)], X.at[c, pl.ds(k * tok, tok)], in_sem.at[k]) for c in range(n_cols)]

    def dy_copy(k):
        return [pltpu.make_async_copy(dy_hbm.at[k, :, pl.ds(c * LANES, LANES)], DY.at[c, pl.ds(k * tok, tok)], in_sem.at[n_micro + k]) for c in range(n_cols)]

    def landed(ref, k, sem):
        block = ref.at[:, pl.ds(k * tok, tok)]
        pltpu.make_async_copy(block, block, sem).wait()

    def w_parts(t):
        slot = t % W_SLOTS
        lo = pl.multiple_of(t * 128, 128)
        hi = pl.multiple_of(half_ff + t * 128, 128)
        up_rows = pl.ds(pl.multiple_of(me * 512, 512), 512)
        down_rows = pl.ds(pl.multiple_of(me * 128, 128), 128)
        return (
            (wu_hbm.at[0, :, pl.ds(lo, 128)], WU.at[slot, up_rows, pl.ds(0, 128)]),
            (wu_hbm.at[0, :, pl.ds(hi, 128)], WU.at[slot, up_rows, pl.ds(128, 128)]),
            (wd_hbm.at[0, pl.ds(lo, 128), :], WD.at[slot, down_rows, :]),
        )

    def load_w(t):
        for s, d in w_parts(t):
            pltpu.make_async_copy(s, d, w_local.at[t % W_SLOTS]).start()

    def push_w(t, from_vmem):
        for s, d in w_parts(t):
            pltpu.make_async_remote_copy(
                d if from_vmem else s, d, w_send.at[t % W_SLOTS], w_recv.at[t % W_SLOTS],
                device_id=dev(rep, mate), device_id_type=MESH_ID).start()

    def start_w(t):
        push_w(t, False)
        load_w(t)

    def wait_w(t, sems=None):
        slot = t % W_SLOTS
        ref = WU.at[slot]
        for sem in sems or (w_local, w_recv, w_send):
            pltpu.make_async_copy(ref, ref, sem.at[slot]).wait()

    def load_tokens(part):
        for k in range(part * n_micro // 2, (part + 1) * n_micro // 2):
            for copy in dy_copy(k) + x_copy(k):
                copy.start()

    load_w(0)
    load_tokens(0)
    with jax.named_scope("entry"):
        pl.semaphore_wait(barrier, 10)
    wait_w(0, (w_local,))
    push_w(0, True)
    load_tokens(1)

    mb = min(128, tok)
    clean = MIN_LEN if tok > MIN_LEN else 0

    def mask_micro(k):
        with jax.named_scope("dywait"):
            landed(DY, k, in_sem.at[n_micro + k])
        n_valid = len_ref[k]

        def mask_rows(s, carry):
            rows = pl.ds(pl.multiple_of(k * tok + clean + s * mb, mb), mb)
            at = clean + s * mb + lax.broadcasted_iota(jnp.int32, (mb, LANES), 0)
            keep = jnp.where(at < n_valid, 1.0, 0.0).astype(BF16)
            for c in range(n_cols):
                DY[c, rows, :] = DY[c, rows, :] * keep
            return carry

        lax.fori_loop(0, (tok - clean) // mb, mask_rows, 0)

    def wide(ref, rows, lo, hi):
        return jnp.concatenate([ref[c, rows, :] for c in range(lo, hi)], axis=1)

    cb = min(256, n_tok // 2)

    def hidden(t, lo, hi, turn=False):
        slot = t % W_SLOTS
        for at in range(lo, hi, cb):
            rows = pl.ds(at, cb)
            if turn:
                for c in range(n_cols):
                    XT[pl.ds(c * LANES, LANES), rows] = X[c, rows, :].T
            h = jnp.dot(wide(X, rows, 0, n_cols), WU[slot], preferred_element_type=F32).astype(BF16).astype(F32)
            da = lax.dot_general(wide(DY, rows, 0, n_cols), WD[slot], NT_DIMS, preferred_element_type=F32)
            a, slope = gelu_and_slope(h)
            AT[:, rows] = a.astype(BF16).T
            DH[rows, :] = (da * slope).astype(BF16)

    def free_w(t):
        @pl.when(t + W_SLOTS < n_ticks)
        def _():
            pl.semaphore_signal(w_credit, inc=1, device_id=dev(rep, mate), device_id_type=MESH_ID)

    def more_w(t):
        @pl.when((t < n_ticks) & (t >= W_SLOTS))
        def _():
            pl.semaphore_wait(w_credit, 1)

        @pl.when(t < n_ticks)
        def _():
            start_w(t)

    def send_to_mate(t, part):
        slot = t % P_SLOTS
        if part == 0:
            src, dst = SU.at[slot, pl.ds(pl.multiple_of(mate * 512, 512), 512)], RU.at[slot]
        else:
            src, dst = SD.at[slot, pl.ds(pl.multiple_of(mate * 128, 128), 128)], RD.at[slot]
        pltpu.make_async_remote_copy(
            src, dst, p_send.at[slot], p_recv.at[slot], device_id=dev(rep, mate), device_id_type=MESH_ID).start()

    def take_pair_room(t):
        @pl.when(t >= P_SLOTS)
        def _():
            pl.semaphore_wait(r_credit, 1)

    def up(t):
        slot = t % P_SLOTS
        for s in range(2):
            rows = pl.ds(s * 512, 512)
            SU[slot, rows, :] = jnp.dot(XT[rows, :], DH[...], preferred_element_type=F32)

    def down(t):
        slot = t % P_SLOTS
        for s in range(2):
            cols = pl.ds(s * 512, 512)
            SD[slot, :, cols] = jnp.dot(AT[...], wide(DY, slice(None), 4 * s, 4 * s + 4), preferred_element_type=F32)

    def send(sent, src, dst, recv, to):
        pltpu.make_async_remote_copy(
            src, dst, sent, recv, device_id=dev(to, me), device_id_type=MESH_ID).start()

    def pair_stage(t):
        slot = t % P_SLOTS
        whole = SU.at[slot]
        pltpu.make_async_copy(whole, whole, p_recv.at[slot]).wait()
        own = pl.ds(pl.multiple_of(me * 512, 512), 512)
        for s in range(2):
            cols = pl.ds(s * 128, 128)
            GU[:, pl.ds(s * half_ff + t * 128, 128)] = SU[slot, own, cols] + RU[slot, :, cols]
        own = pl.ds(pl.multiple_of(me * 128, 128), 128)
        GD[pl.ds(t * 128, 128), :] = SD[slot, own, :] + RD[slot]
        pltpu.make_async_copy(whole, whole, p_send.at[slot]).wait()
        if t + P_SLOTS < n_ticks:
            pl.semaphore_signal(r_credit, inc=1, device_id=dev(rep, mate), device_id_type=MESH_ID)
        rs_a(t, 0)

    def rs_a(t, p):
        sent = (send0 if p == 0 else send1).at[t]
        m, off = PH_ROWS[p], PH_OFF[p]
        if p > 0 and t in DIRECT:
            for k in (2, 1, 3):
                for g, axes, dirs in subs_of(t):
                    a = axes[p]
                    src = g_part(g, coord[axes[0]], row_in_quarter(axes, p) + quarter[a][k] * m, m)
                    send(sent, src, r_part(g, off + (k - 1) * m, m), rs2.at[t * 3 + p], near[a][k])
            return
        for relay in (True, False):
            for g, axes, dirs in subs_of(t):
                a, d = axes[p], dirs[p]
                q = quarter[a][2 if relay else -d % RING]
                src = g_part(g, q, 0, m) if p == 0 else g_part(g, coord[axes[0]], row_in_quarter(axes, p) + q * m, m)
                if relay:
                    send(sent, src, r_part(g, off, m), rs1.at[t * 3 + p], near[a][d])
                else:
                    send(sent, src, r_part(g, off + m, m), rs2.at[t * 3 + p], near[a][-d])

    def rs_b(t, p):
        sent = (send0 if p == 0 else send1).at[t]
        m, off = PH_ROWS[p], PH_OFF[p]
        wait_rows(rs1.at[t * 3 + p], SUBS * m)
        for g, axes, dirs in subs_of(t):
            a, d = axes[p], dirs[p]
            q = quarter[a][d % RING]
            part = g_part(g, q, 0, m) if p == 0 else g_part(g, coord[axes[0]], row_in_quarter(axes, p) + q * m, m)
            part[...] = part[...] + r_part(g, off, m)[...]
            send(sent, part, r_part(g, off + 2 * m, m), rs2.at[t * 3 + p], near[a][d])

    def rs_c(t, p):
        m, off = PH_ROWS[p], PH_OFF[p]
        straight = p > 0 and t in DIRECT
        wait_rows(rs2.at[t * 3 + p], (3 if straight else 2) * SUBS * m)
        for g, axes, dirs in subs_of(t):
            row = 0 if p == 0 else row_in_quarter(axes, p) + coord[axes[p]] * m
            part = g_part(g, coord[axes[0]], row, m)
            out = e_part(g, row, m) if p == 2 else part
            total = part[...] + (r_part(g, off + m, m)[...] + r_part(g, off + 2 * m, m)[...])
            out[...] = total + r_part(g, off, m)[...] if straight else total
        if p < 2:
            rs_a(t, p + 1)
        else:
            ag_a(t, 2)
        if p == 1:
            wait_rows(send0.at[t], 3 * SUBS * PH_ROWS[0])
            for a in sorted({axes[0] for _, axes, _ in subs_of(t)}):
                for d in (1, -1):
                    pl.semaphore_signal(g_free.at[t], inc=1, device_id=dev(near[a][d], me), device_id_type=MESH_ID)

    def ag_part(g, axes, p, q):
        if p == 0:
            return g_part(g, q, 0, PH_ROWS[0])
        return e_part(g, row_in_quarter(axes, p) + q * PH_ROWS[p], PH_ROWS[p])

    def ag_a(t, p):
        if p == 0:
            pl.semaphore_wait(g_free.at[t], 2 * len({axes[0] for _, axes, _ in subs_of(t)}))
        if p > 0 and t in DIRECT:
            for k in (2, 1, 3):
                for g, axes, dirs in subs_of(t):
                    part = ag_part(g, axes, p, coord[axes[p]])
                    send(out_send.at[t], part, part, ag2.at[t * 3 + p], near[axes[p]][k])
            return
        for recv, sign in ((ag1, 1), (ag2, -1)):
            for g, axes, dirs in subs_of(t):
                a, d = axes[p], dirs[p]
                part = ag_part(g, axes, p, coord[a])
                src = e_part(g, 0, PH_ROWS[0]) if p == 0 else part
                send(out_send.at[t], src, part, recv.at[t * 3 + p], near[a][sign * d])
        if p == 0:
            wait_rows(send1.at[t], 3 * SUBS * (PH_ROWS[1] + PH_ROWS[2]))
            for g, axes, dirs in subs_of(t):
                g_part(g, coord[axes[0]], 0, PH_ROWS[0])[...] = e_part(g, 0, PH_ROWS[0])[...]

    def ag_b(t, p):
        wait_rows(ag1.at[t * 3 + p], SUBS * PH_ROWS[p])
        for g, axes, dirs in subs_of(t):
            a, d = axes[p], dirs[p]
            part = ag_part(g, axes, p, quarter[a][-d % RING])
            send(out_send.at[t], part, part, ag2.at[t * 3 + p], near[a][d])

    def ag_c(t, p):
        wait_rows(ag2.at[t * 3 + p], (3 if p > 0 and t in DIRECT else 2) * SUBS * PH_ROWS[p])
        if p > 0:
            ag_a(t, p - 1)

    def run(ops):
        for s, t in ops:
            name = STAGES[s]
            with jax.named_scope(name):
                if name == "pair":
                    pair_stage(t)
                else:
                    p = int(name[2])
                    {"rsb": rs_b, "rsc": rs_c, "agb": ag_b, "agc": ag_c}[name[:2] + name[3]](t, p)

    slots = program(n_ticks)

    def pick(t, first, lo, hi):
        lists = [slots[first(k)] for k in range(lo, hi)]
        if not any(lists):
            return
        if hi - lo == 1:
            run(lists[0])
            return
        mid = (lo + hi) // 2
        pl.when(t < mid)(lambda: pick(t, first, lo, mid))
        pl.when(t >= mid)(lambda: pick(t, first, mid, hi))

    n_half = n_tok // 2
    for part in range(2):
        for k in range(part * n_micro // 2, (part + 1) * n_micro // 2):
            with jax.named_scope("mask"):
                mask_micro(k)
            with jax.named_scope("xwait"):
                landed(X, k, in_sem.at[k])
        if part == 0:
            with jax.named_scope("wwait"):
                wait_w(0, (w_recv, w_send))
        with jax.named_scope("hidfirst"):
            hidden(0, part * n_half, (part + 1) * n_half, turn=True)
        if part == 0 and n_ticks > 1:
            start_w(1)
        run(slots[part])
    free_w(0)
    more_w(2)
    with jax.named_scope("upfirst"):
        up(0)
    send_to_mate(0, 0)
    run(slots[2])
    with jax.named_scope("downfirst"):
        down(0)
    send_to_mate(0, 1)
    run(slots[3])

    def tick(t, carry):
        with jax.named_scope("wwait"):
            wait_w(t)
        with jax.named_scope("hidden"):
            hidden(t, 0, n_tok)
        free_w(t)
        pick(t, lambda k: OPENING + 2 * k - 2, 1, n_ticks)
        more_w(t + 2)
        take_pair_room(t)
        with jax.named_scope("grad"):
            up(t)
            down(t)
            send_to_mate(t, 0)
            send_to_mate(t, 1)
        pick(t, lambda k: OPENING + 2 * k - 1, 1, n_ticks)
        return carry

    lax.fori_loop(1, n_ticks, tick, 0)
    run(slots[-1])
    for t in range(n_ticks):
        wait_rows(out_send.at[t], SUBS * R_ROWS)


FLUSH = 8


def flush(gu, gd, gu_hbm, gd_hbm, sem):
    copies = []
    for k in range(FLUSH):
        for ref, out, s in ((gu, gu_hbm, 0), (gd, gd_hbm, 1)):
            rows = pl.ds(k * (ref.shape[0] // FLUSH), ref.shape[0] // FLUSH)
            copies.append(pltpu.make_async_copy(ref.at[rows], out.at[0, rows], sem.at[2 * k + s]))
    for copy in copies:
        copy.start()
    for copy in copies:
        copy.wait()


def solution(mesh):
    tok_spec = P(None, ("model", "replica", "fsdp"), None)
    len_spec = P(None, ("model", "replica", "fsdp"))
    w_spec = P(None, ("model", "fsdp"), None)

    def device_grads(x_in, dy_out, lengths, w_up, w_down):
        n_micro, tok, d = x_in.shape
        n_tok = n_micro * tok
        d_ff = w_up.shape[2]
        n_ticks = d_ff // FC
        any_spec = pl.BlockSpec(memory_space=pl.ANY)
        dma = pltpu.SemaphoreType.DMA
        regular = pltpu.SemaphoreType.REGULAR
        sems = [
            dma((2 * n_micro,)),
            dma((W_SLOTS,)),
            dma((W_SLOTS,)),
            dma((W_SLOTS,)),
            dma((P_SLOTS,)),
            dma((P_SLOTS,)),
            dma((3 * n_ticks,)),
            dma((3 * n_ticks,)),
            dma((3 * n_ticks,)),
            dma((3 * n_ticks,)),
            dma((n_ticks,)),
            dma((n_ticks,)),
            dma((n_ticks,)),
            regular((n_ticks,)),
            regular,
            regular,
        ]
        gu, gd = pl.pallas_call(
            functools.partial(kernel, n_ticks, n_tok, n_micro, sems),
            out_shape=(
                pltpu.VMEM((d // 2, d_ff), F32),
                pltpu.VMEM((d_ff // 2, d), F32),
            ),
            in_specs=[any_spec, any_spec, pl.BlockSpec(memory_space=pltpu.SMEM), any_spec, any_spec],
            out_specs=(pl.BlockSpec(memory_space=pltpu.VMEM),) * 2,
            scratch_shapes=[
                pltpu.VMEM((d // LANES, n_tok, LANES), BF16),
                pltpu.VMEM((d // LANES, n_tok, LANES), BF16),
                pltpu.VMEM((d, n_tok), BF16),
                pltpu.VMEM((W_SLOTS, d, FC), BF16),
                pltpu.VMEM((W_SLOTS, FC, d), BF16),
                pltpu.VMEM((FC, n_tok), BF16),
                pltpu.VMEM((n_tok, FC), BF16),
                pltpu.VMEM((P_SLOTS, d, FC), F32),
                pltpu.VMEM((P_SLOTS, FC, d), F32),
                pltpu.VMEM((P_SLOTS, d // 2, FC), F32),
                pltpu.VMEM((P_SLOTS, FC // 2, d), F32),
                pltpu.VMEM((n_ticks * SUBS * R_ROWS, 128), F32),
                pltpu.VMEM((n_ticks * SUBS * PH_ROWS[0], 128), F32),
            ],
            compiler_params=pltpu.CompilerParams(
                collective_id=0, has_side_effects=True, vmem_limit_bytes=67043328 - (16 << 20)),
            name="grads",
        )(x_in, dy_out, lengths.reshape(n_micro), w_up, w_down)
        vmem = pl.BlockSpec(memory_space=pltpu.VMEM)
        return pl.pallas_call(
            flush,
            out_shape=(
                jax.ShapeDtypeStruct(w_up.shape, F32),
                jax.ShapeDtypeStruct(w_down.shape, F32),
            ),
            in_specs=[vmem, vmem],
            out_specs=(any_spec, any_spec),
            scratch_shapes=[dma((2 * FLUSH,))],
            compiler_params=pltpu.CompilerParams(vmem_limit_bytes=1 << 20),
            name="flush",
        )(pltpu.with_memory_space_constraint(gu, pltpu.VMEM), pltpu.with_memory_space_constraint(gd, pltpu.VMEM))

    return jax.shard_map(device_grads, mesh=mesh, in_specs=(tok_spec, tok_spec, len_spec, w_spec, w_spec), out_specs=(w_spec, w_spec), check_vma=False)
```

```python
import functools

import jax
import jax.numpy as jnp
from jax import lax
from jax.experimental import pallas as pl
from jax.experimental.pallas import tpu as pltpu
from jax.sharding import PartitionSpec as P

F32, BF16 = jnp.float32, jnp.bfloat16
MESH_ID = pl.DeviceIdType.MESH
SQRT_2_OVER_PI = 0.7978845608028654
CUBIC = 0.044715
NT_DIMS = (((1,), (1,)), ((), ()))

FC = 256
RING = 4
SUBS = 4
PH_ROWS = (128, 32, 8)
PH_OFF = (0, 384, 480)
R_ROWS = 504
W_SLOTS = 3
P_SLOTS = 2
STAGES = ("pair", "rs0b", "rs0c", "rs1b", "rs1c", "rs2b", "rs2c", "ag2b", "ag2c", "ag1b", "ag1c", "ag0b", "ag0c")

OPENING = 4
MIN_LEN = 128
TABLE = (
    (),
    (),
    (),
    (),
    (),
    ((0, 0),),
    ((0, 1),),
    ((1, 0),),
    ((1, 1), (0, 2),),
    ((2, 0),),
    ((2, 1), (0, 3),),
    ((3, 0), (1, 2),),
    ((3, 1), (0, 4),),
    ((4, 0), (1, 3), (2, 2),),
    ((4, 1), (0, 5),),
    ((6, 0), (1, 4), (3, 2), (2, 3),),
    ((6, 1), (1, 5), (0, 6),),
    ((2, 4), (8, 0), (3, 3), (4, 2),),
    ((8, 1), (2, 5), (0, 7),),
    ((9, 0), (1, 6), (3, 4), (4, 3),),
    ((6, 2), (3, 5), (0, 8), (9, 1), (1, 7),),
    ((10, 0), (2, 6),),
    ((4, 5), (4, 4), (8, 2), (6, 3), (1, 8), (0, 9),),
    ((10, 1),),
    ((2, 7), (11, 0), (3, 6),),
    ((8, 3), (2, 8), (5, 5), (9, 2), (6, 4), (0, 10),),
    ((3, 7), (0, 11), (1, 9),),
    ((9, 3), (3, 8), (4, 6), (10, 2),),
    ((6, 5), (1, 10), (0, 12), (4, 7), (12, 0),),
    ((4, 8), (5, 6), (8, 4), (1, 11), (2, 9), (10, 3),),
    ((2, 10), (0, 13),),
    ((9, 4), (6, 6), (1, 12), (2, 11), (5, 8), (11, 2),),
    ((5, 7), (3, 9), (3, 10), (7, 5), (0, 14), (10, 4),),
    (),
    ((7, 6), (1, 13), (4, 9), (3, 11), (6, 7), (6, 8), (4, 10), (8, 5), (2, 12), (0, 15), (1, 14), (11, 1), (7, 7), (8, 6), (4, 11), (5, 9), (2, 13), (7, 8), (3, 12), (5, 10), (9, 5), (11, 4), (1, 15), (11, 3), (8, 7), (2, 14), (12, 1), (5, 11), (9, 6), (6, 9), (3, 13), (4, 12), (6, 10), (8, 8), (12, 2), (10, 5), (2, 15), (3, 14), (6, 11), (7, 9), (4, 13), (9, 7), (10, 6), (7, 10), (11, 5), (5, 12), (3, 15), (4, 14), (5, 13), (7, 11), (8, 9), (9, 8), (10, 7), (8, 10), (12, 3), (4, 15), (6, 12), (5, 14), (6, 13), (9, 9), (11, 6), (8, 11), (10, 8), (5, 15), (9, 10), (7, 12), (6, 14), (11, 7), (7, 13), (10, 9), (11, 8), (6, 15), (8, 12), (7, 14), (9, 11), (10, 10), (8, 13), (11, 9), (7, 15), (8, 14), (9, 12), (10, 11), (9, 13), (11, 10), (8, 15), (9, 14), (12, 7), (12, 6), (10, 12), (11, 11), (9, 15), (10, 13), (10, 14), (10, 15), (11, 12), (12, 9), (12, 8), (11, 13), (11, 14), (12, 11), (11, 15), (12, 4), (12, 12), (12, 10), (12, 14), (12, 5), (12, 13), (12, 15),),
)
DIRECT = (2, 2, 2, 2, 2, 0, 0, 0, 0, 0, 0, 0, 0, 0, 0, 0)
LANES = 128
SHAPES = (
    3, 0, 0, 6, 6, 6, 0, 2, 0, 6, 6, 6, 0, 0, 0, 6, 2, 5, 0, 0, 0, 6, 2, 6, 6, 0, 0, 6, 6, 7, 0, 0,
    0, 6, 6, 6, 0, 6, 0, 6, 6, 6, 0, 0, 6, 6, 6, 6, 5, 0, 4, 6, 6, 6, 0, 0, 5, 6, 6, 6, 0, 0, 4, 6,
)


def is_direct(t, phase):
    return phase > 0 and DIRECT[t % len(DIRECT)] >> (phase - 1) & 1 == 1


def stages_of(t):
    return [k for k, n in enumerate(STAGES) if not (n[3:] == "b" and is_direct(t, int(n[2])))]


def program(n_ticks):
    if n_ticks == 16 and TABLE:
        return TABLE
    last = OPENING + 2 * (n_ticks - 1)
    slots = [[] for _ in range(last + 1)]
    for t in range(n_ticks):
        for k, s in enumerate(stages_of(t)):
            slots[min(OPENING + 2 * t + k, last)].append((s, t))
    slots[-1].sort()
    return slots


def gelu_and_slope(u):
    u2 = u * u
    half = 0.5 + 0.5 * jnp.tanh(u * (SQRT_2_OVER_PI + (CUBIC * SQRT_2_OVER_PI) * u2))
    a = u * half
    return a, half + (a * (1.0 - half)) * (2.0 * SQRT_2_OVER_PI + (6.0 * CUBIC * SQRT_2_OVER_PI) * u2)


def subs_of(t):
    blocks = []
    for g in range(SUBS * t, SUBS * t + SUBS):
        code, a = SHAPES[g % len(SHAPES)], g % 3
        b, c = ((a + 1) % 3, (a + 2) % 3) if code % 2 == 0 else ((a + 2) % 3, (a + 1) % 3)
        dirs = (1 if g // 3 % 2 == 0 else -1, -1 if code & 2 else 1, -1 if code & 4 else 1)
        blocks.append((g, (a, b, c), dirs))
    return blocks


def kernel(n_ticks, n_tok, n_micro, sems, *refs):
    pl.run_scoped(functools.partial(body, n_ticks, n_tok, n_micro, refs), *sems)


def body(n_ticks, n_tok, n_micro, refs,
         in_sem, w_local, w_send, w_recv, p_send, p_recv, rs1, rs2, ag1, ag2, send0, send1, out_send,
         g_free, w_credit, r_credit):
    (x_hbm, dy_hbm, len_ref, wu_hbm, wd_hbm, GU, GD,
     X, DY, XT, WU, WD, AT, DH, SU, SD, RU, RD, R, E) = refs
    tok = n_tok // n_micro
    half_ff = n_ticks * 128
    rep = lax.axis_index("replica")
    me = lax.axis_index("fsdp")
    mate = 1 - me

    def dev(replica, core):
        return (0, replica, core)

    strides = [RING**a for a in range(3)]
    coord = [(rep // s) % RING for s in strides]
    quarter = [[coord[a]] + [(coord[a] + k) % RING for k in range(1, RING)] for a in range(3)]
    near = [{d: rep + strides[a] * (quarter[a][d % RING] - coord[a]) for d in (1, -1, 2, 3)} for a in range(3)]

    def row_in_quarter(axes, phase):
        row = 0
        for p in range(1, phase):
            row = row + coord[axes[p]] * PH_ROWS[p]
        return row

    def g_part(g, q, row, n):
        t, s = g // SUBS, g % SUBS
        if s < 2:
            start = q * 128 + row
            return GU.at[pl.ds(pl.multiple_of(start, 8), n), pl.ds(s * half_ff + t * 128, 128)]
        start = t * 128 + row
        if not isinstance(start, int):
            start = pl.multiple_of(start, 8)
        return GD.at[pl.ds(start, n), pl.ds(pl.multiple_of((s - 2) * 512 + q * 128, 128), 128)]

    def r_part(g, start, n):
        return R.at[pl.ds(g * R_ROWS + start, n)]

    def e_part(g, row, n):
        start = g * PH_ROWS[0] + row
        if not isinstance(start, int):
            start = pl.multiple_of(start, 8)
        return E.at[pl.ds(start, n)]

    def wait_rows(sem, n):
        ref = R.at[pl.ds(0, n)]
        pltpu.make_async_copy(ref, ref, sem).wait()

    barrier = pltpu.get_barrier_semaphore()
    for a in range(3):
        for d in (1, -1, 2):
            pl.semaphore_signal(barrier, inc=1, device_id=dev(near[a][d], me), device_id_type=MESH_ID)
    pl.semaphore_signal(barrier, inc=1, device_id=dev(rep, mate), device_id_type=MESH_ID)

    n_cols = X.shape[0]

    def x_copy(k):
        return [pltpu.make_async_copy(x_hbm.at[k, :, pl.ds(c * LANES, LANES)], X.at[c, pl.ds(k * tok, tok)], in_sem.at[k]) for c in range(n_cols)]

    def dy_copy(k):
        return [pltpu.make_async_copy(dy_hbm.at[k, :, pl.ds(c * LANES, LANES)], DY.at[c, pl.ds(k * tok, tok)], in_sem.at[n_micro + k]) for c in range(n_cols)]

    def landed(ref, k, sem):
        block = ref.at[:, pl.ds(k * tok, tok)]
        pltpu.make_async_copy(block, block, sem).wait()

    def w_parts(t):
        slot = t % W_SLOTS
        lo = pl.multiple_of(t * 128, 128)
        hi = pl.multiple_of(half_ff + t * 128, 128)
        up_rows = pl.ds(pl.multiple_of(me * 512, 512), 512)
        down_rows = pl.ds(pl.multiple_of(me * 128, 128), 128)
        return (
            (wu_hbm.at[0, :, pl.ds(lo, 128)], WU.at[slot, up_rows, pl.ds(0, 128)]),
            (wu_hbm.at[0, :, pl.ds(hi, 128)], WU.at[slot, up_rows, pl.ds(128, 128)]),
            (wd_hbm.at[0, pl.ds(lo, 128), :], WD.at[slot, down_rows, :]),
        )

    def load_w(t):
        for s, d in w_parts(t):
            pltpu.make_async_copy(s, d, w_local.at[t % W_SLOTS]).start()

    def push_w(t, from_vmem):
        for s, d in w_parts(t):
            pltpu.make_async_remote_copy(
                d if from_vmem else s, d, w_send.at[t % W_SLOTS], w_recv.at[t % W_SLOTS],
                device_id=dev(rep, mate), device_id_type=MESH_ID).start()

    def start_w(t):
        push_w(t, False)
        load_w(t)

    def wait_w(t, sems=None):
        slot = t % W_SLOTS
        ref = WU.at[slot]
        for sem in sems or (w_local, w_recv, w_send):
            pltpu.make_async_copy(ref, ref, sem.at[slot]).wait()

    def load_tokens(part):
        for k in range(part * n_micro // 2, (part + 1) * n_micro // 2):
            for copy in dy_copy(k) + x_copy(k):
                copy.start()

    load_w(0)
    load_tokens(0)
    with jax.named_scope("entry"):
        pl.semaphore_wait(barrier, 10)
    wait_w(0, (w_local,))
    push_w(0, True)
    load_tokens(1)

    mb = min(128, tok)
    clean = MIN_LEN if tok > MIN_LEN else 0

    def mask_micro(k):
        with jax.named_scope("dywait"):
            landed(DY, k, in_sem.at[n_micro + k])
        n_valid = len_ref[k]

        def mask_rows(s, carry):
            rows = pl.ds(pl.multiple_of(k * tok + clean + s * mb, mb), mb)
            at = clean + s * mb + lax.broadcasted_iota(jnp.int32, (mb, LANES), 0)
            keep = jnp.where(at < n_valid, 1.0, 0.0).astype(BF16)
            for c in range(n_cols):
                DY[c, rows, :] = DY[c, rows, :] * keep
            return carry

        lax.fori_loop(0, (tok - clean) // mb, mask_rows, 0)

    def wide(ref, rows, lo, hi):
        return jnp.concatenate([ref[c, rows, :] for c in range(lo, hi)], axis=1)

    cb = min(256, n_tok // 2)

    def hidden(t, lo, hi, turn=False):
        slot = t % W_SLOTS
        for at in range(lo, hi, cb):
            rows = pl.ds(at, cb)
            if turn:
                for c in range(n_cols):
                    XT[pl.ds(c * LANES, LANES), rows] = X[c, rows, :].T
            h = jnp.dot(wide(X, rows, 0, n_cols), WU[slot], preferred_element_type=F32).astype(BF16).astype(F32)
            da = lax.dot_general(wide(DY, rows, 0, n_cols), WD[slot], NT_DIMS, preferred_element_type=F32)
            a, slope = gelu_and_slope(h)
            AT[:, rows] = a.astype(BF16).T
            DH[rows, :] = (da * slope).astype(BF16)

    def free_w(t):
        @pl.when(t + W_SLOTS < n_ticks)
        def _():
            pl.semaphore_signal(w_credit, inc=1, device_id=dev(rep, mate), device_id_type=MESH_ID)

    def more_w(t):
        @pl.when((t < n_ticks) & (t >= W_SLOTS))
        def _():
            pl.semaphore_wait(w_credit, 1)

        @pl.when(t < n_ticks)
        def _():
            start_w(t)

    def send_to_mate(t, part):
        slot = t % P_SLOTS
        if part == 0:
            src, dst = SU.at[slot, pl.ds(pl.multiple_of(mate * 512, 512), 512)], RU.at[slot]
        else:
            src, dst = SD.at[slot, pl.ds(pl.multiple_of(mate * 128, 128), 128)], RD.at[slot]
        pltpu.make_async_remote_copy(
            src, dst, p_send.at[slot], p_recv.at[slot], device_id=dev(rep, mate), device_id_type=MESH_ID).start()

    def take_pair_room(t):
        @pl.when(t >= P_SLOTS)
        def _():
            pl.semaphore_wait(r_credit, 1)

    def up(t):
        slot = t % P_SLOTS
        for s in range(2):
            rows = pl.ds(s * 512, 512)
            SU[slot, rows, :] = jnp.dot(XT[rows, :], DH[...], preferred_element_type=F32)

    def down(t):
        slot = t % P_SLOTS
        for s in range(2):
            cols = pl.ds(s * 512, 512)
            SD[slot, :, cols] = jnp.dot(AT[...], wide(DY, slice(None), 4 * s, 4 * s + 4), preferred_element_type=F32)

    def send(sent, src, dst, recv, to):
        pltpu.make_async_remote_copy(
            src, dst, sent, recv, device_id=dev(to, me), device_id_type=MESH_ID).start()

    def pair_stage(t):
        slot = t % P_SLOTS
        whole = SU.at[slot]
        pltpu.make_async_copy(whole, whole, p_recv.at[slot]).wait()
        own = pl.ds(pl.multiple_of(me * 512, 512), 512)
        for s in range(2):
            cols = pl.ds(s * 128, 128)
            GU[:, pl.ds(s * half_ff + t * 128, 128)] = SU[slot, own, cols] + RU[slot, :, cols]
        own = pl.ds(pl.multiple_of(me * 128, 128), 128)
        GD[pl.ds(t * 128, 128), :] = SD[slot, own, :] + RD[slot]
        pltpu.make_async_copy(whole, whole, p_send.at[slot]).wait()
        if t + P_SLOTS < n_ticks:
            pl.semaphore_signal(r_credit, inc=1, device_id=dev(rep, mate), device_id_type=MESH_ID)
        rs_a(t, 0)

    def rs_a(t, p):
        sent = (send0 if p == 0 else send1).at[t]
        m, off = PH_ROWS[p], PH_OFF[p]
        if is_direct(t, p):
            for k in (2, 1, 3):
                for g, axes, dirs in subs_of(t):
                    a = axes[p]
                    src = g_part(g, coord[axes[0]], row_in_quarter(axes, p) + quarter[a][k] * m, m)
                    send(sent, src, r_part(g, off + (k - 1) * m, m), rs2.at[t * 3 + p], near[a][k])
            return
        for relay in (True, False):
            for g, axes, dirs in subs_of(t):
                a, d = axes[p], dirs[p]
                q = quarter[a][2 if relay else -d % RING]
                src = g_part(g, q, 0, m) if p == 0 else g_part(g, coord[axes[0]], row_in_quarter(axes, p) + q * m, m)
                if relay:
                    send(sent, src, r_part(g, off, m), rs1.at[t * 3 + p], near[a][d])
                else:
                    send(sent, src, r_part(g, off + m, m), rs2.at[t * 3 + p], near[a][-d])

    def rs_b(t, p):
        sent = (send0 if p == 0 else send1).at[t]
        m, off = PH_ROWS[p], PH_OFF[p]
        wait_rows(rs1.at[t * 3 + p], SUBS * m)
        for g, axes, dirs in subs_of(t):
            a, d = axes[p], dirs[p]
            q = quarter[a][d % RING]
            part = g_part(g, q, 0, m) if p == 0 else g_part(g, coord[axes[0]], row_in_quarter(axes, p) + q * m, m)
            part[...] = part[...] + r_part(g, off, m)[...]
            send(sent, part, r_part(g, off + 2 * m, m), rs2.at[t * 3 + p], near[a][d])

    def rs_c(t, p):
        m, off = PH_ROWS[p], PH_OFF[p]
        straight = is_direct(t, p)
        wait_rows(rs2.at[t * 3 + p], (3 if straight else 2) * SUBS * m)
        for g, axes, dirs in subs_of(t):
            row = 0 if p == 0 else row_in_quarter(axes, p) + coord[axes[p]] * m
            part = g_part(g, coord[axes[0]], row, m)
            out = e_part(g, row, m) if p == 2 else part
            total = part[...] + (r_part(g, off + m, m)[...] + r_part(g, off + 2 * m, m)[...])
            out[...] = total + r_part(g, off, m)[...] if straight else total
        if p < 2:
            rs_a(t, p + 1)
        else:
            ag_a(t, 2)
        if p == 1:
            wait_rows(send0.at[t], 3 * SUBS * PH_ROWS[0])
            for a in sorted({axes[0] for _, axes, _ in subs_of(t)}):
                for d in (1, -1):
                    pl.semaphore_signal(g_free.at[t], inc=1, device_id=dev(near[a][d], me), device_id_type=MESH_ID)

    def ag_part(g, axes, p, q):
        if p == 0:
            return g_part(g, q, 0, PH_ROWS[0])
        return e_part(g, row_in_quarter(axes, p) + q * PH_ROWS[p], PH_ROWS[p])

    def ag_a(t, p):
        if p == 0:
            pl.semaphore_wait(g_free.at[t], 2 * len({axes[0] for _, axes, _ in subs_of(t)}))
        if is_direct(t, p):
            for k in (2, 1, 3):
                for g, axes, dirs in subs_of(t):
                    part = ag_part(g, axes, p, coord[axes[p]])
                    send(out_send.at[t], part, part, ag2.at[t * 3 + p], near[axes[p]][k])
            return
        for recv, sign in ((ag1, 1), (ag2, -1)):
            for g, axes, dirs in subs_of(t):
                a, d = axes[p], dirs[p]
                part = ag_part(g, axes, p, coord[a])
                src = e_part(g, 0, PH_ROWS[0]) if p == 0 else part
                send(out_send.at[t], src, part, recv.at[t * 3 + p], near[a][sign * d])
        if p == 0:
            wait_rows(send1.at[t], 3 * SUBS * (PH_ROWS[1] + PH_ROWS[2]))
            for g, axes, dirs in subs_of(t):
                g_part(g, coord[axes[0]], 0, PH_ROWS[0])[...] = e_part(g, 0, PH_ROWS[0])[...]

    def ag_b(t, p):
        wait_rows(ag1.at[t * 3 + p], SUBS * PH_ROWS[p])
        for g, axes, dirs in subs_of(t):
            a, d = axes[p], dirs[p]
            part = ag_part(g, axes, p, quarter[a][-d % RING])
            send(out_send.at[t], part, part, ag2.at[t * 3 + p], near[a][d])

    def ag_c(t, p):
        wait_rows(ag2.at[t * 3 + p], (3 if is_direct(t, p) else 2) * SUBS * PH_ROWS[p])
        if p > 0:
            ag_a(t, p - 1)

    def run(ops):
        for s, t in ops:
            name = STAGES[s]
            with jax.named_scope(name):
                if name == "pair":
                    pair_stage(t)
                else:
                    p = int(name[2])
                    {"rsb": rs_b, "rsc": rs_c, "agb": ag_b, "agc": ag_c}[name[:2] + name[3]](t, p)

    slots = program(n_ticks)

    def pick(t, first, lo, hi):
        lists = [slots[first(k)] for k in range(lo, hi)]
        if not any(lists):
            return
        if hi - lo == 1:
            run(lists[0])
            return
        mid = (lo + hi) // 2
        pl.when(t < mid)(lambda: pick(t, first, lo, mid))
        pl.when(t >= mid)(lambda: pick(t, first, mid, hi))

    n_half = n_tok // 2
    for part in range(2):
        for k in range(part * n_micro // 2, (part + 1) * n_micro // 2):
            with jax.named_scope("mask"):
                mask_micro(k)
            with jax.named_scope("xwait"):
                landed(X, k, in_sem.at[k])
        if part == 0:
            with jax.named_scope("wwait"):
                wait_w(0, (w_recv, w_send))
        with jax.named_scope("hidfirst"):
            hidden(0, part * n_half, (part + 1) * n_half, turn=True)
        if part == 0 and n_ticks > 1:
            start_w(1)
        run(slots[part])
    free_w(0)
    more_w(2)
    with jax.named_scope("upfirst"):
        up(0)
    send_to_mate(0, 0)
    run(slots[2])
    with jax.named_scope("downfirst"):
        down(0)
    send_to_mate(0, 1)
    run(slots[3])

    def tick(t, carry):
        with jax.named_scope("wwait"):
            wait_w(t)
        with jax.named_scope("hidden"):
            hidden(t, 0, n_tok)
        free_w(t)
        pick(t, lambda k: OPENING + 2 * k - 2, 1, n_ticks)
        more_w(t + 2)
        take_pair_room(t)
        with jax.named_scope("grad"):
            up(t)
            down(t)
            send_to_mate(t, 0)
            send_to_mate(t, 1)
        pick(t, lambda k: OPENING + 2 * k - 1, 1, n_ticks)
        return carry

    lax.fori_loop(1, n_ticks, tick, 0)
    run(slots[-1])
    for t in range(n_ticks):
        wait_rows(out_send.at[t], SUBS * R_ROWS)


FLUSH = 8


def flush(gu, gd, gu_hbm, gd_hbm, sem):
    copies = []
    for k in range(FLUSH):
        for ref, out, s in ((gu, gu_hbm, 0), (gd, gd_hbm, 1)):
            rows = pl.ds(k * (ref.shape[0] // FLUSH), ref.shape[0] // FLUSH)
            copies.append(pltpu.make_async_copy(ref.at[rows], out.at[0, rows], sem.at[2 * k + s]))
    for copy in copies:
        copy.start()
    for copy in copies:
        copy.wait()


def solution(mesh):
    tok_spec = P(None, ("model", "replica", "fsdp"), None)
    len_spec = P(None, ("model", "replica", "fsdp"))
    w_spec = P(None, ("model", "fsdp"), None)

    def device_grads(x_in, dy_out, lengths, w_up, w_down):
        n_micro, tok, d = x_in.shape
        n_tok = n_micro * tok
        d_ff = w_up.shape[2]
        n_ticks = d_ff // FC
        any_spec = pl.BlockSpec(memory_space=pl.ANY)
        dma = pltpu.SemaphoreType.DMA
        regular = pltpu.SemaphoreType.REGULAR
        sems = [
            dma((2 * n_micro,)),
            dma((W_SLOTS,)),
            dma((W_SLOTS,)),
            dma((W_SLOTS,)),
            dma((P_SLOTS,)),
            dma((P_SLOTS,)),
            dma((3 * n_ticks,)),
            dma((3 * n_ticks,)),
            dma((3 * n_ticks,)),
            dma((3 * n_ticks,)),
            dma((n_ticks,)),
            dma((n_ticks,)),
            dma((n_ticks,)),
            regular((n_ticks,)),
            regular,
            regular,
        ]
        gu, gd = pl.pallas_call(
            functools.partial(kernel, n_ticks, n_tok, n_micro, sems),
            out_shape=(
                pltpu.VMEM((d // 2, d_ff), F32),
                pltpu.VMEM((d_ff // 2, d), F32),
            ),
            in_specs=[any_spec, any_spec, pl.BlockSpec(memory_space=pltpu.SMEM), any_spec, any_spec],
            out_specs=(pl.BlockSpec(memory_space=pltpu.VMEM),) * 2,
            scratch_shapes=[
                pltpu.VMEM((d // LANES, n_tok, LANES), BF16),
                pltpu.VMEM((d // LANES, n_tok, LANES), BF16),
                pltpu.VMEM((d, n_tok), BF16),
                pltpu.VMEM((W_SLOTS, d, FC), BF16),
                pltpu.VMEM((W_SLOTS, FC, d), BF16),
                pltpu.VMEM((FC, n_tok), BF16),
                pltpu.VMEM((n_tok, FC), BF16),
                pltpu.VMEM((P_SLOTS, d, FC), F32),
                pltpu.VMEM((P_SLOTS, FC, d), F32),
                pltpu.VMEM((P_SLOTS, d // 2, FC), F32),
                pltpu.VMEM((P_SLOTS, FC // 2, d), F32),
                pltpu.VMEM((n_ticks * SUBS * R_ROWS, 128), F32),
                pltpu.VMEM((n_ticks * SUBS * PH_ROWS[0], 128), F32),
            ],
            compiler_params=pltpu.CompilerParams(
                collective_id=0, has_side_effects=True, vmem_limit_bytes=67043328 - (16 << 20)),
            name="grads",
        )(x_in, dy_out, lengths.reshape(n_micro), w_up, w_down)
        vmem = pl.BlockSpec(memory_space=pltpu.VMEM)
        return pl.pallas_call(
            flush,
            out_shape=(
                jax.ShapeDtypeStruct(w_up.shape, F32),
                jax.ShapeDtypeStruct(w_down.shape, F32),
            ),
            in_specs=[vmem, vmem],
            out_specs=(any_spec, any_spec),
            scratch_shapes=[dma((2 * FLUSH,))],
            compiler_params=pltpu.CompilerParams(vmem_limit_bytes=1 << 20),
            name="flush",
        )(pltpu.with_memory_space_constraint(gu, pltpu.VMEM), pltpu.with_memory_space_constraint(gd, pltpu.VMEM))

    return jax.shard_map(device_grads, mesh=mesh, in_specs=(tok_spec, tok_spec, len_spec, w_spec, w_spec), out_specs=(w_spec, w_spec), check_vma=False)
```

```python
import functools

import jax
import jax.numpy as jnp
from jax import lax
from jax.experimental import pallas as pl
from jax.experimental.pallas import tpu as pltpu
from jax.sharding import PartitionSpec as P

F32, BF16 = jnp.float32, jnp.bfloat16
MESH_ID = pl.DeviceIdType.MESH
SQRT_2_OVER_PI = 0.7978845608028654
CUBIC = 0.044715
NT_DIMS = (((1,), (1,)), ((), ()))

FC = 256
RING = 4
SUBS = 4
PH_ROWS = (128, 32, 8)
PH_OFF = (0, 384, 480)
R_ROWS = 504
W_SLOTS = 3
P_SLOTS = 2
STAGES = ("pair", "rs0b", "rs0c", "rs1b", "rs1c", "rs2b", "rs2c", "ag2b", "ag2c", "ag1b", "ag1c", "ag0b", "ag0c")

OPENING = 4
MIN_LEN = 128
TABLE = (
    (),
    (),
    (),
    (),
    ((0, 0),),
    (),
    ((1, 0),),
    ((0, 1),),
    ((2, 0),),
    ((1, 1), (0, 2),),
    ((4, 0), (0, 3),),
    ((1, 2), (2, 1),),
    ((6, 0), (0, 4), (1, 3),),
    ((2, 2),),
    ((8, 0), (4, 1), (1, 4), (0, 5),),
    ((2, 3),),
    ((4, 2), (6, 1), (0, 6), (2, 4),),
    ((1, 5), (10, 0),),
    ((6, 2), (0, 7), (8, 1), (4, 3),),
    ((2, 5), (3, 4), (1, 6),),
    ((1, 7), (0, 8),),
    ((6, 3), (10, 1), (4, 4), (3, 5), (8, 2),),
    ((2, 6), (1, 8), (11, 0), (2, 7), (0, 9),),
    (),
    ((5, 4), (3, 6), (4, 5), (0, 10), (10, 2),),
    ((2, 8),),
    ((5, 5), (6, 4), (4, 6), (1, 9), (3, 7), (8, 3), (0, 11),),
    ((1, 10), (3, 8), (11, 2),),
    ((5, 6), (6, 5), (4, 7), (7, 4), (2, 9), (0, 12),),
    ((1, 11), (10, 3),),
    ((2, 10), (4, 8), (6, 6), (0, 13), (3, 9), (8, 4), (5, 7), (7, 5),),
    ((2, 11), (1, 12), (11, 1),),
    ((7, 6), (5, 8), (0, 14),),
    (),
    ((3, 11), (4, 9), (3, 10), (1, 13), (8, 5), (6, 7), (9, 4), (2, 12), (8, 6), (0, 15), (5, 9), (4, 11), (6, 8), (1, 14), (2, 13), (3, 12), (9, 6), (4, 10), (7, 7), (9, 5), (10, 4), (6, 9), (1, 15), (5, 10), (7, 8), (4, 12), (5, 11), (2, 14), (10, 6), (3, 13), (8, 7), (5, 12), (7, 9), (6, 10), (8, 8), (2, 15), (3, 14), (6, 11), (10, 5), (7, 10), (8, 9), (4, 13), (9, 7), (6, 12), (3, 15), (11, 6), (7, 11), (4, 14), (11, 4), (11, 5), (8, 10), (4, 15), (9, 8), (7, 12), (5, 13), (5, 14), (8, 11), (10, 7), (9, 9), (11, 3), (12, 2), (5, 15), (6, 13), (9, 10), (6, 14), (10, 8), (9, 11), (8, 12), (7, 13), (6, 15), (7, 14), (11, 7), (10, 9), (11, 8), (7, 15), (8, 13), (9, 12), (8, 14), (10, 10), (12, 3), (11, 9), (12, 6), (8, 15), (9, 13), (12, 4), (12, 1), (10, 12), (12, 5), (9, 14), (10, 11), (9, 15), (10, 13), (12, 9), (10, 14), (10, 15), (12, 0), (11, 13), (11, 12), (12, 8), (11, 11), (11, 15), (12, 7), (11, 10), (11, 14), (12, 11), (12, 13), (12, 15), (12, 12), (12, 10), (12, 14),),
)
DIRECT = (3, 3, 3, 3, 0, 0, 0, 0, 0, 0, 0, 0, 0, 0, 0, 0)
LANES = 128
SHAPES = (
    3, 0, 0, 6, 6, 6, 0, 2, 0, 6, 6, 6, 0, 0, 0, 6, 2, 5, 0, 0, 0, 6, 2, 6, 6, 0, 0, 6, 6, 7, 0, 0,
    0, 6, 6, 6, 0, 6, 0, 6, 6, 6, 0, 0, 6, 6, 6, 6, 5, 0, 4, 6, 6, 6, 0, 0, 5, 6, 6, 6, 0, 0, 4, 6,
)


def is_direct(t, phase):
    return phase > 0 and DIRECT[t % len(DIRECT)] >> (phase - 1) & 1 == 1


def stages_of(t):
    return [k for k, n in enumerate(STAGES) if not (n[3:] == "b" and is_direct(t, int(n[2])))]


def program(n_ticks):
    if n_ticks == 16 and TABLE:
        return TABLE
    last = OPENING + 2 * (n_ticks - 1)
    slots = [[] for _ in range(last + 1)]
    for t in range(n_ticks):
        for k, s in enumerate(stages_of(t)):
            slots[min(OPENING + 2 * t + k, last)].append((s, t))
    slots[-1].sort()
    return slots


def gelu_and_slope(u):
    u2 = u * u
    half = 0.5 + 0.5 * jnp.tanh(u * (SQRT_2_OVER_PI + (CUBIC * SQRT_2_OVER_PI) * u2))
    a = u * half
    return a, half + (a * (1.0 - half)) * (2.0 * SQRT_2_OVER_PI + (6.0 * CUBIC * SQRT_2_OVER_PI) * u2)


def subs_of(t):
    blocks = []
    for g in range(SUBS * t, SUBS * t + SUBS):
        code, a = SHAPES[g % len(SHAPES)], g % 3
        b, c = ((a + 1) % 3, (a + 2) % 3) if code % 2 == 0 else ((a + 2) % 3, (a + 1) % 3)
        dirs = (1 if g // 3 % 2 == 0 else -1, -1 if code & 2 else 1, -1 if code & 4 else 1)
        blocks.append((g, (a, b, c), dirs))
    return blocks


def kernel(n_ticks, n_tok, n_micro, sems, *refs):
    pl.run_scoped(functools.partial(body, n_ticks, n_tok, n_micro, refs), *sems)


def body(n_ticks, n_tok, n_micro, refs,
         in_sem, w_local, w_send, w_recv, p_send, p_recv, rs1, rs2, ag1, ag2, send0, send1, out_send,
         g_free, w_credit, r_credit):
    (x_hbm, dy_hbm, len_ref, wu_hbm, wd_hbm, GU, GD,
     X, DY, XT, WU, WD, AT, DH, SU, SD, RU, RD, R, E) = refs
    tok = n_tok // n_micro
    half_ff = n_ticks * 128
    rep = lax.axis_index("replica")
    me = lax.axis_index("fsdp")
    mate = 1 - me

    def dev(replica, core):
        return (0, replica, core)

    strides = [RING**a for a in range(3)]
    coord = [(rep // s) % RING for s in strides]
    quarter = [[coord[a]] + [(coord[a] + k) % RING for k in range(1, RING)] for a in range(3)]
    near = [{d: rep + strides[a] * (quarter[a][d % RING] - coord[a]) for d in (1, -1, 2, 3)} for a in range(3)]

    def row_in_quarter(axes, phase):
        row = 0
        for p in range(1, phase):
            row = row + coord[axes[p]] * PH_ROWS[p]
        return row

    def g_part(g, q, row, n):
        t, s = g // SUBS, g % SUBS
        if s < 2:
            start = q * 128 + row
            return GU.at[pl.ds(pl.multiple_of(start, 8), n), pl.ds(s * half_ff + t * 128, 128)]
        start = t * 128 + row
        if not isinstance(start, int):
            start = pl.multiple_of(start, 8)
        return GD.at[pl.ds(start, n), pl.ds(pl.multiple_of((s - 2) * 512 + q * 128, 128), 128)]

    def r_part(g, start, n):
        return R.at[pl.ds(g * R_ROWS + start, n)]

    def e_part(g, row, n):
        start = g * PH_ROWS[0] + row
        if not isinstance(start, int):
            start = pl.multiple_of(start, 8)
        return E.at[pl.ds(start, n)]

    def wait_rows(sem, n):
        ref = R.at[pl.ds(0, n)]
        pltpu.make_async_copy(ref, ref, sem).wait()

    barrier = pltpu.get_barrier_semaphore()
    for a in range(3):
        for d in (1, -1, 2):
            pl.semaphore_signal(barrier, inc=1, device_id=dev(near[a][d], me), device_id_type=MESH_ID)
    pl.semaphore_signal(barrier, inc=1, device_id=dev(rep, mate), device_id_type=MESH_ID)

    n_cols = X.shape[0]

    def x_copy(k):
        return [pltpu.make_async_copy(x_hbm.at[k, :, pl.ds(c * LANES, LANES)], X.at[c, pl.ds(k * tok, tok)], in_sem.at[k]) for c in range(n_cols)]

    def dy_copy(k):
        return [pltpu.make_async_copy(dy_hbm.at[k, :, pl.ds(c * LANES, LANES)], DY.at[c, pl.ds(k * tok, tok)], in_sem.at[n_micro + k]) for c in range(n_cols)]

    def landed(ref, k, sem):
        block = ref.at[:, pl.ds(k * tok, tok)]
        pltpu.make_async_copy(block, block, sem).wait()

    def w_parts(t):
        slot = t % W_SLOTS
        lo = pl.multiple_of(t * 128, 128)
        hi = pl.multiple_of(half_ff + t * 128, 128)
        up_rows = pl.ds(pl.multiple_of(me * 512, 512), 512)
        down_rows = pl.ds(pl.multiple_of(me * 128, 128), 128)
        return (
            (wu_hbm.at[0, :, pl.ds(lo, 128)], WU.at[slot, up_rows, pl.ds(0, 128)]),
            (wu_hbm.at[0, :, pl.ds(hi, 128)], WU.at[slot, up_rows, pl.ds(128, 128)]),
            (wd_hbm.at[0, pl.ds(lo, 128), :], WD.at[slot, down_rows, :]),
        )

    def start_w(t):
        for s, d in w_parts(t):
            pltpu.make_async_remote_copy(
                s, d, w_send.at[t % W_SLOTS], w_recv.at[t % W_SLOTS],
                device_id=dev(rep, mate), device_id_type=MESH_ID).start()

        for s, d in w_parts(t):
            pltpu.make_async_copy(s, d, w_local.at[t % W_SLOTS]).start()

    def wait_w(t):
        slot = t % W_SLOTS
        ref = WU.at[slot]
        for sem in (w_local, w_recv, w_send):
            pltpu.make_async_copy(ref, ref, sem.at[slot]).wait()

    def load_tokens(part):
        for k in range(part * n_micro // 2, (part + 1) * n_micro // 2):
            for copy in x_copy(k) + dy_copy(k):
                copy.start()

    load_tokens(0)
    with jax.named_scope("entry"):
        pl.semaphore_wait(barrier, 10)
    start_w(0)
    load_tokens(1)

    mb = min(128, tok)
    clean = MIN_LEN if tok > MIN_LEN else 0

    def mask_micro(k):
        with jax.named_scope("dywait"):
            landed(DY, k, in_sem.at[n_micro + k])
        n_valid = len_ref[k]

        def mask_rows(s, carry):
            rows = pl.ds(pl.multiple_of(k * tok + clean + s * mb, mb), mb)
            at = clean + s * mb + lax.broadcasted_iota(jnp.int32, (mb, LANES), 0)
            keep = jnp.where(at < n_valid, 1.0, 0.0).astype(BF16)
            for c in range(n_cols):
                DY[c, rows, :] = DY[c, rows, :] * keep
            return carry

        lax.fori_loop(0, (tok - clean) // mb, mask_rows, 0)

    def wide(ref, rows, lo, hi):
        return jnp.concatenate([ref[c, rows, :] for c in range(lo, hi)], axis=1)

    cb = min(256, n_tok // 2)

    def hidden(t, lo, hi, turn=False):
        slot = t % W_SLOTS
        for at in range(lo, hi, cb):
            rows = pl.ds(at, cb)
            if turn:
                for c in range(n_cols):
                    XT[pl.ds(c * LANES, LANES), rows] = X[c, rows, :].T
            h = jnp.dot(wide(X, rows, 0, n_cols), WU[slot], preferred_element_type=F32).astype(BF16).astype(F32)
            da = lax.dot_general(wide(DY, rows, 0, n_cols), WD[slot], NT_DIMS, preferred_element_type=F32)
            a, slope = gelu_and_slope(h)
            AT[:, rows] = a.astype(BF16).T
            DH[rows, :] = (da * slope).astype(BF16)

    def free_w(t):
        @pl.when(t + W_SLOTS < n_ticks)
        def _():
            pl.semaphore_signal(w_credit, inc=1, device_id=dev(rep, mate), device_id_type=MESH_ID)

    def more_w(t):
        @pl.when((t < n_ticks) & (t >= W_SLOTS))
        def _():
            pl.semaphore_wait(w_credit, 1)

        @pl.when(t < n_ticks)
        def _():
            start_w(t)

    def send_to_mate(t, part):
        slot = t % P_SLOTS
        if part == 0:
            src, dst = SU.at[slot, pl.ds(pl.multiple_of(mate * 512, 512), 512)], RU.at[slot]
        else:
            src, dst = SD.at[slot, pl.ds(pl.multiple_of(mate * 128, 128), 128)], RD.at[slot]
        pltpu.make_async_remote_copy(
            src, dst, p_send.at[slot], p_recv.at[slot], device_id=dev(rep, mate), device_id_type=MESH_ID).start()

    def take_pair_room(t):
        @pl.when(t >= P_SLOTS)
        def _():
            pl.semaphore_wait(r_credit, 1)

    def up(t):
        slot = t % P_SLOTS
        for s in range(2):
            rows = pl.ds(s * 512, 512)
            SU[slot, rows, :] = jnp.dot(XT[rows, :], DH[...], preferred_element_type=F32)

    def down(t):
        slot = t % P_SLOTS
        for s in range(2):
            cols = pl.ds(s * 512, 512)
            SD[slot, :, cols] = jnp.dot(AT[...], wide(DY, slice(None), 4 * s, 4 * s + 4), preferred_element_type=F32)

    def send(sent, src, dst, recv, to):
        pltpu.make_async_remote_copy(
            src, dst, sent, recv, device_id=dev(to, me), device_id_type=MESH_ID).start()

    def pair_stage(t):
        slot = t % P_SLOTS
        whole = SU.at[slot]
        pltpu.make_async_copy(whole, whole, p_recv.at[slot]).wait()
        own = pl.ds(pl.multiple_of(me * 512, 512), 512)
        for s in range(2):
            cols = pl.ds(s * 128, 128)
            GU[:, pl.ds(s * half_ff + t * 128, 128)] = SU[slot, own, cols] + RU[slot, :, cols]
        own = pl.ds(pl.multiple_of(me * 128, 128), 128)
        GD[pl.ds(t * 128, 128), :] = SD[slot, own, :] + RD[slot]
        pltpu.make_async_copy(whole, whole, p_send.at[slot]).wait()
        if t + P_SLOTS < n_ticks:
            pl.semaphore_signal(r_credit, inc=1, device_id=dev(rep, mate), device_id_type=MESH_ID)
        rs_a(t, 0)

    def rs_a(t, p):
        sent = (send0 if p == 0 else send1).at[t]
        m, off = PH_ROWS[p], PH_OFF[p]
        if is_direct(t, p):
            for k in (2, 1, 3):
                for g, axes, dirs in subs_of(t):
                    a = axes[p]
                    src = g_part(g, coord[axes[0]], row_in_quarter(axes, p) + quarter[a][k] * m, m)
                    send(sent, src, r_part(g, off + (k - 1) * m, m), rs2.at[t * 3 + p], near[a][k])
            return
        for relay in (True, False):
            for g, axes, dirs in subs_of(t):
                a, d = axes[p], dirs[p]
                q = quarter[a][2 if relay else -d % RING]
                src = g_part(g, q, 0, m) if p == 0 else g_part(g, coord[axes[0]], row_in_quarter(axes, p) + q * m, m)
                if relay:
                    send(sent, src, r_part(g, off, m), rs1.at[t * 3 + p], near[a][d])
                else:
                    send(sent, src, r_part(g, off + m, m), rs2.at[t * 3 + p], near[a][-d])

    def rs_b(t, p):
        sent = (send0 if p == 0 else send1).at[t]
        m, off = PH_ROWS[p], PH_OFF[p]
        wait_rows(rs1.at[t * 3 + p], SUBS * m)
        for g, axes, dirs in subs_of(t):
            a, d = axes[p], dirs[p]
            q = quarter[a][d % RING]
            part = g_part(g, q, 0, m) if p == 0 else g_part(g, coord[axes[0]], row_in_quarter(axes, p) + q * m, m)
            part[...] = part[...] + r_part(g, off, m)[...]
            send(sent, part, r_part(g, off + 2 * m, m), rs2.at[t * 3 + p], near[a][d])

    def rs_c(t, p):
        m, off = PH_ROWS[p], PH_OFF[p]
        straight = is_direct(t, p)
        wait_rows(rs2.at[t * 3 + p], (3 if straight else 2) * SUBS * m)
        for g, axes, dirs in subs_of(t):
            row = 0 if p == 0 else row_in_quarter(axes, p) + coord[axes[p]] * m
            part = g_part(g, coord[axes[0]], row, m)
            out = e_part(g, row, m) if p == 2 else part
            total = part[...] + (r_part(g, off + m, m)[...] + r_part(g, off + 2 * m, m)[...])
            out[...] = total + r_part(g, off, m)[...] if straight else total
        if p < 2:
            rs_a(t, p + 1)
        else:
            ag_a(t, 2)
        if p == 1:
            wait_rows(send0.at[t], 3 * SUBS * PH_ROWS[0])
            for a in sorted({axes[0] for _, axes, _ in subs_of(t)}):
                for d in (1, -1):
                    pl.semaphore_signal(g_free.at[t], inc=1, device_id=dev(near[a][d], me), device_id_type=MESH_ID)

    def ag_part(g, axes, p, q):
        if p == 0:
            return g_part(g, q, 0, PH_ROWS[0])
        return e_part(g, row_in_quarter(axes, p) + q * PH_ROWS[p], PH_ROWS[p])

    def ag_a(t, p):
        if p == 0:
            pl.semaphore_wait(g_free.at[t], 2 * len({axes[0] for _, axes, _ in subs_of(t)}))
        if is_direct(t, p):
            for k in (2, 1, 3):
                for g, axes, dirs in subs_of(t):
                    part = ag_part(g, axes, p, coord[axes[p]])
                    send(out_send.at[t], part, part, ag2.at[t * 3 + p], near[axes[p]][k])
            return
        for recv, sign in ((ag1, 1), (ag2, -1)):
            for g, axes, dirs in subs_of(t):
                a, d = axes[p], dirs[p]
                part = ag_part(g, axes, p, coord[a])
                src = e_part(g, 0, PH_ROWS[0]) if p == 0 else part
                send(out_send.at[t], src, part, recv.at[t * 3 + p], near[a][sign * d])
        if p == 0:
            wait_rows(send1.at[t], 3 * SUBS * (PH_ROWS[1] + PH_ROWS[2]))
            for g, axes, dirs in subs_of(t):
                g_part(g, coord[axes[0]], 0, PH_ROWS[0])[...] = e_part(g, 0, PH_ROWS[0])[...]

    def ag_b(t, p):
        wait_rows(ag1.at[t * 3 + p], SUBS * PH_ROWS[p])
        for g, axes, dirs in subs_of(t):
            a, d = axes[p], dirs[p]
            part = ag_part(g, axes, p, quarter[a][-d % RING])
            send(out_send.at[t], part, part, ag2.at[t * 3 + p], near[a][d])

    def ag_c(t, p):
        wait_rows(ag2.at[t * 3 + p], (3 if is_direct(t, p) else 2) * SUBS * PH_ROWS[p])
        if p > 0:
            ag_a(t, p - 1)

    def run(ops):
        for s, t in ops:
            name = STAGES[s]
            with jax.named_scope(name):
                if name == "pair":
                    pair_stage(t)
                else:
                    p = int(name[2])
                    {"rsb": rs_b, "rsc": rs_c, "agb": ag_b, "agc": ag_c}[name[:2] + name[3]](t, p)

    slots = program(n_ticks)

    def pick(t, first, lo, hi):
        lists = [slots[first(k)] for k in range(lo, hi)]
        if not any(lists):
            return
        if hi - lo == 1:
            run(lists[0])
            return
        mid = (lo + hi) // 2
        pl.when(t < mid)(lambda: pick(t, first, lo, mid))
        pl.when(t >= mid)(lambda: pick(t, first, mid, hi))

    n_half = n_tok // 2
    for part in range(2):
        for k in range(part * n_micro // 2, (part + 1) * n_micro // 2):
            with jax.named_scope("mask"):
                mask_micro(k)
            with jax.named_scope("xwait"):
                landed(X, k, in_sem.at[k])
        if part == 0:
            with jax.named_scope("wwait"):
                wait_w(0)
        with jax.named_scope("hidfirst"):
            hidden(0, part * n_half, (part + 1) * n_half, turn=True)
        if part == 0 and n_ticks > 1:
            start_w(1)
        run(slots[part])
    free_w(0)
    more_w(2)
    with jax.named_scope("upfirst"):
        up(0)
    send_to_mate(0, 0)
    run(slots[2])
    with jax.named_scope("downfirst"):
        down(0)
    send_to_mate(0, 1)
    run(slots[3])

    def tick(t, carry):
        with jax.named_scope("wwait"):
            wait_w(t)
        with jax.named_scope("hidden"):
            hidden(t, 0, n_tok)
        free_w(t)
        pick(t, lambda k: OPENING + 2 * k - 2, 1, n_ticks)
        more_w(t + 2)
        take_pair_room(t)
        with jax.named_scope("grad"):
            up(t)
            down(t)
            send_to_mate(t, 0)
            send_to_mate(t, 1)
        pick(t, lambda k: OPENING + 2 * k - 1, 1, n_ticks)
        return carry

    lax.fori_loop(1, n_ticks, tick, 0)
    run(slots[-1])
    for t in range(n_ticks):
        wait_rows(out_send.at[t], SUBS * R_ROWS)


FLUSH = 8


def flush(gu, gd, gu_hbm, gd_hbm, sem):
    copies = []
    for k in range(FLUSH):
        for ref, out, s in ((gu, gu_hbm, 0), (gd, gd_hbm, 1)):
            rows = pl.ds(k * (ref.shape[0] // FLUSH), ref.shape[0] // FLUSH)
            copies.append(pltpu.make_async_copy(ref.at[rows], out.at[0, rows], sem.at[2 * k + s]))
    for copy in copies:
        copy.start()
    for copy in copies:
        copy.wait()


def solution(mesh):
    tok_spec = P(None, ("model", "replica", "fsdp"), None)
    len_spec = P(None, ("model", "replica", "fsdp"))
    w_spec = P(None, ("model", "fsdp"), None)

    def device_grads(x_in, dy_out, lengths, w_up, w_down):
        n_micro, tok, d = x_in.shape
        n_tok = n_micro * tok
        d_ff = w_up.shape[2]
        n_ticks = d_ff // FC
        any_spec = pl.BlockSpec(memory_space=pl.ANY)
        dma = pltpu.SemaphoreType.DMA
        regular = pltpu.SemaphoreType.REGULAR
        sems = [
            dma((2 * n_micro,)),
            dma((W_SLOTS,)),
            dma((W_SLOTS,)),
            dma((W_SLOTS,)),
            dma((P_SLOTS,)),
            dma((P_SLOTS,)),
            dma((3 * n_ticks,)),
            dma((3 * n_ticks,)),
            dma((3 * n_ticks,)),
            dma((3 * n_ticks,)),
            dma((n_ticks,)),
            dma((n_ticks,)),
            dma((n_ticks,)),
            regular((n_ticks,)),
            regular,
            regular,
        ]
        gu, gd = pl.pallas_call(
            functools.partial(kernel, n_ticks, n_tok, n_micro, sems),
            out_shape=(
                pltpu.VMEM((d // 2, d_ff), F32),
                pltpu.VMEM((d_ff // 2, d), F32),
            ),
            in_specs=[any_spec, any_spec, pl.BlockSpec(memory_space=pltpu.SMEM), any_spec, any_spec],
            out_specs=(pl.BlockSpec(memory_space=pltpu.VMEM),) * 2,
            scratch_shapes=[
                pltpu.VMEM((d // LANES, n_tok, LANES), BF16),
                pltpu.VMEM((d // LANES, n_tok, LANES), BF16),
                pltpu.VMEM((d, n_tok), BF16),
                pltpu.VMEM((W_SLOTS, d, FC), BF16),
                pltpu.VMEM((W_SLOTS, FC, d), BF16),
                pltpu.VMEM((FC, n_tok), BF16),
                pltpu.VMEM((n_tok, FC), BF16),
                pltpu.VMEM((P_SLOTS, d, FC), F32),
                pltpu.VMEM((P_SLOTS, FC, d), F32),
                pltpu.VMEM((P_SLOTS, d // 2, FC), F32),
                pltpu.VMEM((P_SLOTS, FC // 2, d), F32),
                pltpu.VMEM((n_ticks * SUBS * R_ROWS, 128), F32),
                pltpu.VMEM((n_ticks * SUBS * PH_ROWS[0], 128), F32),
            ],
            compiler_params=pltpu.CompilerParams(
                collective_id=0, has_side_effects=True, vmem_limit_bytes=67043328 - (16 << 20)),
            name="grads",
        )(x_in, dy_out, lengths.reshape(n_micro), w_up, w_down)
        vmem = pl.BlockSpec(memory_space=pltpu.VMEM)
        return pl.pallas_call(
            flush,
            out_shape=(
                jax.ShapeDtypeStruct(w_up.shape, F32),
                jax.ShapeDtypeStruct(w_down.shape, F32),
            ),
            in_specs=[vmem, vmem],
            out_specs=(any_spec, any_spec),
            scratch_shapes=[dma((2 * FLUSH,))],
            compiler_params=pltpu.CompilerParams(vmem_limit_bytes=1 << 20),
            name="flush",
        )(pltpu.with_memory_space_constraint(gu, pltpu.VMEM), pltpu.with_memory_space_constraint(gd, pltpu.VMEM))

    return jax.shard_map(device_grads, mesh=mesh, in_specs=(tok_spec, tok_spec, len_spec, w_spec, w_spec), out_specs=(w_spec, w_spec), check_vma=False)
```

```python
import functools

import jax
import jax.numpy as jnp
from jax import lax
from jax.experimental import pallas as pl
from jax.experimental.pallas import tpu as pltpu
from jax.sharding import PartitionSpec as P

F32, BF16 = jnp.float32, jnp.bfloat16
MESH_ID = pl.DeviceIdType.MESH
SQRT_2_OVER_PI = 0.7978845608028654
CUBIC = 0.044715
NT_DIMS = (((1,), (1,)), ((), ()))

FC = 256
RING = 4
SUBS = 4
PH_ROWS = (128, 32, 8)
PH_OFF = (0, 384, 480)
R_ROWS = 504
W_SLOTS = 3
P_SLOTS = 2
STAGES = ("pair", "rs0b", "rs0c", "rs1b", "rs1c", "rs2b", "rs2c", "ag2b", "ag2c", "ag1b", "ag1c", "ag0b", "ag0c")

OPENING = 4
MIN_LEN = 128
TABLE = (
    (),
    (),
    (),
    (),
    ((0, 0),),
    (),
    ((1, 0),),
    ((0, 1),),
    ((2, 0),),
    ((1, 1), (0, 2),),
    ((4, 0), (0, 3),),
    ((1, 2), (2, 1),),
    ((6, 0), (0, 4), (1, 3),),
    ((2, 2),),
    ((4, 1), (8, 0), (1, 4), (0, 5),),
    ((4, 2), (2, 3),),
    ((6, 1), (0, 6),),
    ((6, 2), (1, 5), (2, 4), (10, 0),),
    ((4, 3), (1, 6), (8, 1),),
    ((0, 7), (8, 2),),
    ((2, 5), (3, 4), (0, 8),),
    ((2, 6), (1, 7), (11, 0), (10, 1),),
    (),
    ((6, 3), (3, 5), (4, 4), (1, 8), (3, 6), (0, 9),),
    ((2, 7), (0, 10),),
    ((4, 5), (4, 6), (5, 4), (2, 8), (10, 2),),
    ((1, 9), (3, 7), (0, 11), (1, 10),),
    ((5, 6), (5, 5), (3, 8), (6, 4), (8, 3),),
    ((0, 12), (11, 2),),
    ((4, 7), (12, 0), (2, 10), (11, 1), (2, 9), (6, 6),),
    ((6, 5), (4, 8), (7, 4), (1, 11), (10, 3),),
    ((1, 12), (3, 10), (3, 9), (5, 7), (0, 13), (5, 8), (7, 5), (7, 6),),
    ((2, 11), (8, 4), (0, 14),),
    (),
    ((4, 9), (4, 10), (2, 12), (8, 6), (1, 13), (3, 11), (6, 8), (8, 5), (9, 4), (0, 15), (5, 9), (5, 10), (3, 12), (9, 6), (6, 7), (1, 14), (2, 13), (4, 11), (10, 4), (1, 15), (6, 10), (5, 11), (4, 12), (7, 7), (6, 9), (2, 14), (9, 5), (3, 13), (7, 8), (10, 6), (6, 11), (8, 7), (7, 9), (7, 10), (2, 15), (5, 12), (3, 14), (4, 13), (10, 5), (8, 8), (8, 9), (7, 11), (3, 15), (9, 7), (8, 10), (6, 12), (4, 14), (5, 13), (11, 6), (11, 4), (11, 5), (6, 13), (5, 14), (4, 15), (9, 8), (7, 12), (9, 10), (9, 9), (10, 7), (8, 11), (6, 14), (5, 15), (7, 13), (11, 3), (10, 8), (8, 12), (7, 14), (12, 6), (6, 15), (9, 11), (10, 9), (11, 7), (8, 13), (8, 14), (7, 15), (12, 4), (9, 12), (10, 10), (11, 8), (11, 9), (12, 3), (8, 15), (9, 14), (10, 12), (9, 13), (10, 11), (9, 15), (10, 14), (10, 13), (12, 9), (10, 15), (11, 10), (11, 12), (11, 11), (12, 7), (11, 15), (11, 14), (11, 13), (12, 11), (12, 2), (12, 15), (12, 12), (12, 5), (12, 1), (12, 8), (12, 10), (12, 14), (12, 13),),
)
DIRECT = (3, 3, 3, 3, 0, 0, 0, 0, 0, 0, 0, 0, 0, 0, 0, 0)
LANES = 128
SHAPES = (
    4, 0, 6, 5, 12, 5, 4, 13, 8, 7, 4, 10, 4, 0, 6, 2, 8, 9, 6, 12, 0, 6, 14, 6, 0, 10, 8, 0, 8, 5, 2, 15,
    12, 4, 0, 14, 14, 0, 4, 14, 14, 0, 2, 10, 4, 8, 2, 6, 10, 6, 6, 4, 6, 2, 1, 4, 8, 6, 6, 9, 14, 6, 0, 10,
)


def is_direct(t, phase):
    return phase > 0 and DIRECT[t % len(DIRECT)] >> (phase - 1) & 1 == 1


def stages_of(t):
    return [k for k, n in enumerate(STAGES) if not (n[3:] == "b" and is_direct(t, int(n[2])))]


def program(n_ticks):
    if n_ticks == 16 and TABLE:
        return TABLE
    last = OPENING + 2 * (n_ticks - 1)
    slots = [[] for _ in range(last + 1)]
    for t in range(n_ticks):
        for k, s in enumerate(stages_of(t)):
            slots[min(OPENING + 2 * t + k, last)].append((s, t))
    slots[-1].sort()
    return slots


def gelu_and_slope(u):
    u2 = u * u
    half = 0.5 + 0.5 * jnp.tanh(u * (SQRT_2_OVER_PI + (CUBIC * SQRT_2_OVER_PI) * u2))
    a = u * half
    return a, half + (a * (1.0 - half)) * (2.0 * SQRT_2_OVER_PI + (6.0 * CUBIC * SQRT_2_OVER_PI) * u2)


def subs_of(t):
    blocks = []
    for g in range(SUBS * t, SUBS * t + SUBS):
        code, a = SHAPES[g % len(SHAPES)], g % 3
        b, c = ((a + 1) % 3, (a + 2) % 3) if code % 2 == 0 else ((a + 2) % 3, (a + 1) % 3)
        first = 1 if g // 3 % 2 == 0 else -1
        dirs = (-first if code & 8 else first, -1 if code & 2 else 1, -1 if code & 4 else 1)
        blocks.append((g, (a, b, c), dirs))
    return blocks


def kernel(n_ticks, n_tok, n_micro, sems, *refs):
    pl.run_scoped(functools.partial(body, n_ticks, n_tok, n_micro, refs), *sems)


def body(n_ticks, n_tok, n_micro, refs,
         in_sem, w_local, w_send, w_recv, p_send, p_recv, rs1, rs2, ag1, ag2, send0, send1, out_send,
         g_free, w_credit, r_credit):
    (x_hbm, dy_hbm, len_ref, wu_hbm, wd_hbm, GU, GD,
     X, DY, XT, WU, WD, AT, DH, SU, SD, RU, RD, R, E) = refs
    tok = n_tok // n_micro
    half_ff = n_ticks * 128
    rep = lax.axis_index("replica")
    me = lax.axis_index("fsdp")
    mate = 1 - me

    def dev(replica, core):
        return (0, replica, core)

    strides = [RING**a for a in range(3)]
    coord = [(rep // s) % RING for s in strides]
    quarter = [[coord[a]] + [(coord[a] + k) % RING for k in range(1, RING)] for a in range(3)]
    near = [{d: rep + strides[a] * (quarter[a][d % RING] - coord[a]) for d in (1, -1, 2, 3)} for a in range(3)]

    def row_in_quarter(axes, phase):
        row = 0
        for p in range(1, phase):
            row = row + coord[axes[p]] * PH_ROWS[p]
        return row

    def g_part(g, q, row, n):
        t, s = g // SUBS, g % SUBS
        if s < 2:
            start = q * 128 + row
            return GU.at[pl.ds(pl.multiple_of(start, 8), n), pl.ds(s * half_ff + t * 128, 128)]
        start = t * 128 + row
        if not isinstance(start, int):
            start = pl.multiple_of(start, 8)
        return GD.at[pl.ds(start, n), pl.ds(pl.multiple_of((s - 2) * 512 + q * 128, 128), 128)]

    def r_part(g, start, n):
        return R.at[pl.ds(g * R_ROWS + start, n)]

    def e_part(g, row, n):
        start = g * PH_ROWS[0] + row
        if not isinstance(start, int):
            start = pl.multiple_of(start, 8)
        return E.at[pl.ds(start, n)]

    def wait_rows(sem, n):
        ref = R.at[pl.ds(0, n)]
        pltpu.make_async_copy(ref, ref, sem).wait()

    barrier = pltpu.get_barrier_semaphore()
    for a in range(3):
        for d in (1, -1, 2):
            pl.semaphore_signal(barrier, inc=1, device_id=dev(near[a][d], me), device_id_type=MESH_ID)
    pl.semaphore_signal(barrier, inc=1, device_id=dev(rep, mate), device_id_type=MESH_ID)

    n_cols = X.shape[0]

    def x_copy(k):
        return [pltpu.make_async_copy(x_hbm.at[k, :, pl.ds(c * LANES, LANES)], X.at[c, pl.ds(k * tok, tok)], in_sem.at[k]) for c in range(n_cols)]

    def dy_copy(k):
        return [pltpu.make_async_copy(dy_hbm.at[k, :, pl.ds(c * LANES, LANES)], DY.at[c, pl.ds(k * tok, tok)], in_sem.at[n_micro + k]) for c in range(n_cols)]

    def landed(ref, k, sem):
        block = ref.at[:, pl.ds(k * tok, tok)]
        pltpu.make_async_copy(block, block, sem).wait()

    def w_parts(t):
        slot = t % W_SLOTS
        lo = pl.multiple_of(t * 128, 128)
        hi = pl.multiple_of(half_ff + t * 128, 128)
        up_rows = pl.ds(pl.multiple_of(me * 512, 512), 512)
        down_rows = pl.ds(pl.multiple_of(me * 128, 128), 128)
        return (
            (wu_hbm.at[0, :, pl.ds(lo, 128)], WU.at[slot, up_rows, pl.ds(0, 128)]),
            (wu_hbm.at[0, :, pl.ds(hi, 128)], WU.at[slot, up_rows, pl.ds(128, 128)]),
            (wd_hbm.at[0, pl.ds(lo, 128), :], WD.at[slot, down_rows, :]),
        )

    def start_w(t):
        for s, d in w_parts(t):
            pltpu.make_async_remote_copy(
                s, d, w_send.at[t % W_SLOTS], w_recv.at[t % W_SLOTS],
                device_id=dev(rep, mate), device_id_type=MESH_ID).start()

        for s, d in w_parts(t):
            pltpu.make_async_copy(s, d, w_local.at[t % W_SLOTS]).start()

    def wait_w(t):
        slot = t % W_SLOTS
        ref = WU.at[slot]
        for sem in (w_local, w_recv, w_send):
            pltpu.make_async_copy(ref, ref, sem.at[slot]).wait()

    def load_tokens(part):
        for k in range(part * n_micro // 2, (part + 1) * n_micro // 2):
            for copy in x_copy(k) + dy_copy(k):
                copy.start()

    load_tokens(0)
    with jax.named_scope("entry"):
        pl.semaphore_wait(barrier, 10)
    start_w(0)
    load_tokens(1)

    mb = min(128, tok)
    clean = MIN_LEN if tok > MIN_LEN else 0

    def mask_micro(k):
        with jax.named_scope("dywait"):
            landed(DY, k, in_sem.at[n_micro + k])
        n_valid = len_ref[k]

        def mask_rows(s, carry):
            rows = pl.ds(pl.multiple_of(k * tok + clean + s * mb, mb), mb)
            at = clean + s * mb + lax.broadcasted_iota(jnp.int32, (mb, LANES), 0)
            keep = jnp.where(at < n_valid, 1.0, 0.0).astype(BF16)
            for c in range(n_cols):
                DY[c, rows, :] = DY[c, rows, :] * keep
            return carry

        lax.fori_loop(0, (tok - clean) // mb, mask_rows, 0)

    def wide(ref, rows, lo, hi):
        return jnp.concatenate([ref[c, rows, :] for c in range(lo, hi)], axis=1)

    cb = min(256, n_tok // 2)

    def hidden(t, lo, hi, turn=False):
        slot = t % W_SLOTS
        for at in range(lo, hi, cb):
            rows = pl.ds(at, cb)
            if turn:
                for c in range(n_cols):
                    XT[pl.ds(c * LANES, LANES), rows] = X[c, rows, :].T
            h = jnp.dot(wide(X, rows, 0, n_cols), WU[slot], preferred_element_type=F32).astype(BF16).astype(F32)
            da = lax.dot_general(wide(DY, rows, 0, n_cols), WD[slot], NT_DIMS, preferred_element_type=F32)
            a, slope = gelu_and_slope(h)
            AT[:, rows] = a.astype(BF16).T
            DH[rows, :] = (da * slope).astype(BF16)

    def free_w(t):
        @pl.when(t + W_SLOTS < n_ticks)
        def _():
            pl.semaphore_signal(w_credit, inc=1, device_id=dev(rep, mate), device_id_type=MESH_ID)

    def more_w(t):
        @pl.when((t < n_ticks) & (t >= W_SLOTS))
        def _():
            pl.semaphore_wait(w_credit, 1)

        @pl.when(t < n_ticks)
        def _():
            start_w(t)

    def send_to_mate(t, part):
        slot = t % P_SLOTS
        if part == 0:
            src, dst = SU.at[slot, pl.ds(pl.multiple_of(mate * 512, 512), 512)], RU.at[slot]
        else:
            src, dst = SD.at[slot, pl.ds(pl.multiple_of(mate * 128, 128), 128)], RD.at[slot]
        pltpu.make_async_remote_copy(
            src, dst, p_send.at[slot], p_recv.at[slot], device_id=dev(rep, mate), device_id_type=MESH_ID).start()

    def take_pair_room(t):
        @pl.when(t >= P_SLOTS)
        def _():
            pl.semaphore_wait(r_credit, 1)

    def up(t):
        slot = t % P_SLOTS
        for s in range(2):
            rows = pl.ds(s * 512, 512)
            SU[slot, rows, :] = jnp.dot(XT[rows, :], DH[...], preferred_element_type=F32)

    def down(t):
        slot = t % P_SLOTS
        for s in range(2):
            cols = pl.ds(s * 512, 512)
            SD[slot, :, cols] = jnp.dot(AT[...], wide(DY, slice(None), 4 * s, 4 * s + 4), preferred_element_type=F32)

    def send(sent, src, dst, recv, to):
        pltpu.make_async_remote_copy(
            src, dst, sent, recv, device_id=dev(to, me), device_id_type=MESH_ID).start()

    def pair_stage(t):
        slot = t % P_SLOTS
        whole = SU.at[slot]
        pltpu.make_async_copy(whole, whole, p_recv.at[slot]).wait()
        own = pl.ds(pl.multiple_of(me * 512, 512), 512)
        for s in range(2):
            cols = pl.ds(s * 128, 128)
            GU[:, pl.ds(s * half_ff + t * 128, 128)] = SU[slot, own, cols] + RU[slot, :, cols]
        own = pl.ds(pl.multiple_of(me * 128, 128), 128)
        GD[pl.ds(t * 128, 128), :] = SD[slot, own, :] + RD[slot]
        pltpu.make_async_copy(whole, whole, p_send.at[slot]).wait()
        if t + P_SLOTS < n_ticks:
            pl.semaphore_signal(r_credit, inc=1, device_id=dev(rep, mate), device_id_type=MESH_ID)
        rs_a(t, 0)

    def rs_a(t, p):
        sent = (send0 if p == 0 else send1).at[t]
        m, off = PH_ROWS[p], PH_OFF[p]
        if is_direct(t, p):
            for k in (2, 1, 3):
                for g, axes, dirs in subs_of(t):
                    a = axes[p]
                    src = g_part(g, coord[axes[0]], row_in_quarter(axes, p) + quarter[a][k] * m, m)
                    send(sent, src, r_part(g, off + (k - 1) * m, m), rs2.at[t * 3 + p], near[a][k])
            return
        for relay in (True, False):
            for g, axes, dirs in subs_of(t):
                a, d = axes[p], dirs[p]
                q = quarter[a][2 if relay else -d % RING]
                src = g_part(g, q, 0, m) if p == 0 else g_part(g, coord[axes[0]], row_in_quarter(axes, p) + q * m, m)
                if relay:
                    send(sent, src, r_part(g, off, m), rs1.at[t * 3 + p], near[a][d])
                else:
                    send(sent, src, r_part(g, off + m, m), rs2.at[t * 3 + p], near[a][-d])

    def rs_b(t, p):
        sent = (send0 if p == 0 else send1).at[t]
        m, off = PH_ROWS[p], PH_OFF[p]
        wait_rows(rs1.at[t * 3 + p], SUBS * m)
        for g, axes, dirs in subs_of(t):
            a, d = axes[p], dirs[p]
            q = quarter[a][d % RING]
            part = g_part(g, q, 0, m) if p == 0 else g_part(g, coord[axes[0]], row_in_quarter(axes, p) + q * m, m)
            part[...] = part[...] + r_part(g, off, m)[...]
            send(sent, part, r_part(g, off + 2 * m, m), rs2.at[t * 3 + p], near[a][d])

    def rs_c(t, p):
        m, off = PH_ROWS[p], PH_OFF[p]
        straight = is_direct(t, p)
        wait_rows(rs2.at[t * 3 + p], (3 if straight else 2) * SUBS * m)
        for g, axes, dirs in subs_of(t):
            row = 0 if p == 0 else row_in_quarter(axes, p) + coord[axes[p]] * m
            part = g_part(g, coord[axes[0]], row, m)
            out = e_part(g, row, m) if p == 2 else part
            total = part[...] + (r_part(g, off + m, m)[...] + r_part(g, off + 2 * m, m)[...])
            out[...] = total + r_part(g, off, m)[...] if straight else total
        if p < 2:
            rs_a(t, p + 1)
        else:
            ag_a(t, 2)
        if p == 1:
            wait_rows(send0.at[t], 3 * SUBS * PH_ROWS[0])
            for a in sorted({axes[0] for _, axes, _ in subs_of(t)}):
                for d in (1, -1):
                    pl.semaphore_signal(g_free.at[t], inc=1, device_id=dev(near[a][d], me), device_id_type=MESH_ID)

    def ag_part(g, axes, p, q):
        if p == 0:
            return g_part(g, q, 0, PH_ROWS[0])
        return e_part(g, row_in_quarter(axes, p) + q * PH_ROWS[p], PH_ROWS[p])

    def ag_a(t, p):
        if p == 0:
            pl.semaphore_wait(g_free.at[t], 2 * len({axes[0] for _, axes, _ in subs_of(t)}))
        if is_direct(t, p):
            for k in (2, 1, 3):
                for g, axes, dirs in subs_of(t):
                    part = ag_part(g, axes, p, coord[axes[p]])
                    send(out_send.at[t], part, part, ag2.at[t * 3 + p], near[axes[p]][k])
            return
        for recv, sign in ((ag1, 1), (ag2, -1)):
            for g, axes, dirs in subs_of(t):
                a, d = axes[p], dirs[p]
                part = ag_part(g, axes, p, coord[a])
                src = e_part(g, 0, PH_ROWS[0]) if p == 0 else part
                send(out_send.at[t], src, part, recv.at[t * 3 + p], near[a][sign * d])
        if p == 0:
            wait_rows(send1.at[t], 3 * SUBS * (PH_ROWS[1] + PH_ROWS[2]))
            for g, axes, dirs in subs_of(t):
                g_part(g, coord[axes[0]], 0, PH_ROWS[0])[...] = e_part(g, 0, PH_ROWS[0])[...]

    def ag_b(t, p):
        wait_rows(ag1.at[t * 3 + p], SUBS * PH_ROWS[p])
        for g, axes, dirs in subs_of(t):
            a, d = axes[p], dirs[p]
            part = ag_part(g, axes, p, quarter[a][-d % RING])
            send(out_send.at[t], part, part, ag2.at[t * 3 + p], near[a][d])

    def ag_c(t, p):
        wait_rows(ag2.at[t * 3 + p], (3 if is_direct(t, p) else 2) * SUBS * PH_ROWS[p])
        if p > 0:
            ag_a(t, p - 1)

    def run(ops):
        for s, t in ops:
            name = STAGES[s]
            with jax.named_scope(name):
                if name == "pair":
                    pair_stage(t)
                else:
                    p = int(name[2])
                    {"rsb": rs_b, "rsc": rs_c, "agb": ag_b, "agc": ag_c}[name[:2] + name[3]](t, p)

    slots = program(n_ticks)

    def pick(t, first, lo, hi):
        lists = [slots[first(k)] for k in range(lo, hi)]
        if not any(lists):
            return
        if hi - lo == 1:
            run(lists[0])
            return
        mid = (lo + hi) // 2
        pl.when(t < mid)(lambda: pick(t, first, lo, mid))
        pl.when(t >= mid)(lambda: pick(t, first, mid, hi))

    n_half = n_tok // 2
    for part in range(2):
        for k in range(part * n_micro // 2, (part + 1) * n_micro // 2):
            with jax.named_scope("mask"):
                mask_micro(k)
            with jax.named_scope("xwait"):
                landed(X, k, in_sem.at[k])
        if part == 0:
            with jax.named_scope("wwait"):
                wait_w(0)
        with jax.named_scope("hidfirst"):
            hidden(0, part * n_half, (part + 1) * n_half, turn=True)
        if part == 0 and n_ticks > 1:
            start_w(1)
        run(slots[part])
    free_w(0)
    more_w(2)
    with jax.named_scope("upfirst"):
        up(0)
    send_to_mate(0, 0)
    run(slots[2])
    with jax.named_scope("downfirst"):
        down(0)
    send_to_mate(0, 1)
    run(slots[3])

    def tick(t, carry):
        with jax.named_scope("wwait"):
            wait_w(t)
        with jax.named_scope("hidden"):
            hidden(t, 0, n_tok)
        free_w(t)
        pick(t, lambda k: OPENING + 2 * k - 2, 1, n_ticks)
        more_w(t + 2)
        take_pair_room(t)
        with jax.named_scope("grad"):
            up(t)
            down(t)
            send_to_mate(t, 0)
            send_to_mate(t, 1)
        pick(t, lambda k: OPENING + 2 * k - 1, 1, n_ticks)
        return carry

    lax.fori_loop(1, n_ticks, tick, 0)
    run(slots[-1])
    for t in range(n_ticks):
        wait_rows(out_send.at[t], SUBS * R_ROWS)


FLUSH = 8


def flush(gu, gd, gu_hbm, gd_hbm, sem):
    copies = []
    for k in range(FLUSH):
        for ref, out, s in ((gu, gu_hbm, 0), (gd, gd_hbm, 1)):
            rows = pl.ds(k * (ref.shape[0] // FLUSH), ref.shape[0] // FLUSH)
            copies.append(pltpu.make_async_copy(ref.at[rows], out.at[0, rows], sem.at[2 * k + s]))
    for copy in copies:
        copy.start()
    for copy in copies:
        copy.wait()


def solution(mesh):
    tok_spec = P(None, ("model", "replica", "fsdp"), None)
    len_spec = P(None, ("model", "replica", "fsdp"))
    w_spec = P(None, ("model", "fsdp"), None)

    def device_grads(x_in, dy_out, lengths, w_up, w_down):
        n_micro, tok, d = x_in.shape
        n_tok = n_micro * tok
        d_ff = w_up.shape[2]
        n_ticks = d_ff // FC
        any_spec = pl.BlockSpec(memory_space=pl.ANY)
        dma = pltpu.SemaphoreType.DMA
        regular = pltpu.SemaphoreType.REGULAR
        sems = [
            dma((2 * n_micro,)),
            dma((W_SLOTS,)),
            dma((W_SLOTS,)),
            dma((W_SLOTS,)),
            dma((P_SLOTS,)),
            dma((P_SLOTS,)),
            dma((3 * n_ticks,)),
            dma((3 * n_ticks,)),
            dma((3 * n_ticks,)),
            dma((3 * n_ticks,)),
            dma((n_ticks,)),
            dma((n_ticks,)),
            dma((n_ticks,)),
            regular((n_ticks,)),
            regular,
            regular,
        ]
        gu, gd = pl.pallas_call(
            functools.partial(kernel, n_ticks, n_tok, n_micro, sems),
            out_shape=(
                pltpu.VMEM((d // 2, d_ff), F32),
                pltpu.VMEM((d_ff // 2, d), F32),
            ),
            in_specs=[any_spec, any_spec, pl.BlockSpec(memory_space=pltpu.SMEM), any_spec, any_spec],
            out_specs=(pl.BlockSpec(memory_space=pltpu.VMEM),) * 2,
            scratch_shapes=[
                pltpu.VMEM((d // LANES, n_tok, LANES), BF16),
                pltpu.VMEM((d // LANES, n_tok, LANES), BF16),
                pltpu.VMEM((d, n_tok), BF16),
                pltpu.VMEM((W_SLOTS, d, FC), BF16),
                pltpu.VMEM((W_SLOTS, FC, d), BF16),
                pltpu.VMEM((FC, n_tok), BF16),
                pltpu.VMEM((n_tok, FC), BF16),
                pltpu.VMEM((P_SLOTS, d, FC), F32),
                pltpu.VMEM((P_SLOTS, FC, d), F32),
                pltpu.VMEM((P_SLOTS, d // 2, FC), F32),
                pltpu.VMEM((P_SLOTS, FC // 2, d), F32),
                pltpu.VMEM((n_ticks * SUBS * R_ROWS, 128), F32),
                pltpu.VMEM((n_ticks * SUBS * PH_ROWS[0], 128), F32),
            ],
            compiler_params=pltpu.CompilerParams(
                collective_id=0, has_side_effects=True, vmem_limit_bytes=67043328 - (16 << 20)),
            name="grads",
        )(x_in, dy_out, lengths.reshape(n_micro), w_up, w_down)
        vmem = pl.BlockSpec(memory_space=pltpu.VMEM)
        return pl.pallas_call(
            flush,
            out_shape=(
                jax.ShapeDtypeStruct(w_up.shape, F32),
                jax.ShapeDtypeStruct(w_down.shape, F32),
            ),
            in_specs=[vmem, vmem],
            out_specs=(any_spec, any_spec),
            scratch_shapes=[dma((2 * FLUSH,))],
            compiler_params=pltpu.CompilerParams(vmem_limit_bytes=1 << 20),
            name="flush",
        )(pltpu.with_memory_space_constraint(gu, pltpu.VMEM), pltpu.with_memory_space_constraint(gd, pltpu.VMEM))

    return jax.shard_map(device_grads, mesh=mesh, in_specs=(tok_spec, tok_spec, len_spec, w_spec, w_spec), out_specs=(w_spec, w_spec), check_vma=False)
```

```python
import functools

import jax
import jax.numpy as jnp
from jax import lax
from jax.experimental import pallas as pl
from jax.experimental.pallas import tpu as pltpu
from jax.sharding import PartitionSpec as P

F32, BF16 = jnp.float32, jnp.bfloat16
MESH_ID = pl.DeviceIdType.MESH
SQRT_2_OVER_PI = 0.7978845608028654
CUBIC = 0.044715
NT_DIMS = (((1,), (1,)), ((), ()))

FC = 256
RING = 4
SUBS = 4
PH_ROWS = (128, 32, 8)
PH_OFF = (0, 384, 480)
R_ROWS = 504
W_SLOTS = 3
P_SLOTS = 2
STAGES = ("pair", "rs0b", "rs0c", "rs1b", "rs1c", "rs2b", "rs2c", "ag2b", "ag2c", "ag1b", "ag1c", "ag0b", "ag0c")

OPENING = 4
MIN_LEN = 128
TABLE = (
    (),
    (),
    (),
    (),
    ((0, 0),),
    (),
    ((1, 0),),
    ((0, 1),),
    ((2, 0),),
    ((1, 1), (0, 2),),
    ((4, 0), (0, 3),),
    ((1, 2), (2, 1),),
    ((6, 0), (0, 4), (1, 3),),
    ((2, 2),),
    ((4, 1), (8, 0), (1, 4), (0, 5),),
    ((4, 2), (2, 3),),
    ((6, 1), (0, 6),),
    ((6, 2), (1, 5), (2, 4), (10, 0),),
    ((4, 3), (1, 6), (8, 1),),
    ((0, 7), (8, 2),),
    ((2, 5), (3, 4), (0, 8),),
    ((2, 6), (1, 7), (11, 0), (10, 1),),
    (),
    ((6, 3), (3, 5), (4, 4), (1, 8), (3, 6), (0, 9),),
    ((2, 7), (0, 10),),
    ((4, 5), (4, 6), (5, 4), (2, 8), (10, 2),),
    ((1, 9), (3, 7), (0, 11), (1, 10),),
    ((5, 6), (5, 5), (3, 8), (6, 4), (8, 3),),
    ((0, 12), (11, 2),),
    ((4, 7), (12, 0), (2, 10), (11, 1), (2, 9), (6, 6),),
    ((6, 5), (4, 8), (7, 4), (1, 11), (10, 3),),
    ((1, 12), (3, 10), (3, 9), (5, 7), (0, 13), (5, 8), (7, 5), (7, 6),),
    ((2, 11), (8, 4), (0, 14),),
    (),
    ((4, 9), (4, 10), (2, 12), (8, 6), (1, 13), (3, 11), (6, 8), (8, 5), (9, 4), (0, 15), (5, 9), (5, 10), (3, 12), (9, 6), (6, 7), (1, 14), (2, 13), (4, 11), (10, 4), (1, 15), (6, 10), (5, 11), (4, 12), (7, 7), (6, 9), (2, 14), (9, 5), (3, 13), (7, 8), (10, 6), (6, 11), (8, 7), (7, 9), (7, 10), (2, 15), (5, 12), (3, 14), (4, 13), (10, 5), (8, 8), (8, 9), (7, 11), (3, 15), (9, 7), (8, 10), (6, 12), (4, 14), (5, 13), (11, 6), (11, 4), (11, 5), (6, 13), (5, 14), (4, 15), (9, 8), (7, 12), (9, 10), (9, 9), (10, 7), (8, 11), (6, 14), (5, 15), (7, 13), (11, 3), (10, 8), (8, 12), (7, 14), (12, 6), (6, 15), (9, 11), (10, 9), (11, 7), (8, 13), (8, 14), (7, 15), (12, 4), (9, 12), (10, 10), (11, 8), (11, 9), (12, 3), (8, 15), (9, 14), (10, 12), (9, 13), (10, 11), (9, 15), (10, 14), (10, 13), (12, 9), (10, 15), (11, 10), (11, 12), (11, 11), (12, 7), (11, 15), (11, 14), (11, 13), (12, 11), (12, 2), (12, 15), (12, 12), (12, 5), (12, 1), (12, 8), (12, 10), (12, 14), (12, 13),),
)
DIRECT = (3, 3, 3, 3, 0, 0, 0, 0, 0, 0, 0, 0, 0, 0, 0, 0)
LANES = 128
SHAPES = (
    4, 0, 6, 5, 12, 5, 4, 13, 8, 7, 4, 10, 4, 0, 6, 2, 8, 9, 6, 12, 0, 6, 14, 6, 0, 10, 8, 0, 8, 5, 2, 15,
    12, 4, 0, 14, 14, 0, 4, 14, 14, 0, 2, 10, 4, 8, 2, 6, 10, 6, 6, 4, 6, 2, 1, 4, 8, 6, 6, 9, 14, 6, 0, 10,
)


def is_direct(t, phase):
    return phase > 0 and DIRECT[t % len(DIRECT)] >> (phase - 1) & 1 == 1


def stages_of(t):
    return [k for k, n in enumerate(STAGES) if not (n[3:] == "b" and is_direct(t, int(n[2])))]


def program(n_ticks):
    if n_ticks == 16 and TABLE:
        return TABLE
    last = OPENING + 2 * (n_ticks - 1)
    slots = [[] for _ in range(last + 1)]
    for t in range(n_ticks):
        for k, s in enumerate(stages_of(t)):
            slots[min(OPENING + 2 * t + k, last)].append((s, t))
    slots[-1].sort()
    return slots


def gelu_and_slope(u):
    u2 = u * u
    half = 0.5 + 0.5 * jnp.tanh(u * (SQRT_2_OVER_PI + (CUBIC * SQRT_2_OVER_PI) * u2))
    a = u * half
    return a, half + (a * (1.0 - half)) * (2.0 * SQRT_2_OVER_PI + (6.0 * CUBIC * SQRT_2_OVER_PI) * u2)


def subs_of(t):
    blocks = []
    for g in range(SUBS * t, SUBS * t + SUBS):
        code, a = SHAPES[g % len(SHAPES)], g % 3
        b, c = ((a + 1) % 3, (a + 2) % 3) if code % 2 == 0 else ((a + 2) % 3, (a + 1) % 3)
        first = 1 if g // 3 % 2 == 0 else -1
        dirs = (-first if code & 8 else first, -1 if code & 2 else 1, -1 if code & 4 else 1)
        blocks.append((g, (a, b, c), dirs))
    return blocks


def kernel(n_ticks, n_tok, n_micro, sems, *refs):
    pl.run_scoped(functools.partial(body, n_ticks, n_tok, n_micro, refs), *sems)


def body(n_ticks, n_tok, n_micro, refs,
         in_sem, w_local, w_send, w_recv, p_send, p_recv, rs1, rs2, ag1, ag2, send0, send1, out_send,
         g_free, w_credit, r_credit):
    (x_hbm, dy_hbm, len_ref, wu_hbm, wd_hbm, GU, GD,
     X, DY, XT, WU, WD, AT, DH, SU, SD, RU, RD, R, E) = refs
    tok = n_tok // n_micro
    half_ff = n_ticks * 128
    rep = lax.axis_index("replica")
    me = lax.axis_index("fsdp")
    mate = 1 - me

    def dev(replica, core):
        return (0, replica, core)

    strides = [RING**a for a in range(3)]
    coord = [(rep // s) % RING for s in strides]
    quarter = [[coord[a]] + [(coord[a] + k) % RING for k in range(1, RING)] for a in range(3)]
    near = [{d: rep + strides[a] * (quarter[a][d % RING] - coord[a]) for d in (1, -1, 2, 3)} for a in range(3)]

    def row_in_quarter(axes, phase):
        row = 0
        for p in range(1, phase):
            row = row + coord[axes[p]] * PH_ROWS[p]
        return row

    def g_part(g, q, row, n):
        t, s = g // SUBS, g % SUBS
        if s < 2:
            start = q * 128 + row
            return GU.at[pl.ds(pl.multiple_of(start, 8), n), pl.ds(s * half_ff + t * 128, 128)]
        start = t * 128 + row
        if not isinstance(start, int):
            start = pl.multiple_of(start, 8)
        return GD.at[pl.ds(start, n), pl.ds(pl.multiple_of((s - 2) * 512 + q * 128, 128), 128)]

    def r_part(g, start, n):
        return R.at[pl.ds(g * R_ROWS + start, n)]

    def e_part(g, row, n):
        start = g * PH_ROWS[0] + row
        if not isinstance(start, int):
            start = pl.multiple_of(start, 8)
        return E.at[pl.ds(start, n)]

    def wait_rows(sem, n):
        ref = R.at[pl.ds(0, n)]
        pltpu.make_async_copy(ref, ref, sem).wait()

    barrier = pltpu.get_barrier_semaphore()
    for a in range(3):
        for d in (1, -1, 2):
            pl.semaphore_signal(barrier, inc=1, device_id=dev(near[a][d], me), device_id_type=MESH_ID)
    pl.semaphore_signal(barrier, inc=1, device_id=dev(rep, mate), device_id_type=MESH_ID)

    n_cols = X.shape[0]

    def x_copy(k):
        return [pltpu.make_async_copy(x_hbm.at[k, :, pl.ds(c * LANES, LANES)], X.at[c, pl.ds(k * tok, tok)], in_sem.at[k]) for c in range(n_cols)]

    def dy_copy(k):
        return [pltpu.make_async_copy(dy_hbm.at[k, :, pl.ds(c * LANES, LANES)], DY.at[c, pl.ds(k * tok, tok)], in_sem.at[n_micro + k]) for c in range(n_cols)]

    def landed(ref, k, sem):
        block = ref.at[:, pl.ds(k * tok, tok)]
        pltpu.make_async_copy(block, block, sem).wait()

    def w_parts(t):
        slot = t % W_SLOTS
        lo = pl.multiple_of(t * 128, 128)
        hi = pl.multiple_of(half_ff + t * 128, 128)
        up_rows = pl.ds(pl.multiple_of(me * 512, 512), 512)
        down_rows = pl.ds(pl.multiple_of(me * 128, 128), 128)
        return (
            (wu_hbm.at[0, :, pl.ds(lo, 128)], WU.at[slot, up_rows, pl.ds(0, 128)]),
            (wu_hbm.at[0, :, pl.ds(hi, 128)], WU.at[slot, up_rows, pl.ds(128, 128)]),
            (wd_hbm.at[0, pl.ds(lo, 128), :], WD.at[slot, down_rows, :]),
        )

    def start_w(t):
        for s, d in w_parts(t):
            pltpu.make_async_remote_copy(
                s, d, w_send.at[t % W_SLOTS], w_recv.at[t % W_SLOTS],
                device_id=dev(rep, mate), device_id_type=MESH_ID).start()

        for s, d in w_parts(t):
            pltpu.make_async_copy(s, d, w_local.at[t % W_SLOTS]).start()

    def wait_w(t):
        slot = t % W_SLOTS
        ref = WU.at[slot]
        for sem in (w_local, w_recv, w_send):
            pltpu.make_async_copy(ref, ref, sem.at[slot]).wait()

    for k in range(n_micro):
        for copy in x_copy(k):
            copy.start()
    for k in range(n_micro):
        for copy in dy_copy(k):
            copy.start()
    with jax.named_scope("entry"):
        pl.semaphore_wait(barrier, 10)
    start_w(0)
    if n_ticks > 1:
        start_w(1)

    mb = min(128, tok)
    clean = MIN_LEN if tok > MIN_LEN else 0

    def mask_micro(k):
        with jax.named_scope("dywait"):
            landed(DY, k, in_sem.at[n_micro + k])
        n_valid = len_ref[k]

        def mask_rows(s, carry):
            rows = pl.ds(pl.multiple_of(k * tok + clean + s * mb, mb), mb)
            at = clean + s * mb + lax.broadcasted_iota(jnp.int32, (mb, LANES), 0)
            keep = jnp.where(at < n_valid, 1.0, 0.0).astype(BF16)
            for c in range(n_cols):
                DY[c, rows, :] = DY[c, rows, :] * keep
            return carry

        lax.fori_loop(0, (tok - clean) // mb, mask_rows, 0)

    def wide(ref, rows, lo, hi):
        return jnp.concatenate([ref[c, rows, :] for c in range(lo, hi)], axis=1)

    cb = min(256, n_tok // 2)

    def hidden(t, lo, hi, turn=False):
        slot = t % W_SLOTS
        for at in range(lo, hi, cb):
            rows = pl.ds(at, cb)
            if turn:
                for c in range(n_cols):
                    XT[pl.ds(c * LANES, LANES), rows] = X[c, rows, :].T
            h = jnp.dot(wide(X, rows, 0, n_cols), WU[slot], preferred_element_type=F32).astype(BF16).astype(F32)
            da = lax.dot_general(wide(DY, rows, 0, n_cols), WD[slot], NT_DIMS, preferred_element_type=F32)
            a, slope = gelu_and_slope(h)
            AT[:, rows] = a.astype(BF16).T
            DH[rows, :] = (da * slope).astype(BF16)

    def free_w(t):
        @pl.when(t + W_SLOTS < n_ticks)
        def _():
            pl.semaphore_signal(w_credit, inc=1, device_id=dev(rep, mate), device_id_type=MESH_ID)

    def more_w(t):
        @pl.when((t < n_ticks) & (t >= W_SLOTS))
        def _():
            pl.semaphore_wait(w_credit, 1)

        @pl.when(t < n_ticks)
        def _():
            start_w(t)

    def send_to_mate(t, part):
        slot = t % P_SLOTS
        if part == 0:
            src, dst = SU.at[slot, pl.ds(pl.multiple_of(mate * 512, 512), 512)], RU.at[slot]
        else:
            src, dst = SD.at[slot, pl.ds(pl.multiple_of(mate * 128, 128), 128)], RD.at[slot]
        pltpu.make_async_remote_copy(
            src, dst, p_send.at[slot], p_recv.at[slot], device_id=dev(rep, mate), device_id_type=MESH_ID).start()

    def take_pair_room(t):
        @pl.when(t >= P_SLOTS)
        def _():
            pl.semaphore_wait(r_credit, 1)

    def up(t):
        slot = t % P_SLOTS
        for s in range(2):
            rows = pl.ds(s * 512, 512)
            SU[slot, rows, :] = jnp.dot(XT[rows, :], DH[...], preferred_element_type=F32)

    def down(t):
        slot = t % P_SLOTS
        for s in range(2):
            cols = pl.ds(s * 512, 512)
            SD[slot, :, cols] = jnp.dot(AT[...], wide(DY, slice(None), 4 * s, 4 * s + 4), preferred_element_type=F32)

    def send(sent, src, dst, recv, to):
        pltpu.make_async_remote_copy(
            src, dst, sent, recv, device_id=dev(to, me), device_id_type=MESH_ID).start()

    def pair_stage(t):
        slot = t % P_SLOTS
        whole = SU.at[slot]
        pltpu.make_async_copy(whole, whole, p_recv.at[slot]).wait()
        own = pl.ds(pl.multiple_of(me * 512, 512), 512)
        for s in range(2):
            cols = pl.ds(s * 128, 128)
            GU[:, pl.ds(s * half_ff + t * 128, 128)] = SU[slot, own, cols] + RU[slot, :, cols]
        own = pl.ds(pl.multiple_of(me * 128, 128), 128)
        GD[pl.ds(t * 128, 128), :] = SD[slot, own, :] + RD[slot]
        pltpu.make_async_copy(whole, whole, p_send.at[slot]).wait()
        if t + P_SLOTS < n_ticks:
            pl.semaphore_signal(r_credit, inc=1, device_id=dev(rep, mate), device_id_type=MESH_ID)
        rs_a(t, 0)

    def rs_a(t, p):
        sent = (send0 if p == 0 else send1).at[t]
        m, off = PH_ROWS[p], PH_OFF[p]
        if is_direct(t, p):
            for k in (2, 1, 3):
                for g, axes, dirs in subs_of(t):
                    a = axes[p]
                    src = g_part(g, coord[axes[0]], row_in_quarter(axes, p) + quarter[a][k] * m, m)
                    send(sent, src, r_part(g, off + (k - 1) * m, m), rs2.at[t * 3 + p], near[a][k])
            return
        for relay in (True, False):
            for g, axes, dirs in subs_of(t):
                a, d = axes[p], dirs[p]
                q = quarter[a][2 if relay else -d % RING]
                src = g_part(g, q, 0, m) if p == 0 else g_part(g, coord[axes[0]], row_in_quarter(axes, p) + q * m, m)
                if relay:
                    send(sent, src, r_part(g, off, m), rs1.at[t * 3 + p], near[a][d])
                else:
                    send(sent, src, r_part(g, off + m, m), rs2.at[t * 3 + p], near[a][-d])

    def rs_b(t, p):
        sent = (send0 if p == 0 else send1).at[t]
        m, off = PH_ROWS[p], PH_OFF[p]
        wait_rows(rs1.at[t * 3 + p], SUBS * m)
        for g, axes, dirs in subs_of(t):
            a, d = axes[p], dirs[p]
            q = quarter[a][d % RING]
            part = g_part(g, q, 0, m) if p == 0 else g_part(g, coord[axes[0]], row_in_quarter(axes, p) + q * m, m)
            part[...] = part[...] + r_part(g, off, m)[...]
            send(sent, part, r_part(g, off + 2 * m, m), rs2.at[t * 3 + p], near[a][d])

    def rs_c(t, p):
        m, off = PH_ROWS[p], PH_OFF[p]
        straight = is_direct(t, p)
        wait_rows(rs2.at[t * 3 + p], (3 if straight else 2) * SUBS * m)
        for g, axes, dirs in subs_of(t):
            row = 0 if p == 0 else row_in_quarter(axes, p) + coord[axes[p]] * m
            part = g_part(g, coord[axes[0]], row, m)
            out = e_part(g, row, m) if p == 2 else part
            total = part[...] + (r_part(g, off + m, m)[...] + r_part(g, off + 2 * m, m)[...])
            out[...] = total + r_part(g, off, m)[...] if straight else total
        if p < 2:
            rs_a(t, p + 1)
        else:
            ag_a(t, 2)
        if p == 1:
            wait_rows(send0.at[t], 3 * SUBS * PH_ROWS[0])
            for a in sorted({axes[0] for _, axes, _ in subs_of(t)}):
                for d in (1, -1):
                    pl.semaphore_signal(g_free.at[t], inc=1, device_id=dev(near[a][d], me), device_id_type=MESH_ID)

    def ag_part(g, axes, p, q):
        if p == 0:
            return g_part(g, q, 0, PH_ROWS[0])
        return e_part(g, row_in_quarter(axes, p) + q * PH_ROWS[p], PH_ROWS[p])

    def ag_a(t, p):
        if p == 0:
            pl.semaphore_wait(g_free.at[t], 2 * len({axes[0] for _, axes, _ in subs_of(t)}))
        if is_direct(t, p):
            for k in (2, 1, 3):
                for g, axes, dirs in subs_of(t):
                    part = ag_part(g, axes, p, coord[axes[p]])
                    send(out_send.at[t], part, part, ag2.at[t * 3 + p], near[axes[p]][k])
            return
        for recv, sign in ((ag1, 1), (ag2, -1)):
            for g, axes, dirs in subs_of(t):
                a, d = axes[p], dirs[p]
                part = ag_part(g, axes, p, coord[a])
                src = e_part(g, 0, PH_ROWS[0]) if p == 0 else part
                send(out_send.at[t], src, part, recv.at[t * 3 + p], near[a][sign * d])
        if p == 0:
            wait_rows(send1.at[t], 3 * SUBS * (PH_ROWS[1] + PH_ROWS[2]))
            for g, axes, dirs in subs_of(t):
                g_part(g, coord[axes[0]], 0, PH_ROWS[0])[...] = e_part(g, 0, PH_ROWS[0])[...]

    def ag_b(t, p):
        wait_rows(ag1.at[t * 3 + p], SUBS * PH_ROWS[p])
        for g, axes, dirs in subs_of(t):
            a, d = axes[p], dirs[p]
            part = ag_part(g, axes, p, quarter[a][-d % RING])
            send(out_send.at[t], part, part, ag2.at[t * 3 + p], near[a][d])

    def ag_c(t, p):
        wait_rows(ag2.at[t * 3 + p], (3 if is_direct(t, p) else 2) * SUBS * PH_ROWS[p])
        if p > 0:
            ag_a(t, p - 1)

    def run(ops):
        for s, t in ops:
            name = STAGES[s]
            with jax.named_scope(name):
                if name == "pair":
                    pair_stage(t)
                else:
                    p = int(name[2])
                    {"rsb": rs_b, "rsc": rs_c, "agb": ag_b, "agc": ag_c}[name[:2] + name[3]](t, p)

    slots = program(n_ticks)

    def pick(t, first, lo, hi):
        lists = [slots[first(k)] for k in range(lo, hi)]
        if not any(lists):
            return
        if hi - lo == 1:
            run(lists[0])
            return
        mid = (lo + hi) // 2
        pl.when(t < mid)(lambda: pick(t, first, lo, mid))
        pl.when(t >= mid)(lambda: pick(t, first, mid, hi))

    n_half = n_tok // 2
    for part in range(2):
        for k in range(part * n_micro // 2, (part + 1) * n_micro // 2):
            with jax.named_scope("mask"):
                mask_micro(k)
            with jax.named_scope("xwait"):
                landed(X, k, in_sem.at[k])
        if part == 0:
            with jax.named_scope("wwait"):
                wait_w(0)
        with jax.named_scope("hidfirst"):
            hidden(0, part * n_half, (part + 1) * n_half, turn=True)
        run(slots[part])
    free_w(0)
    more_w(2)
    with jax.named_scope("upfirst"):
        up(0)
    send_to_mate(0, 0)
    run(slots[2])
    with jax.named_scope("downfirst"):
        down(0)
    send_to_mate(0, 1)
    run(slots[3])

    def tick(t, carry):
        with jax.named_scope("wwait"):
            wait_w(t)
        with jax.named_scope("hidden"):
            hidden(t, 0, n_tok)
        free_w(t)
        pick(t, lambda k: OPENING + 2 * k - 2, 1, n_ticks)
        more_w(t + 2)
        take_pair_room(t)
        with jax.named_scope("grad"):
            up(t)
            down(t)
            send_to_mate(t, 0)
            send_to_mate(t, 1)
        pick(t, lambda k: OPENING + 2 * k - 1, 1, n_ticks)
        return carry

    lax.fori_loop(1, n_ticks, tick, 0)
    run(slots[-1])
    for t in range(n_ticks):
        wait_rows(out_send.at[t], SUBS * R_ROWS)


FLUSH = 8


def flush(gu, gd, gu_hbm, gd_hbm, sem):
    copies = []
    for k in range(FLUSH):
        for ref, out, s in ((gu, gu_hbm, 0), (gd, gd_hbm, 1)):
            rows = pl.ds(k * (ref.shape[0] // FLUSH), ref.shape[0] // FLUSH)
            copies.append(pltpu.make_async_copy(ref.at[rows], out.at[0, rows], sem.at[2 * k + s]))
    for copy in copies:
        copy.start()
    for copy in copies:
        copy.wait()


def solution(mesh):
    tok_spec = P(None, ("model", "replica", "fsdp"), None)
    len_spec = P(None, ("model", "replica", "fsdp"))
    w_spec = P(None, ("model", "fsdp"), None)

    def device_grads(x_in, dy_out, lengths, w_up, w_down):
        n_micro, tok, d = x_in.shape
        n_tok = n_micro * tok
        d_ff = w_up.shape[2]
        n_ticks = d_ff // FC
        any_spec = pl.BlockSpec(memory_space=pl.ANY)
        dma = pltpu.SemaphoreType.DMA
        regular = pltpu.SemaphoreType.REGULAR
        sems = [
            dma((2 * n_micro,)),
            dma((W_SLOTS,)),
            dma((W_SLOTS,)),
            dma((W_SLOTS,)),
            dma((P_SLOTS,)),
            dma((P_SLOTS,)),
            dma((3 * n_ticks,)),
            dma((3 * n_ticks,)),
            dma((3 * n_ticks,)),
            dma((3 * n_ticks,)),
            dma((n_ticks,)),
            dma((n_ticks,)),
            dma((n_ticks,)),
            regular((n_ticks,)),
            regular,
            regular,
        ]
        gu, gd = pl.pallas_call(
            functools.partial(kernel, n_ticks, n_tok, n_micro, sems),
            out_shape=(
                pltpu.VMEM((d // 2, d_ff), F32),
                pltpu.VMEM((d_ff // 2, d), F32),
            ),
            in_specs=[any_spec, any_spec, pl.BlockSpec(memory_space=pltpu.SMEM), any_spec, any_spec],
            out_specs=(pl.BlockSpec(memory_space=pltpu.VMEM),) * 2,
            scratch_shapes=[
                pltpu.VMEM((d // LANES, n_tok, LANES), BF16),
                pltpu.VMEM((d // LANES, n_tok, LANES), BF16),
                pltpu.VMEM((d, n_tok), BF16),
                pltpu.VMEM((W_SLOTS, d, FC), BF16),
                pltpu.VMEM((W_SLOTS, FC, d), BF16),
                pltpu.VMEM((FC, n_tok), BF16),
                pltpu.VMEM((n_tok, FC), BF16),
                pltpu.VMEM((P_SLOTS, d, FC), F32),
                pltpu.VMEM((P_SLOTS, FC, d), F32),
                pltpu.VMEM((P_SLOTS, d // 2, FC), F32),
                pltpu.VMEM((P_SLOTS, FC // 2, d), F32),
                pltpu.VMEM((n_ticks * SUBS * R_ROWS, 128), F32),
                pltpu.VMEM((n_ticks * SUBS * PH_ROWS[0], 128), F32),
            ],
            compiler_params=pltpu.CompilerParams(
                collective_id=0, has_side_effects=True, vmem_limit_bytes=67043328 - (16 << 20)),
            name="grads",
        )(x_in, dy_out, lengths.reshape(n_micro), w_up, w_down)
        vmem = pl.BlockSpec(memory_space=pltpu.VMEM)
        return pl.pallas_call(
            flush,
            out_shape=(
                jax.ShapeDtypeStruct(w_up.shape, F32),
                jax.ShapeDtypeStruct(w_down.shape, F32),
            ),
            in_specs=[vmem, vmem],
            out_specs=(any_spec, any_spec),
            scratch_shapes=[dma((2 * FLUSH,))],
            compiler_params=pltpu.CompilerParams(vmem_limit_bytes=1 << 20),
            name="flush",
        )(pltpu.with_memory_space_constraint(gu, pltpu.VMEM), pltpu.with_memory_space_constraint(gd, pltpu.VMEM))

    return jax.shard_map(device_grads, mesh=mesh, in_specs=(tok_spec, tok_spec, len_spec, w_spec, w_spec), out_specs=(w_spec, w_spec), check_vma=False)
```
